32 devices in a mesh: fsdp: 4 (over y, core), context: 4 (over z), tensor: 2 (over x).
Axes of the slice: x: 2, y: 2, z: 4, core: 2. Of those that a mesh axis runs over, the one named last changes fastest.
Arguments:
- hidden_in: float32 [4, 512, 2560], P('fsdp', 'context'), may hold values from -6 to 6
- cotangent: float32 [4, 512, 2560], P('fsdp', 'context'), may hold values from -6 to 6
- segment_ids: int32 [4, 512], P('fsdp', 'context'), may hold values from 0 to 3, as said below
- positions: int32 [4, 512], P('fsdp', 'context'), may hold values from 0 to 511, as said below
- attn_scale: float32 [2560], P(('fsdp', 'context')), may hold values from -0.5 to 0.5
- query_weight: float32 [2560, 2560], P(('fsdp', 'context'), 'tensor')
- keyval_weight: float32 [2560, 512], P(('fsdp', 'context'))
- output_weight: float32 [2560, 2560], P('tensor', ('fsdp', 'context')), may hold values from -0.5 to 0.5
- mlp_scale: float32 [2560], P(('fsdp', 'context')), may hold values from -0.5 to 0.5
- gate_weight: float32 [2560, 7680], P(('fsdp', 'context'), 'tensor'), may hold values from -0.125 to 0.125
- up_weight: float32 [2560, 7680], P(('fsdp', 'context'), 'tensor'), may hold values from -0.125 to 0.125
- down_weight: float32 [7680, 2560], P('tensor', ('fsdp', 'context')), may hold values from -0.0625 to 0.0625
- first_attn_scale: float32 [2560], P(('fsdp', 'context')), may hold values from -40 to 40
- first_query_weight: float32 [2560, 2560], P(('fsdp', 'context'), 'tensor'), may hold values from -16 to 16
- first_keyval_weight: float32 [2560, 512], P(('fsdp', 'context')), may hold values from -80 to 80
- first_output_weight: float32 [2560, 2560], P('tensor', ('fsdp', 'context')), may hold values from -4 to 4
- first_mlp_scale: float32 [2560], P(('fsdp', 'context')), may hold values from -20 to 20
- first_gate_weight: float32 [2560, 7680], P(('fsdp', 'context'), 'tensor'), may hold values from -16 to 16
- first_up_weight: float32 [2560, 7680], P(('fsdp', 'context'), 'tensor'), may hold values from -16 to 16
- first_down_weight: float32 [7680, 2560], P('tensor', ('fsdp', 'context')), may hold values from -24 to 24
- second_attn_scale: float32 [2560], P(('fsdp', 'context')), may hold values from 0.6144 to 6.144
- second_query_weight: float32 [2560, 2560], P(('fsdp', 'context'), 'tensor'), may hold values from 0.1024 to 1.024
- second_keyval_weight: float32 [2560, 512], P(('fsdp', 'context')), may hold values from 2.4576 to 24.576
- second_output_weight: float32 [2560, 2560], P('tensor', ('fsdp', 'context')), may hold values from 0.006 to 0.06
- second_mlp_scale: float32 [2560], P(('fsdp', 'context')), may hold values from 0.2048 to 2.048
- second_gate_weight: float32 [2560, 7680], P(('fsdp', 'context'), 'tensor'), may hold values from 0.1024 to 1.024
- second_up_weight: float32 [2560, 7680], P(('fsdp', 'context'), 'tensor'), may hold values from 0.1024 to 1.024
- second_down_weight: float32 [7680, 2560], P('tensor', ('fsdp', 'context')), may hold values from 0.2048 to 2.048
Outputs:
- block_output: float32 [4, 512, 2560], P('fsdp', 'context')
- input_grad: float32 [4, 512, 2560], P('fsdp', 'context')
- grad_attn_scale: float32 [2560], P(('fsdp', 'context'))
- grad_query_weight: float32 [2560, 2560], P(('fsdp', 'context'), 'tensor')
- grad_keyval_weight: float32 [2560, 512], P(('fsdp', 'context'))
- grad_output_weight: float32 [2560, 2560], P('tensor', ('fsdp', 'context'))
- grad_mlp_scale: float32 [2560], P(('fsdp', 'context'))
- grad_gate_weight: float32 [2560, 7680], P(('fsdp', 'context'), 'tensor')
- grad_up_weight: float32 [2560, 7680], P(('fsdp', 'context'), 'tensor')
- grad_down_weight: float32 [7680, 2560], P('tensor', ('fsdp', 'context'))
- new_attn_scale: float32 [2560], P(('fsdp', 'context'))
- new_query_weight: float32 [2560, 2560], P(('fsdp', 'context'), 'tensor')
- new_keyval_weight: float32 [2560, 512], P(('fsdp', 'context'))
- new_output_weight: float32 [2560, 2560], P('tensor', ('fsdp', 'context'))
- new_mlp_scale: float32 [2560], P(('fsdp', 'context'))
- new_gate_weight: float32 [2560, 7680], P(('fsdp', 'context'), 'tensor')
- new_up_weight: float32 [2560, 7680], P(('fsdp', 'context'), 'tensor')
- new_down_weight: float32 [7680, 2560], P('tensor', ('fsdp', 'context'))
- new_first_attn_scale: float32 [2560], P(('fsdp', 'context'))
- new_first_query_weight: float32 [2560, 2560], P(('fsdp', 'context'), 'tensor')
- new_first_keyval_weight: float32 [2560, 512], P(('fsdp', 'context'))
- new_first_output_weight: float32 [2560, 2560], P('tensor', ('fsdp', 'context'))
- new_first_mlp_scale: float32 [2560], P(('fsdp', 'context'))
- new_first_gate_weight: float32 [2560, 7680], P(('fsdp', 'context'), 'tensor')
- new_first_up_weight: float32 [2560, 7680], P(('fsdp', 'context'), 'tensor')
- new_first_down_weight: float32 [7680, 2560], P('tensor', ('fsdp', 'context'))
- new_second_attn_scale: float32 [2560], P(('fsdp', 'context'))
- new_second_query_weight: float32 [2560, 2560], P(('fsdp', 'context'), 'tensor')
- new_second_keyval_weight: float32 [2560, 512], P(('fsdp', 'context'))
- new_second_output_weight: float32 [2560, 2560], P('tensor', ('fsdp', 'context'))
- new_second_mlp_scale: float32 [2560], P(('fsdp', 'context'))
- new_second_gate_weight: float32 [2560, 7680], P(('fsdp', 'context'), 'tensor')
- new_second_up_weight: float32 [2560, 7680], P(('fsdp', 'context'), 'tensor')
- new_second_down_weight: float32 [7680, 2560], P('tensor', ('fsdp', 'context'))
The draws below stay inside these ranges and needn't reach their ends.
Inputs may be any that keep to these rules, and one draw needn't show every extreme that they name: segment_ids start at 0 and never fall along a sequence; a document is a run of equal values; the first sequence is one document, every other sequence holds four. positions count the tokens from the first token of the token's document, which has 0.
All inputs are finite; a program needn't handle non-finite values.
Results may differ from the reference program's by a relative error of at most 0.014.
Values may be sent and summed in bfloat16 or wider, within the bound.
A program may use at most 448 MiB of HBM per device.

```python
import math
import jax
import jax.numpy as jnp
from jax import lax

D = 2560
HEADS = 10
HD = 256
FF = 7680
LEN = 512
SEQS = 4


def document_layout(key):
    row_keys = jax.random.split(jax.random.fold_in(key, 31), SEQS)

    def three_cuts(row_key):
        return (jax.random.permutation(row_key, LEN - 1)[:3] + 1).astype(jnp.int32)
    cuts = jax.vmap(three_cuts)(row_keys)
    steps = jnp.arange(LEN, dtype=jnp.int32)[None, :] * jnp.ones((SEQS, 1), jnp.int32)
    marks = jnp.any(steps[:, :, None] == cuts[:, None, :], axis=-1)
    first_row = jnp.arange(SEQS, dtype=jnp.int32)[:, None] == 0
    marks = jnp.where(first_row, False, marks)
    starts = lax.cummax(jnp.where(marks, steps, 0), axis=1)
    segments = jnp.cumsum(marks.astype(jnp.int32), axis=1).astype(jnp.int32)
    return (segments, (steps - starts).astype(jnp.int32))


def projection_pair(key):
    keyval = jax.random.truncated_normal(jax.random.fold_in(key, 41), -6.0, 6.0, (D, 2 * HD), jnp.float32) * D ** (-0.5)
    query = jax.random.truncated_normal(jax.random.fold_in(key, 42), -6.0, 6.0, (D, HEADS, HD), jnp.float32) * D ** (-0.5)
    return (query.reshape(D, HEADS * HD), keyval)


def draw_segment_ids(key, part):
    return document_layout(key)[0]


def draw_positions(key, part):
    return document_layout(key)[1]


def draw_query_weight(key, part):
    return projection_pair(key)[0]


def draw_keyval_weight(key, part):
    return projection_pair(key)[1]


def level_of(rng, dims, shards, low, largest):
    level = 1.0
    for dim, shards_of in shards:
        draws = jax.random.uniform(jax.random.fold_in(jax.random.fold_in(rng, 6), dim), (shards_of,), jnp.float32, low / len(shards), largest / len(shards))
        level = level * jnp.repeat(jnp.exp(draws), dims[dim] // shards_of).reshape((-1,) + (1,) * (len(dims) - 1 - dim))
    return level


def bell_draw(key, extent, width, bound, cuts=(), held_as=jnp.bfloat16):
    entries = width * jax.random.normal(key, extent, jnp.float32)
    if cuts:
        entries = entries * level_of(key, extent, cuts, -0.22, 0.18)
    return jnp.clip(entries, -bound, bound).astype(held_as)


def setup_inputs(seed: int = 0) -> dict:
    seeds = jax.random.split(jax.random.key(seed), 29)
    return {
        "hidden_in": bell_draw(seeds[0], (SEQS, LEN, D), 1.0, 6.0, ((0, 4), (1, 4)), jnp.float32),
        "cotangent": bell_draw(seeds[1], (SEQS, LEN, D), 1.0, 6.0, ((0, 4), (1, 4)), jnp.float32),
        "segment_ids": draw_segment_ids(jax.random.fold_in(seeds[28], 71), 0),
        "positions": draw_positions(jax.random.fold_in(seeds[28], 71), 0),
        "attn_scale": bell_draw(seeds[4], (D,), 0.1, 0.5, ((0, 16),), jnp.float32),
        "query_weight": draw_query_weight(jax.random.fold_in(seeds[28], 71), 0),
        "keyval_weight": draw_keyval_weight(jax.random.fold_in(seeds[28], 71), 0),
        "output_weight": bell_draw(seeds[7], (HEADS * HD, D), (HEADS * HD * 32 // LEN) ** -0.5, 0.5, ((0, 2), (1, 16)), jnp.float32),
        "mlp_scale": bell_draw(seeds[8], (D,), 0.1, 0.5, ((0, 16),), jnp.float32),
        "gate_weight": bell_draw(seeds[9], (D, FF), D ** -0.5, 0.125, ((0, 16), (1, 2)), jnp.float32),
        "up_weight": bell_draw(seeds[10], (D, FF), D ** -0.5, 0.125, ((0, 16), (1, 2)), jnp.float32),
        "down_weight": bell_draw(seeds[11], (FF, D), FF ** -0.5, 0.0625, ((0, 2), (1, 16)), jnp.float32),
        "first_attn_scale": bell_draw(seeds[12], (D,), (0.15 * (SEQS * LEN) ** 0.5), 40.0, ((0, 16),), jnp.float32),
        "first_query_weight": bell_draw(seeds[13], (D, HEADS * HD), (0.06 * (SEQS * LEN) ** 0.5), 16.0, ((0, 16), (1, 2)), jnp.float32),
        "first_keyval_weight": bell_draw(seeds[14], (D, 2 * HD), (0.3 * (SEQS * LEN) ** 0.5), 80.0, ((0, 16),), jnp.float32),
        "first_output_weight": bell_draw(seeds[15], (HEADS * HD, D), (0.15 * (5 * SEQS) ** 0.5), 4.0, ((0, 2), (1, 16)), jnp.float32),
        "first_mlp_scale": bell_draw(seeds[16], (D,), (0.08 * (SEQS * LEN) ** 0.5), 20.0, ((0, 16),), jnp.float32),
        "first_gate_weight": bell_draw(seeds[17], (D, FF), (0.06 * (SEQS * LEN) ** 0.5), 16.0, ((0, 16), (1, 2)), jnp.float32),
        "first_up_weight": bell_draw(seeds[18], (D, FF), (0.06 * (SEQS * LEN) ** 0.5), 16.0, ((0, 16), (1, 2)), jnp.float32),
        "first_down_weight": bell_draw(seeds[19], (FF, D), (0.09 * (SEQS * LEN) ** 0.5), 24.0, ((0, 2), (1, 16)), jnp.float32),
        "second_attn_scale": jnp.clip(jnp.exp(math.log(6.144) - 2.3025851 * jax.random.uniform(seeds[20], (D,), jnp.float32) ** level_of(seeds[20], (D,), ((0, 16),), -0.2, 0.2)), 0.6144, 6.144),
        "second_query_weight": jnp.clip(jnp.exp(math.log(1.024) - 2.3025852 * jax.random.uniform(seeds[21], (D, HEADS * HD), jnp.float32) ** level_of(seeds[21], (D, HEADS * HD), ((0, 16), (1, 2)), -0.2, 0.2)), 0.1024, 1.024),
        "second_keyval_weight": jnp.clip(jnp.exp(math.log(24.576) - 2.3025851 * jax.random.uniform(seeds[22], (D, 2 * HD), jnp.float32) ** level_of(seeds[22], (D, 2 * HD), ((0, 16),), -0.2, 0.2)), 2.4576, 24.576),
        "second_output_weight": jnp.clip(jnp.exp(math.log(0.06) - 2.3025851 * jax.random.uniform(seeds[23], (HEADS * HD, D), jnp.float32) ** level_of(seeds[23], (HEADS * HD, D), ((0, 2), (1, 16)), -0.2, 0.2)), 0.006, 0.06),
        "second_mlp_scale": jnp.clip(jnp.exp(math.log(2.048) - 2.3025852 * jax.random.uniform(seeds[24], (D,), jnp.float32) ** level_of(seeds[24], (D,), ((0, 16),), -0.2, 0.2)), 0.2048, 2.048),
        "second_gate_weight": jnp.clip(jnp.exp(math.log(1.024) - 2.3025852 * jax.random.uniform(seeds[25], (D, FF), jnp.float32) ** level_of(seeds[25], (D, FF), ((0, 16), (1, 2)), -0.2, 0.2)), 0.1024, 1.024),
        "second_up_weight": jnp.clip(jnp.exp(math.log(1.024) - 2.3025852 * jax.random.uniform(seeds[26], (D, FF), jnp.float32) ** level_of(seeds[26], (D, FF), ((0, 16), (1, 2)), -0.2, 0.2)), 0.1024, 1.024),
        "second_down_weight": jnp.clip(jnp.exp(math.log(2.048) - 2.3025852 * jax.random.uniform(seeds[27], (FF, D), jnp.float32) ** level_of(seeds[27], (FF, D), ((0, 2), (1, 16)), -0.2, 0.2)), 0.2048, 2.048),
    }


norm_eps = 1e-06
beta_one = 0.9
beta_two = 0.999
adam_eps = 1e-08
learn_rate = 0.03
decay_rate = 0.1
adam_step = 4.0
rope_base = 10000.0
masked_value = -1e+30

def gelu_tanh(values):
    return jax.nn.gelu(values, approximate=True)

def rope_tables(positions):
    half = HD // 2
    freq = rope_base ** (-2.0 * jnp.arange(half).astype(jnp.float32) / HD)
    angle = positions.astype(jnp.float32)[..., None] * freq
    return (jnp.cos(angle), jnp.sin(angle))

def rotate(values, cosine, sine):
    half = values.shape[-1] // 2
    first = values[..., :half]
    second = values[..., half:]
    return jnp.concatenate([first * cosine - second * sine, second * cosine + first * sine], axis=-1)

def unrotate(values, cosine, sine):
    half = values.shape[-1] // 2
    first = values[..., :half]
    second = values[..., half:]
    return jnp.concatenate([first * cosine + second * sine, second * cosine - first * sine], axis=-1)

def rms_forward(values, scale):
    inverse = lax.rsqrt(lax.optimization_barrier(jnp.mean(values * values, axis=-1, keepdims=True)) + norm_eps)
    normed = values * inverse
    return (normed, inverse, (normed * (1.0 + scale)).astype(jnp.bfloat16))

def rms_backward(dnorm, normed, inverse, scale):
    dnormed = dnorm * (1.0 + scale)
    dvalues = inverse * (dnormed - normed * lax.optimization_barrier(jnp.mean(dnormed * normed, axis=-1, keepdims=True)))
    return (dvalues, dnorm * normed)

def adamw(weight, grad, first, second):
    first_new = beta_one * first + (1.0 - beta_one) * grad
    second_new = beta_two * second + (1.0 - beta_two) * grad * grad
    fix_one = 1.0 - beta_one ** adam_step
    fix_two = 1.0 - beta_two ** adam_step
    update = first_new / fix_one / (jnp.sqrt(second_new / fix_two) + adam_eps)
    return (weight - learn_rate * (update + decay_rate * weight), first_new, second_new)

def sequence_pass(carry, inputs, weights):
    hidden, cotangent, segments, positions = inputs
    scale_one, wq_low, wkv_low, wo_low, scale_two, wg_low, wu_low, wd_low = weights
    single = jnp.float32
    half_type = jnp.bfloat16
    length = hidden.shape[0]
    normed_one, inv_one, low_one = rms_forward(hidden, scale_one)
    query = jnp.dot(low_one, wq_low, preferred_element_type=single).reshape(length, HEADS, HD)
    keyval = jnp.dot(low_one, wkv_low, preferred_element_type=single)
    cosine, sine = rope_tables(positions)
    query_low = (rotate(query, cosine[:, None, :], sine[:, None, :]) * HD ** (-0.5)).astype(half_type)
    key_low = rotate(keyval[:, :HD], cosine, sine).astype(half_type)
    value_low = keyval[:, HD:].astype(half_type)
    index = jnp.arange(length).astype(jnp.int32)
    distance = index[:, None] - index[None, :]
    allowed = ((segments[:, None] == segments[None, :]) & (distance >= 0))[None]
    scores = jnp.einsum('ihd,jd->hij', query_low.astype(single), key_low.astype(single))
    masked = jnp.where(allowed, scores, masked_value)
    top = lax.optimization_barrier(jnp.max(masked, axis=-1, keepdims=True))
    total = lax.optimization_barrier(jnp.sum(jnp.where(allowed, jnp.exp(masked - top), 0.0), axis=-1, keepdims=True))
    lse = top + jnp.log(total)
    prob = jnp.where(allowed, jnp.exp(masked - lse), 0.0)
    prob_low = prob.astype(half_type)
    att_low = jnp.einsum('hij,jd->ihd', prob_low.astype(single), value_low.astype(single)).astype(half_type)
    att_flat = att_low.reshape(length, HEADS * HD)
    mid = hidden + jnp.dot(att_flat, wo_low, preferred_element_type=single)
    normed_two, inv_two, low_two = rms_forward(mid, scale_two)
    gate = jnp.dot(low_two, wg_low, preferred_element_type=single)
    upper = jnp.dot(low_two, wu_low, preferred_element_type=single)
    gelu_gate, gelu_back = jax.vjp(gelu_tanh, gate)
    hid_low = (gelu_gate * upper).astype(half_type)
    output = mid + jnp.dot(hid_low, wd_low, preferred_element_type=single)
    dy_low = cotangent.astype(half_type)
    grad_wd = jnp.dot(hid_low.T, dy_low, preferred_element_type=single)
    dhid = jnp.dot(dy_low, wd_low.T, preferred_element_type=single)
    dgate_low = gelu_back(dhid * upper)[0].astype(half_type)
    dup_low = (dhid * gelu_gate).astype(half_type)
    grad_wg = jnp.dot(low_two.T, dgate_low, preferred_element_type=single)
    grad_wu = jnp.dot(low_two.T, dup_low, preferred_element_type=single)
    dnorm_two = jnp.dot(dgate_low, wg_low.T, preferred_element_type=single) + jnp.dot(dup_low, wu_low.T, preferred_element_type=single)
    dmid_norm, terms_two = rms_backward(dnorm_two, normed_two, inv_two, scale_two)
    grad_s2 = lax.optimization_barrier(jnp.sum(terms_two, axis=0))
    dmid = cotangent + dmid_norm
    dmid_low = dmid.astype(half_type)
    grad_wo = jnp.dot(att_flat.T, dmid_low, preferred_element_type=single)
    datt_low = jnp.dot(dmid_low, wo_low.T, preferred_element_type=single).astype(half_type).reshape(length, HEADS, HD)
    delta = lax.optimization_barrier(jnp.sum(datt_low.astype(single) * att_low.astype(single), axis=-1))
    dprob = jnp.einsum('ihd,jd->hij', datt_low.astype(single), value_low.astype(single))
    dscore_low = (prob * (dprob - delta.T[:, :, None])).astype(half_type)
    dquery = jnp.einsum('hij,jd->ihd', dscore_low.astype(single), key_low.astype(single))
    dkey = jnp.einsum('hij,ihd->jd', dscore_low.astype(single), query_low.astype(single))
    dvalue = jnp.einsum('hij,ihd->jd', prob_low.astype(single), datt_low.astype(single))
    dquery_low = (unrotate(dquery, cosine[:, None, :], sine[:, None, :]) * HD ** (-0.5)).astype(half_type).reshape(length, HEADS * HD)
    dkeyval_low = jnp.concatenate([unrotate(dkey, cosine, sine), dvalue], axis=-1).astype(half_type)
    grad_wq = jnp.dot(low_one.T, dquery_low, preferred_element_type=single)
    grad_wkv = jnp.dot(low_one.T, dkeyval_low, preferred_element_type=single)
    dnorm_one = jnp.dot(dquery_low, wq_low.T, preferred_element_type=single) + jnp.dot(dkeyval_low, wkv_low.T, preferred_element_type=single)
    dinput_norm, terms_one = rms_backward(dnorm_one, normed_one, inv_one, scale_one)
    grad_s1 = lax.optimization_barrier(jnp.sum(terms_one, axis=0))
    input_grad = dmid + dinput_norm
    grads = (grad_s1, grad_wq, grad_wkv, grad_wo, grad_s2, grad_wg, grad_wu, grad_wd)
    new_carry = tuple((left + right for left, right in zip(carry, grads)))
    return (new_carry, (output, input_grad))

def reference(hidden_in, cotangent, segment_ids, positions, attn_scale, query_weight, keyval_weight, output_weight, mlp_scale, gate_weight, up_weight, down_weight, first_attn_scale, first_query_weight, first_keyval_weight, first_output_weight, first_mlp_scale, first_gate_weight, first_up_weight, first_down_weight, second_attn_scale, second_query_weight, second_keyval_weight, second_output_weight, second_mlp_scale, second_gate_weight, second_up_weight, second_down_weight):
    scale_one = lax.optimization_barrier(attn_scale.astype(jnp.bfloat16)).astype(jnp.float32)
    scale_two = lax.optimization_barrier(mlp_scale.astype(jnp.bfloat16)).astype(jnp.float32)
    weights = (scale_one, query_weight.astype(jnp.bfloat16), keyval_weight.astype(jnp.bfloat16), output_weight.astype(jnp.bfloat16), scale_two, gate_weight.astype(jnp.bfloat16), up_weight.astype(jnp.bfloat16), down_weight.astype(jnp.bfloat16))
    masters = (attn_scale, query_weight, keyval_weight, output_weight, mlp_scale, gate_weight, up_weight, down_weight)
    firsts = (first_attn_scale, first_query_weight, first_keyval_weight, first_output_weight, first_mlp_scale, first_gate_weight, first_up_weight, first_down_weight)
    seconds = (second_attn_scale, second_query_weight, second_keyval_weight, second_output_weight, second_mlp_scale, second_gate_weight, second_up_weight, second_down_weight)
    zeros = tuple((jnp.zeros(weight.shape, jnp.float32) for weight in masters))

    def one_sequence(carry, inputs):
        return sequence_pass(carry, inputs, weights)
    grads, (block_output, input_grad) = lax.scan(one_sequence, zeros, (hidden_in, cotangent, segment_ids, positions))
    results = [adamw(weight, grad, first, second) for weight, grad, first, second in zip(masters, grads, firsts, seconds)]
    return (block_output, input_grad, grads[0], grads[1], grads[2], grads[3], grads[4], grads[5], grads[6], grads[7], results[0][0], results[1][0], results[2][0], results[3][0], results[4][0], results[5][0], results[6][0], results[7][0], results[0][1], results[1][1], results[2][1], results[3][1], results[4][1], results[5][1], results[6][1], results[7][1], results[0][2], results[1][2], results[2][2], results[3][2], results[4][2], results[5][2], results[6][2], results[7][2])
```

```python
import jax
import jax.numpy as jnp
from jax import lax
from jax.sharding import PartitionSpec as P

HD = 256


norm_eps = 1e-06
beta_one = 0.9
beta_two = 0.999
adam_eps = 1e-08
learn_rate = 0.03
decay_rate = 0.1
adam_step = 4.0
rope_base = 10000.0
masked_value = -1e30

single = jnp.float32
half_type = jnp.bfloat16


def gelu_tanh(values):
    return jax.nn.gelu(values, approximate=True)


def rope_tables(positions):
    half = HD // 2
    freq = rope_base ** (-2.0 * jnp.arange(half).astype(jnp.float32) / HD)
    angle = positions.astype(jnp.float32)[..., None] * freq
    return (jnp.cos(angle), jnp.sin(angle))


def rotate(values, cosine, sine):
    half = values.shape[-1] // 2
    first = values[..., :half]
    second = values[..., half:]
    return jnp.concatenate(
        [first * cosine - second * sine, second * cosine + first * sine], axis=-1
    )


def unrotate(values, cosine, sine):
    half = values.shape[-1] // 2
    first = values[..., :half]
    second = values[..., half:]
    return jnp.concatenate(
        [first * cosine + second * sine, second * cosine - first * sine], axis=-1
    )


def rms_forward(values, scale):
    inverse = lax.rsqrt(jnp.mean(values * values, axis=-1, keepdims=True) + norm_eps)
    normed = values * inverse
    return (normed, inverse, (normed * (1.0 + scale)).astype(jnp.bfloat16))


def rms_backward(dnorm, normed, inverse, scale):
    dnormed = dnorm * (1.0 + scale)
    dvalues = inverse * (dnormed - normed * jnp.mean(dnormed * normed, axis=-1, keepdims=True))
    return (dvalues, dnorm * normed)


def adamw(weight, grad, first, second):
    first_new = beta_one * first + (1.0 - beta_one) * grad
    second_new = beta_two * second + (1.0 - beta_two) * grad * grad
    fix_one = 1.0 - beta_one**adam_step
    fix_two = 1.0 - beta_two**adam_step
    update = first_new / fix_one / (jnp.sqrt(second_new / fix_two) + adam_eps)
    return (weight - learn_rate * (update + decay_rate * weight), first_new, second_new)


def dot(a, b, dims):
    return lax.dot_general(a, b, (dims, ((), ())), preferred_element_type=single)


def small_gather(attn_scale, mlp_scale, segment_ids):
    scales = jnp.stack([attn_scale, mlp_scale]).astype(half_type)
    scales = lax.all_gather(scales, ("fsdp", "context"), axis=1, tiled=True).astype(single)
    seg_all = lax.all_gather(segment_ids, "context", axis=1, tiled=True)
    return scales[0], scales[1], seg_all


def gather_rows(block):
    return lax.all_gather(block, ("fsdp", "context"), axis=0, tiled=True)


def prepare_slice(block):
    rows, columns = block.shape
    ctx = lax.axis_size("context")
    parts = block.reshape(rows, ctx, columns // ctx).transpose(1, 0, 2)
    parts = lax.all_to_all(parts, "context", split_axis=0, concat_axis=0, tiled=True)
    full = lax.all_gather(parts, "fsdp", axis=0, tiled=True)
    return full.reshape(-1, columns // ctx)


def gather_tokens(block):
    return lax.all_gather(block, ("context", "tensor"), axis=0, tiled=True)


def scatter_tokens(part):
    return lax.psum_scatter(
        part.astype(half_type), ("context", "tensor"), scatter_dimension=0, tiled=True
    ).astype(single)


def scatter_rows(part):
    return lax.psum_scatter(
        part.astype(half_type), ("fsdp", "context"), scatter_dimension=0, tiled=True
    ).astype(single)


def return_slice(part):
    full, columns = part.shape
    ctx = lax.axis_size("context")
    fs = lax.axis_size("fsdp")
    rows = full // (ctx * fs)
    parts = part.astype(half_type).reshape(fs * ctx, rows, columns)
    parts = lax.psum_scatter(parts, "fsdp", scatter_dimension=0, tiled=True)
    parts = lax.all_to_all(parts, "context", split_axis=0, concat_axis=0, tiled=True)
    return parts.transpose(1, 0, 2).reshape(rows, ctx * columns).astype(single)


def on_device(
    hidden_in,
    cotangent,
    segment_ids,
    positions,
    attn_scale,
    query_weight,
    keyval_weight,
    output_weight,
    mlp_scale,
    gate_weight,
    up_weight,
    down_weight,
    first_attn_scale,
    first_query_weight,
    first_keyval_weight,
    first_output_weight,
    first_mlp_scale,
    first_gate_weight,
    first_up_weight,
    first_down_weight,
    second_attn_scale,
    second_query_weight,
    second_keyval_weight,
    second_output_weight,
    second_mlp_scale,
    second_gate_weight,
    second_up_weight,
    second_down_weight,
):
    ten = lax.axis_size("tensor")
    x = lax.axis_index("tensor")
    context_index = lax.axis_index("context")
    block, width = hidden_in.shape[1:]
    half_rows = block // ten
    heads_here = query_weight.shape[1] // HD
    heads_width = heads_here * HD
    hidden = hidden_in[0]
    cot = cotangent[0]
    hidden_half = lax.dynamic_slice_in_dim(hidden, x * half_rows, half_rows, 0)
    cot_half = lax.dynamic_slice_in_dim(cot, x * half_rows, half_rows, 0)

    scale_one, scale_two, seg_all = small_gather(attn_scale, mlp_scale, segment_ids)
    query_full = gather_rows(query_weight.astype(half_type))
    keyval_full = gather_rows(keyval_weight.astype(half_type))
    output_full = gather_rows(output_weight.astype(half_type).T)
    gate_slice = prepare_slice(gate_weight.astype(half_type))
    up_slice = prepare_slice(up_weight.astype(half_type))
    down_slice = prepare_slice(down_weight.astype(half_type).T)
    dy_all = gather_tokens(cot_half.astype(half_type))

    normed_one, inv_one, low_one = rms_forward(hidden, scale_one)
    query = dot(low_one, query_full, ((1,), (0,))).reshape(block, heads_here, HD)
    keyval = dot(low_one, keyval_full, ((1,), (0,)))
    cosine, sine = rope_tables(positions[0])
    query_low = (rotate(query, cosine[:, None, :], sine[:, None, :]) * HD ** (-0.5)).astype(
        half_type
    )
    key_low = rotate(keyval[:, :HD], cosine, sine).astype(half_type)
    keyval_low = jnp.concatenate([key_low, keyval[:, HD:].astype(half_type)], axis=-1)
    keyval_all = lax.all_gather(keyval_low, "context", axis=0, tiled=True)
    keys_all = keyval_all[:, :HD]
    values_all = keyval_all[:, HD:]
    rows_index = context_index * block + jnp.arange(block, dtype=jnp.int32)
    cols_index = jnp.arange(keys_all.shape[0], dtype=jnp.int32)
    allowed = (rows_index[:, None] >= cols_index[None, :]) & (
        segment_ids[0][:, None] == seg_all[0][None, :]
    )
    scores = jnp.einsum("bhd,jd->hbj", query_low, keys_all, preferred_element_type=single)
    masked = jnp.where(allowed, scores, masked_value)
    top = jnp.max(masked, axis=-1, keepdims=True)
    total = jnp.sum(jnp.where(allowed, jnp.exp(masked - top), 0.0), axis=-1, keepdims=True)
    lse = top + jnp.log(total)
    prob = jnp.where(allowed, jnp.exp(masked - lse), 0.0)
    prob_low = prob.astype(half_type)
    att_low = jnp.einsum(
        "hbj,jd->bhd", prob_low, values_all, preferred_element_type=single
    ).astype(half_type)
    att_flat = att_low.reshape(block, heads_width)
    attn_part = dot(att_flat, output_full, ((1,), (1,)))
    attn_half = lax.psum_scatter(
        attn_part.astype(half_type), "tensor", scatter_dimension=0, tiled=True
    )
    mid_half = hidden_half + attn_half.astype(single)

    normed_two, inv_two, low_two = rms_forward(mid_half, scale_two)
    low_all = gather_tokens(low_two)
    gate = dot(low_all, gate_slice, ((1,), (0,)))
    upper = dot(low_all, up_slice, ((1,), (0,)))
    dhid = dot(dy_all, down_slice, ((1,), (0,)))
    gelu_gate, gelu_back = jax.vjp(gelu_tanh, gate)
    hid_low = (gelu_gate * upper).astype(half_type)
    dgate_low = gelu_back(dhid * upper)[0].astype(half_type)
    dup_low = (dhid * gelu_gate).astype(half_type)
    dnorm_two = scatter_tokens(
        dot(dgate_low, gate_slice, ((1,), (1,))) + dot(dup_low, up_slice, ((1,), (1,)))
    )
    mlp_half = scatter_tokens(dot(hid_low, down_slice, ((1,), (1,))))
    grad_wd = return_slice(dot(dy_all, hid_low, ((0,), (0,)))).T
    grad_wg = return_slice(dot(low_all, dgate_low, ((0,), (0,))))
    grad_wu = return_slice(dot(low_all, dup_low, ((0,), (0,))))
    dmid_norm, terms_two = rms_backward(dnorm_two, normed_two, inv_two, scale_two)
    dmid_half = cot_half + dmid_norm

    dmid_low = lax.all_gather(dmid_half.astype(half_type), "tensor", axis=0, tiled=True)
    grad_out_full = dot(dmid_low, att_flat, ((0,), (0,)))
    datt_low = (
        dot(dmid_low, output_full, ((1,), (0,))).astype(half_type).reshape(block, heads_here, HD)
    )
    delta = jnp.einsum("bhd,bhd->hb", datt_low, att_low, preferred_element_type=single)
    dprob = jnp.einsum("bhd,jd->hbj", datt_low, values_all, preferred_element_type=single)
    dscore_low = (prob * (dprob - delta[..., None])).astype(half_type)
    dquery = jnp.einsum("hbj,jd->bhd", dscore_low, keys_all, preferred_element_type=single)
    dkey_part = jnp.einsum("hbj,bhd->jd", dscore_low, query_low, preferred_element_type=single)
    dvalue_part = jnp.einsum("hbj,bhd->jd", prob_low, datt_low, preferred_element_type=single)
    dkeyval_own = lax.psum_scatter(
        jnp.concatenate([dkey_part, dvalue_part], axis=-1).astype(half_type),
        "context",
        scatter_dimension=0,
        tiled=True,
    )
    dkeyval_sum = lax.psum(dkeyval_own.astype(single), "tensor")
    dquery_low = (
        (unrotate(dquery, cosine[:, None, :], sine[:, None, :]) * HD ** (-0.5))
        .astype(half_type)
        .reshape(block, heads_width)
    )
    dnorm_query = dot(dquery_low, query_full, ((1,), (1,)))
    dnorm_query = lax.psum_scatter(
        dnorm_query.astype(half_type), "tensor", scatter_dimension=0, tiled=True
    ).astype(single)
    dkeyval_low = jnp.concatenate(
        [unrotate(dkeyval_sum[:, :HD], cosine, sine), dkeyval_sum[:, HD:]], axis=-1
    ).astype(half_type)
    dkeyval_half = lax.dynamic_slice_in_dim(dkeyval_low, x * half_rows, half_rows, 0)
    dnorm_one = dnorm_query + dot(dkeyval_half, keyval_full, ((1,), (1,)))
    normed_half = lax.dynamic_slice_in_dim(normed_one, x * half_rows, half_rows, 0)
    inv_half = lax.dynamic_slice_in_dim(inv_one, x * half_rows, half_rows, 0)
    dinput_norm, terms_one = rms_backward(dnorm_one, normed_half, inv_half, scale_one)
    grad_query_full = dot(low_one, dquery_low, ((0,), (0,)))
    grad_keyval_full = dot(low_one, dkeyval_low, ((0,), (0,)))
    grad_wq = scatter_rows(grad_query_full)
    grad_wkv = scatter_rows(grad_keyval_full)
    grad_wo = scatter_rows(grad_out_full).T
    terms = jnp.stack([jnp.sum(terms_one, axis=0), jnp.sum(terms_two, axis=0)])
    terms = lax.psum_scatter(terms, ("fsdp", "context"), scatter_dimension=1, tiled=True)
    terms = lax.psum(terms, "tensor")
    grad_s1, grad_s2 = terms[0], terms[1]
    outs = jnp.stack([mid_half + mlp_half, dmid_half + dinput_norm])
    outs = lax.all_gather(outs, "tensor", axis=1, tiled=True)

    masters = (
        attn_scale,
        query_weight,
        keyval_weight,
        output_weight,
        mlp_scale,
        gate_weight,
        up_weight,
        down_weight,
    )
    grads = (grad_s1, grad_wq, grad_wkv, grad_wo, grad_s2, grad_wg, grad_wu, grad_wd)
    firsts = (
        first_attn_scale,
        first_query_weight,
        first_keyval_weight,
        first_output_weight,
        first_mlp_scale,
        first_gate_weight,
        first_up_weight,
        first_down_weight,
    )
    seconds = (
        second_attn_scale,
        second_query_weight,
        second_keyval_weight,
        second_output_weight,
        second_mlp_scale,
        second_gate_weight,
        second_up_weight,
        second_down_weight,
    )
    results = [
        adamw(weight, grad, first, second)
        for weight, grad, first, second in zip(masters, grads, firsts, seconds)
    ]
    return (
        outs[0][None],
        outs[1][None],
        *grads,
        *(entry[0] for entry in results),
        *(entry[1] for entry in results),
        *(entry[2] for entry in results),
    )


def solution(mesh):
    both = ("fsdp", "context")
    tokens = P("fsdp", "context", None)
    weights = (
        P(both),
        P(both, "tensor"),
        P(both, None),
        P("tensor", both),
        P(both),
        P(both, "tensor"),
        P(both, "tensor"),
        P("tensor", both),
    )
    return jax.shard_map(
        on_device,
        mesh=mesh,
        in_specs=(tokens, tokens, P("fsdp", "context"), P("fsdp", "context"), *(weights * 3)),
        out_specs=(tokens, tokens, *(weights * 4)),
        check_vma=False,
    )
```

```python
import functools

import jax
import jax.numpy as jnp
from jax import lax
from jax.experimental import pallas as pl
from jax.experimental.pallas import tpu as pltpu
from jax.sharding import PartitionSpec as P

HD = 256


norm_eps = 1e-06
beta_one = 0.9
beta_two = 0.999
adam_eps = 1e-08
learn_rate = 0.03
decay_rate = 0.1
adam_step = 4.0
rope_base = 10000.0
masked_value = -1e30

single = jnp.float32
half_type = jnp.bfloat16


def gelu_tanh(values):
    return jax.nn.gelu(values, approximate=True)


def rope_tables(positions):
    half = HD // 2
    freq = rope_base ** (-2.0 * jnp.arange(half).astype(jnp.float32) / HD)
    angle = positions.astype(jnp.float32)[..., None] * freq
    return (jnp.cos(angle), jnp.sin(angle))


def rotate(values, cosine, sine):
    half = values.shape[-1] // 2
    first = values[..., :half]
    second = values[..., half:]
    return jnp.concatenate(
        [first * cosine - second * sine, second * cosine + first * sine], axis=-1
    )


def unrotate(values, cosine, sine):
    half = values.shape[-1] // 2
    first = values[..., :half]
    second = values[..., half:]
    return jnp.concatenate(
        [first * cosine + second * sine, second * cosine - first * sine], axis=-1
    )


def rms_forward(values, scale):
    inverse = lax.rsqrt(jnp.mean(values * values, axis=-1, keepdims=True) + norm_eps)
    normed = values * inverse
    return (normed, inverse, (normed * (1.0 + scale)).astype(jnp.bfloat16))


def rms_backward(dnorm, normed, inverse, scale):
    dnormed = dnorm * (1.0 + scale)
    dvalues = inverse * (dnormed - normed * jnp.mean(dnormed * normed, axis=-1, keepdims=True))
    return (dvalues, dnorm * normed)


def adamw(weight, grad, first, second):
    first_new = beta_one * first + (1.0 - beta_one) * grad
    second_new = beta_two * second + (1.0 - beta_two) * grad * grad
    fix_one = 1.0 - beta_one**adam_step
    fix_two = 1.0 - beta_two**adam_step
    update = first_new / fix_one / (jnp.sqrt(second_new / fix_two) + adam_eps)
    return (weight - learn_rate * (update + decay_rate * weight), first_new, second_new)


def dot(a, b, dims):
    return lax.dot_general(a, b, (dims, ((), ())), preferred_element_type=single)


MESH = pl.DeviceIdType.MESH
ANY = pl.BlockSpec(memory_space=pl.ANY)
VMEM = pl.BlockSpec(memory_space=pltpu.VMEM)


def greet(peers):
    barrier = pltpu.get_barrier_semaphore()
    for peer in peers:
        pl.semaphore_signal(barrier, inc=1, device_id=peer, device_id_type=MESH)
    pl.semaphore_wait(barrier, len(peers))


def remote(src, dst, send, recv, peer):
    return pltpu.make_async_remote_copy(
        src_ref=src, dst_ref=dst, send_sem=send, recv_sem=recv, device_id=peer, device_id_type=MESH
    )


def arrived(dst, recv, peer):
    remote(dst, dst, recv, recv, peer).wait_recv()


def fsdp_place(fs):
    f = lax.axis_index("fsdp")
    core = lax.rem(f, 2)
    y = lax.div(f, 2)
    twin = {"fsdp": f + 1 - 2 * core}
    across = [{"fsdp": lax.rem(y + d, fs // 2) * 2 + core} for d in range(1, fs // 2)]
    return f, y, core, twin, across


class Sends:
    def __init__(self, send):
        self.send, self.made = send, []

    def push(self, src, dst, recv, peer, *conditions):
        copy = remote(src, dst, self.send.at[len(self.made)], recv, peer)
        self.made.append((copy, conditions))
        under(conditions, copy.start)

    def drain(self):
        for copy, conditions in self.made:
            under(conditions, copy.wait_send)


def under(conditions, action):
    if not conditions:
        action()
        return
    holds = conditions[0]
    for more in conditions[1:]:
        holds = jnp.logical_and(holds, more)
    pl.when(holds)(action)


def line_steps(z, ctx):
    for s in range(1, ctx):
        yield z - s, z >= s, z + 1, z + 1 < ctx
        yield z + s, z + s < ctx, z - 1, z >= 1


def tokens_kernel(ctx, ten, src, out, local, send, recv):
    z, x = lax.axis_index("context"), lax.axis_index("tensor")
    around = [lax.rem(z + d, ctx) for d in range(ctx)]
    across = [{"tensor": lax.rem(x + d, ten)} for d in range(1, ten)]
    greet([{"context": k} for k in around[1:]] + across)
    sends = []

    def push(ref, source, peer):
        copy = remote(ref, out.at[source, x], send.at[len(sends)], recv.at[source, x], peer)
        copy.start()
        sends.append(copy)

    for d in range(1, ctx):
        push(src, z, {"context": around[d]})
    for peer in across:
        push(src, z, peer)
    keep = pltpu.make_async_copy(src, out.at[z, x], local)
    keep.start()
    back = [lax.rem(z + ctx - d, ctx) for d in range(ctx)]
    for d in range(1, ctx):
        arrived(out.at[back[d], x], recv.at[back[d], x], {"context": back[d]})
        for peer in across:
            push(out.at[back[d], x], back[d], peer)
    for d in range(ctx):
        for peer in across:
            other = peer["tensor"]
            arrived(out.at[back[d], other], recv.at[back[d], other], peer)
    keep.wait()
    for copy in sends:
        copy.wait_send()


def tokens_to_all(block, ctx, ten, ident):
    sends = (ctx - 1) + ctx * (ten - 1)
    out = pl.pallas_call(
        functools.partial(tokens_kernel, ctx, ten),
        out_shape=jax.ShapeDtypeStruct((ctx, ten, *block.shape), block.dtype),
        in_specs=[VMEM],
        out_specs=VMEM,
        scratch_shapes=[
            pltpu.SemaphoreType.DMA(()),
            pltpu.SemaphoreType.DMA((sends,)),
            pltpu.SemaphoreType.DMA((ctx, ten)),
        ],
        compiler_params=pltpu.CompilerParams(collective_id=ident, has_side_effects=True),
        name=f"tokens_{ident}",
    )(block)
    return out.reshape(-1, block.shape[-1])


def sum_tokens_kernel(ctx, ten, src, out, first, mine, second, send, recv_x, recv_z):
    z, x = lax.axis_index("context"), lax.axis_index("tensor")
    around = [lax.rem(z + d, ctx) for d in range(ctx)]
    across = [lax.rem(x + d, ten) for d in range(1, ten)]
    greet([{"context": k} for k in around[1:]] + [{"tensor": k} for k in across])
    sends = []
    order = around[1:] + around[:1]
    for owner in order:
        for k, other in enumerate(across):
            copy = remote(
                src.at[owner, other],
                first.at[k, owner],
                send.at[len(sends)],
                recv_x.at[k, owner],
                {"tensor": other},
            )
            copy.start()
            sends.append(copy)
    for d, owner in enumerate(order):
        total = src[owner, x].astype(single)
        for k, other in enumerate(across):
            arrived(first.at[k, owner], recv_x.at[k, owner], {"tensor": other})
            total = total + first[k, owner].astype(single)
        if d < ctx - 1:
            mine[d] = total.astype(half_type)
            copy = remote(
                mine.at[d],
                second.at[d],
                send.at[len(sends)],
                recv_z.at[d],
                {"context": owner},
            )
            copy.start()
            sends.append(copy)
        else:
            for e in range(ctx - 1):
                arrived(second.at[e], recv_z.at[e], {"context": around[1]})
                total = total + second[e].astype(single)
            out[...] = total
    for copy in sends:
        copy.wait_send()


def sum_tokens(part, ctx, ten, ident):
    rows, columns = part.shape[0] // (ctx * ten), part.shape[1]
    sends = ctx * (ten - 1) + ctx - 1
    return pl.pallas_call(
        functools.partial(sum_tokens_kernel, ctx, ten),
        out_shape=jax.ShapeDtypeStruct((rows, columns), single),
        in_specs=[VMEM],
        out_specs=VMEM,
        scratch_shapes=[
            pltpu.VMEM((ten - 1, ctx, rows, columns), half_type),
            pltpu.VMEM((ctx - 1, rows, columns), half_type),
            pltpu.VMEM((ctx - 1, rows, columns), half_type),
            pltpu.SemaphoreType.DMA((sends,)),
            pltpu.SemaphoreType.DMA((ten - 1, ctx)),
            pltpu.SemaphoreType.DMA((ctx - 1,)),
        ],
        compiler_params=pltpu.CompilerParams(collective_id=ident, has_side_effects=True),
        name=f"sum_tokens_{ident}",
    )(part.reshape(ctx, ten, rows, columns))


def swap_kernel(ten, src, out, local, send, recv):
    x = lax.axis_index("tensor")
    beside = [lax.rem(x + d, ten) for d in range(1, ten)]
    greet([{"tensor": k} for k in beside])
    out_sends = Sends(send)
    for other in beside:
        out_sends.push(src.at[other], out.at[x], recv.at[x], {"tensor": other})
    keep = pltpu.make_async_copy(src.at[x], out.at[x], local)
    keep.start()
    for other in beside:
        arrived(out.at[other], recv.at[other], {"tensor": other})
    keep.wait()
    out_sends.drain()


def swap(blocks, ten, ident):
    return pl.pallas_call(
        functools.partial(swap_kernel, ten),
        out_shape=jax.ShapeDtypeStruct(blocks.shape, blocks.dtype),
        in_specs=[VMEM],
        out_specs=VMEM,
        scratch_shapes=[
            pltpu.SemaphoreType.DMA(()),
            pltpu.SemaphoreType.DMA((ten - 1,)),
            pltpu.SemaphoreType.DMA((ten,)),
        ],
        compiler_params=pltpu.CompilerParams(collective_id=ident, has_side_effects=True),
        name=f"swap_{ident}",
    )(blocks)


VMEM_ALL = 67043328


def cast(v):
    return v.astype(half_type)


def spread_kernel(fs, ctx, ten, count, split, *refs):
    srcs, outs = refs[: count + 1], refs[count + 1 : 2 * count + 2]
    local, send, recv, recv_t = refs[2 * count + 2 :]
    f, y, core, twin, across = fsdp_place(fs)
    z, x = lax.axis_index("context"), lax.axis_index("tensor")
    beside = [{"tensor": lax.rem(x + d, ten)} for d in range(1, ten)]
    around = [lax.rem(z + d, ctx) for d in range(ctx)]
    back = [lax.rem(z + ctx - d, ctx) for d in range(ctx)]
    up, down = {"context": z + 1}, {"context": z - 1}
    greet([{"context": k} for k in around[1:]] + across + [twin] + beside)
    out = Sends(send)
    keeps = []
    order = [count] + list(range(count))

    def where(w, source):
        if w == count:
            return outs[w].at[source, x], recv_t.at[source, x], beside
        return outs[w].at[f, source], recv.at[w, f, source], across + [twin]

    for w in order:
        mine, sem, peers = where(w, z)
        if w < count and split[w]:
            for d in range(1, ctx):
                out.push(srcs[w].at[around[d]], mine, sem, {"context": around[d]})
            src = srcs[w].at[z]
        else:
            src = srcs[w]
            out.push(src, mine, sem, up, z + 1 < ctx)
            out.push(src, mine, sem, down, z >= 1)
        for peer in peers:
            out.push(src, mine, sem, peer)
        keeps.append(pltpu.make_async_copy(src, mine, local.at[w]))
        keeps[-1].start()
    for step, (source, exists, onward, more) in enumerate(line_steps(z, ctx)):
        for w in order:
            if w < count and split[w]:
                if step % 2:
                    continue
                block, sem, peers = where(w, back[step // 2 + 1])
                arrived(block, sem, twin)
                for peer in peers:
                    out.push(block, block, sem, peer)
                continue
            block, sem, peers = where(w, source)
            under((exists,), lambda: arrived(block, sem, twin))
            out.push(block, block, sem, {"context": onward}, exists, more)
            for peer in peers:
                out.push(block, block, sem, peer, exists)
    chain = [(z, ())] + [(source, (exists,)) for source, exists, _, _ in line_steps(z, ctx)]
    ring = [(source, ()) for source in back]
    for w in range(count):
        for source, when in ring if split[w] else chain:
            for peer in across:
                owner = peer["fsdp"]
                block, sem = outs[w].at[owner, source], recv.at[w, owner, source]
                under(when, lambda: arrived(block, sem, twin))
                out.push(block, block, sem, twin, *when)
    for source in back:
        for w in range(count):
            for step in range(fs // 2):
                owner = lax.rem(y + step, fs // 2) * 2 + 1 - core
                arrived(outs[w].at[owner, source], recv.at[w, owner, source], twin)
        for peer in beside:
            arrived(outs[count].at[source, peer["tensor"]], recv_t.at[source, peer["tensor"]], twin)
    for keep in keeps:
        keep.wait()
    out.drain()


def spread(blocks, split, tokens, fs, ctx, ten, ident):
    count = len(blocks)
    chips = fs // 2
    lines = 2 + 2 * (ctx - 1)
    sends = count * (lines + (2 * ctx - 1) * (2 * chips - 1)) + lines + (2 * ctx - 1) * (ten - 1)
    shapes = [b.shape[1:] if s else b.shape for b, s in zip(blocks, split)]
    return pl.pallas_call(
        functools.partial(spread_kernel, fs, ctx, ten, count, split),
        out_shape=[jax.ShapeDtypeStruct((fs, ctx, *s), b.dtype) for s, b in zip(shapes, blocks)]
        + [jax.ShapeDtypeStruct((ctx, ten, *tokens.shape), tokens.dtype)],
        in_specs=[ANY] * (count + 1),
        out_specs=[ANY] * (count + 1),
        scratch_shapes=[
            pltpu.SemaphoreType.DMA((count + 1,)),
            pltpu.SemaphoreType.DMA((sends,)),
            pltpu.SemaphoreType.DMA((count, fs, ctx)),
            pltpu.SemaphoreType.DMA((ctx, ten)),
        ],
        compiler_params=pltpu.CompilerParams(collective_id=ident, has_side_effects=True),
        name=f"spread_{ident}",
    )(*blocks, tokens)


def fill_product(dw, left, right, owner, ctx):
    def one(k, carry):
        dw[owner, k] = cast(
            lax.dot_general(
                left[owner, k], right[...], (((1,), (0,)), ((), ())), preferred_element_type=single
            )
        )
        return carry

    lax.fori_loop(0, ctx, one, 0)


def back_kernel(
    fs, ctx, ten, low_t, dy_t, hid, dgate, dup, dnorm, mlp, dnorm_out, mlp_out, down, gate, up, *refs
):
    dws, nears, fars = refs[0:3], refs[3:6], refs[6:9]
    firsts, mines, seconds = refs[9:11], refs[11:13], refs[13:15]
    local, send, recv_c, recv_y, recv_z, recv_tx, recv_tz = refs[15:]
    f, y, core, twin, across = fsdp_place(fs)
    z, x = lax.axis_index("context"), lax.axis_index("tensor")
    chips = fs // 2
    around = [lax.rem(z + d, ctx) for d in range(ctx)]
    beside = [lax.rem(x + d, ten) for d in range(1, ten)]
    rows_of = [lax.rem(y + d, chips) for d in range(chips)]
    chip_order = rows_of[1:] + rows_of[:1]
    order = around[1:] + around[:1]
    greet([{"context": k} for k in around[1:]] + across + [twin] + [{"tensor": k} for k in beside])
    out = Sends(send)
    outs = (down, gate, up)
    sources = (dnorm, mlp)
    results = (dnorm_out, mlp_out)

    def token_start(t):
        for owner in order:
            for k, other in enumerate(beside):
                out.push(
                    sources[t].at[owner, other],
                    firsts[t].at[k, owner],
                    recv_tx.at[t, k, owner],
                    {"tensor": other},
                )

    def token_pass(t):
        for d, owner in enumerate(order):
            total = sources[t][owner, x].astype(single)
            for k, other in enumerate(beside):
                arrived(firsts[t].at[k, owner], recv_tx.at[t, k, owner], twin)
                total = total + firsts[t][k, owner].astype(single)
            if d < ctx - 1:
                mines[t][d] = cast(total)
                out.push(mines[t].at[d], seconds[t].at[d], recv_tz.at[t, d], {"context": owner})
            else:
                results[t][...] = total

    def token_end(t):
        total = results[t][...]
        for e in range(ctx - 1):
            arrived(seconds[t].at[e], recv_tz.at[t, e], twin)
            total = total + seconds[t][e].astype(single)
        results[t][...] = total

    def products(w):
        left, right = (dy_t, low_t, low_t)[w], (hid, dgate, dup)[w]
        for row in chip_order:
            fill_product(dws[w], left, right, row * 2 + 1 - core, ctx)
            out.push(dws[w].at[row * 2 + 1 - core], nears[w].at[row], recv_c.at[w, row], twin)
        for row in chip_order:
            fill_product(dws[w], left, right, row * 2 + core, ctx)

    def over_chips(w):
        for k, row in enumerate(rows_of[1:]):
            arrived(nears[w].at[row], recv_c.at[w, row], twin)
            for d, owner in enumerate(order):
                mine = dws[w].at[row * 2 + core, owner]
                mine[...] = cast(mine[...].astype(single) + nears[w][row, owner].astype(single))
                out.push(mine, fars[w].at[k, d], recv_y.at[w, k, d], across[k])

    def over_context(w):
        arrived(nears[w].at[y], recv_c.at[w, y], twin)
        for d, owner in enumerate(order):
            mine = dws[w].at[f, owner]
            total = mine[...].astype(single) + nears[w][y, owner].astype(single)
            for k in range(chips - 1):
                arrived(fars[w].at[k, d], recv_y.at[w, k, d], twin)
                total = total + fars[w][k, d].astype(single)
            mine[...] = cast(total)
            if d < ctx - 1:
                out.push(mine, outs[w].at[z], recv_z.at[w, z], {"context": owner})
            else:
                keep = pltpu.make_async_copy(mine, outs[w].at[z], local.at[w])
                keep.start()
                keeps.append(keep)

    keeps = []
    token_start(0)
    products(0)
    token_start(1)
    over_chips(0)
    products(1)
    over_chips(1)
    token_pass(0)
    over_context(0)
    products(2)
    over_chips(2)
    token_pass(1)
    over_context(1)
    over_context(2)
    token_end(0)
    token_end(1)
    for w in range(3):
        for k in around[1:]:
            arrived(outs[w].at[k], recv_z.at[w, k], twin)
    for keep in keeps:
        keep.wait()
    out.drain()


def mlp_back(low_t, dy_t, hid, dgate, dup, dnorm, mlp, fs, ctx, ten, ident):
    rows, columns = low_t.shape[2], hid.shape[1]
    t_rows, width = dnorm.shape[2:]
    chips = fs // 2
    block = (rows, columns)
    sends = 2 * (ctx * (ten - 1) + ctx - 1) + 3 * (chips + (chips - 1) * ctx + ctx - 1)
    dma = pltpu.SemaphoreType.DMA
    return pl.pallas_call(
        functools.partial(back_kernel, fs, ctx, ten),
        out_shape=[jax.ShapeDtypeStruct((t_rows, width), single)] * 2
        + [jax.ShapeDtypeStruct((ctx, *block), half_type)] * 3,
        in_specs=[VMEM] * 7,
        out_specs=[VMEM] * 2 + [ANY] * 3,
        scratch_shapes=[pltpu.VMEM((fs, ctx, *block), half_type)] * 3
        + [pltpu.VMEM((chips, ctx, *block), half_type)] * 3
        + [pltpu.VMEM((chips - 1, ctx, *block), half_type)] * 3
        + [pltpu.VMEM((ten - 1, ctx, t_rows, width), half_type)] * 2
        + [pltpu.VMEM((ctx - 1, t_rows, width), half_type)] * 4
        + [
            dma((3,)),
            dma((sends,)),
            dma((3, chips)),
            dma((3, chips - 1, ctx)),
            dma((3, ctx)),
            dma((2, ten - 1, ctx)),
            dma((2, ctx - 1)),
        ],
        compiler_params=pltpu.CompilerParams(
            collective_id=ident, has_side_effects=True, vmem_limit_bytes=VMEM_ALL
        ),
        name=f"mlp_back_{ident}",
    )(low_t, dy_t, hid, dgate, dup, dnorm, mlp)


def attn_kernel(
    fs, ctx, ten, low_t, dmid_t, d_qkv, att, terms, give, qkv_out, o_out, s_out, kv_out, take_out, *refs
):
    dws, nears, fars = refs[0:3], refs[3:6], refs[6:9]
    ups, downs = refs[9:12], refs[12:15]
    tail, near_s, local, send, recv_c, recv_y, recv_u, recv_d, recv_x = refs[15:]
    dws[2][...] = terms[...]
    f, y, core, twin, across = fsdp_place(fs)
    z, x = lax.axis_index("context"), lax.axis_index("tensor")
    chips = fs // 2
    beside = [lax.rem(x + d, ten) for d in range(1, ten)]
    rows_of = [lax.rem(y + d, chips) for d in range(chips)]
    chip_order = rows_of[1:] + rows_of[:1]
    nxt, prv = lax.rem(z + 1, ctx), lax.rem(z + ctx - 1, ctx)
    greet([{"context": nxt}, {"context": prv}] + across + [twin] + [{"tensor": k} for k in beside])
    out = Sends(send)
    order = []
    for k in range((ctx + 1) // 2):
        order += [ctx - 1 - k] + ([k] if k != ctx - 1 - k else [])
    kinds = (cast, cast, lambda v: v)

    for k, other in enumerate(beside):
        out.push(give, take_out.at[x], recv_x.at[0, x], {"tensor": other})
    keep_give = pltpu.make_async_copy(give, take_out.at[x], local.at[0])
    keep_give.start()

    def start(w):
        for row in chip_order:
            owner = row * 2 + 1 - core
            if w < 2:
                fill_product(dws[w], (low_t, dmid_t)[w], (d_qkv, att)[w], owner, ctx)
            out.push(dws[w].at[owner], nears[w].at[row], recv_c.at[w, row], twin)
        if w < 2:
            for row in chip_order:
                fill_product(dws[w], (low_t, dmid_t)[w], (d_qkv, att)[w], row * 2 + core, ctx)

    def over_chips(w):
        for k, row in enumerate(rows_of[1:]):
            arrived(nears[w].at[row], recv_c.at[w, row], twin)
            for owner in order:
                mine = dws[w].at[row * 2 + core, owner]
                mine[...] = kinds[w](mine[...].astype(single) + nears[w][row, owner].astype(single))
                out.push(mine, fars[w].at[k, owner], recv_y.at[w, k, owner], across[k])

    def over_context(w):
        arrived(nears[w].at[y], recv_c.at[w, y], twin)
        for owner in order:
            mine = dws[w].at[f, owner]
            for k in range(chips - 1):
                arrived(fars[w].at[k, owner], recv_y.at[w, k, owner], twin)

            def gathered():
                total = mine[...].astype(single) + nears[w][y, owner].astype(single)
                for k in range(chips - 1):
                    total = total + fars[w][k, owner].astype(single)
                return total

            @pl.when(z == owner)
            def _():
                mine[...] = kinds[w](gathered())

            for toward, sem, slots, edge, past in (
                ({"context": z + 1}, recv_u, ups[w], z == 0, z < owner),
                ({"context": z - 1}, recv_d, downs[w], z == ctx - 1, z > owner),
            ):

                @pl.when(jnp.logical_and(past, edge))
                def _():
                    mine[...] = kinds[w](gathered())

                @pl.when(jnp.logical_and(past, jnp.logical_not(edge)))
                def _():
                    arrived(slots.at[owner], sem.at[w, owner], twin)
                    mine[...] = kinds[w](gathered() + slots[owner].astype(single))

                out.push(mine, slots.at[owner], sem.at[w, owner], toward, past)

    def finish(w, result):
        for sem, slots, edge in ((recv_u, ups[w], z == 0), (recv_d, downs[w], z == ctx - 1)):
            mine = dws[w].at[f, z]

            @pl.when(jnp.logical_not(edge))
            def _():
                arrived(slots.at[z], sem.at[w, z], twin)
                mine[...] = kinds[w](mine[...].astype(single) + slots[z].astype(single))

        result(dws[w][f, z])

    start(2)
    start(1)
    over_chips(2)
    over_chips(1)
    start(0)
    over_chips(0)
    over_context(2)
    over_context(1)
    over_context(0)

    columns = tail.shape[-1]

    def keep_o(v):
        o_out[...] = v.astype(single)

    def keep_qkv(v):
        qkv_out[...] = v[:, : qkv_out.shape[1]].astype(single)
        tail[x] = v[:, v.shape[1] - columns :]

    def keep_s(v):
        near_s[x] = v

    finish(2, keep_s)
    for other in beside:
        out.push(near_s.at[x], near_s.at[x], recv_x.at[1, x], {"tensor": other})
    finish(1, keep_o)
    finish(0, keep_qkv)
    for other in beside:
        out.push(tail.at[x], tail.at[x], recv_x.at[2, x], {"tensor": other})
    for other in beside:
        arrived(take_out.at[other], recv_x.at[0, other], twin)
        arrived(near_s.at[other], recv_x.at[1, other], twin)
        arrived(tail.at[other], recv_x.at[2, other], twin)
    total = near_s[0]
    for k in range(1, ten):
        total = total + near_s[k]
    s_out[...] = total
    for k in range(ten):
        kv_out[:, k * columns : (k + 1) * columns] = tail[k].astype(single)
    keep_give.wait()
    out.drain()


def attn_back(low_t, dmid_t, d_qkv, att, terms, give, q_columns, fs, ctx, ten, ident):
    rows = low_t.shape[2]
    chips = fs // 2
    tail = d_qkv.shape[1] - q_columns
    blocks = [(rows, d_qkv.shape[1]), (rows, att.shape[1]), terms.shape[2:]]
    kinds = [half_type, half_type, single]
    both = list(zip(blocks, kinds))
    sends = (
        3 * (ten - 1)
        + 3 * (chips + (chips - 1) * ctx + 2 * ctx)
    )
    dma = pltpu.SemaphoreType.DMA
    return pl.pallas_call(
        functools.partial(attn_kernel, fs, ctx, ten),
        out_shape=[
            jax.ShapeDtypeStruct((rows, q_columns), single),
            jax.ShapeDtypeStruct((rows, att.shape[1]), single),
            jax.ShapeDtypeStruct(terms.shape[2:], single),
            jax.ShapeDtypeStruct((rows, ten * tail), single),
            jax.ShapeDtypeStruct((ten, *give.shape), give.dtype),
        ],
        in_specs=[VMEM] * 6,
        out_specs=[VMEM] * 5,
        scratch_shapes=[pltpu.VMEM((fs, ctx, *b), t) for b, t in both]
        + [pltpu.VMEM((chips, ctx, *b), t) for b, t in both]
        + [pltpu.VMEM((chips - 1, ctx, *b), t) for b, t in both]
        + [pltpu.VMEM((ctx, *b), t) for b, t in both] * 2
        + [
            pltpu.VMEM((ten, rows, tail), half_type),
            pltpu.VMEM((ten, *terms.shape[2:]), single),
            dma((1,)),
            dma((sends,)),
            dma((3, chips)),
            dma((3, chips - 1, ctx)),
            dma((3, ctx)),
            dma((3, ctx)),
            dma((3, ten)),
        ],
        compiler_params=pltpu.CompilerParams(
            collective_id=ident, has_side_effects=True, vmem_limit_bytes=VMEM_ALL
        ),
        name=f"attn_back_{ident}",
    )(low_t, dmid_t, d_qkv, att, terms, give)


def own_columns(weight, ctx):
    rows, columns = weight.shape
    return cast(weight).reshape(rows, ctx, columns // ctx).transpose(1, 0, 2)


def on_device(hidden_in, cotangent, segment_ids, positions, *params):
    masters, firsts, seconds = params[:8], params[8:16], params[16:]
    (
        attn_scale,
        query_weight,
        keyval_weight,
        output_weight,
        mlp_scale,
        gate_weight,
        up_weight,
        down_weight,
    ) = masters
    fs, ctx, ten = (lax.axis_size(name) for name in ("fsdp", "context", "tensor"))
    x = lax.axis_index("tensor")
    context_index = lax.axis_index("context")
    block, width = hidden_in.shape[1:]
    rows = query_weight.shape[0]
    half_rows = block // ten
    heads_width = query_weight.shape[1]
    heads_here = heads_width // HD
    hidden = hidden_in[0]
    cot = cotangent[0]
    hidden_half = lax.dynamic_slice_in_dim(hidden, x * half_rows, half_rows, 0)
    cot_half = lax.dynamic_slice_in_dim(cot, x * half_rows, half_rows, 0)
    is_key = x == 0

    qkv_block = jnp.concatenate(
        [
            cast(query_weight),
            cast(lax.dynamic_slice_in_dim(keyval_weight, x * HD, HD, 1)),
        ],
        axis=1,
    )
    lanes = -(-max(rows, block) // 128) * 128
    small = jnp.zeros((8, lanes), single)
    small = small.at[0, :rows].set(attn_scale).at[1, :rows].set(mlp_scale)
    small = small.at[2, :block].set(segment_ids[0].astype(single))
    small_all, qkv_all, out_all, dy_all = spread(
        [small, qkv_block, cast(output_weight).T],
        (False, False, False),
        cast(cot_half),
        fs,
        ctx,
        ten,
        1,
    )
    scale_one = cast(small_all[:, :, 0, :rows].reshape(-1)).astype(single)
    scale_two = cast(small_all[:, :, 1, :rows].reshape(-1)).astype(single)
    f = lax.axis_index("fsdp")
    seg_all = lax.dynamic_index_in_dim(small_all[:, :, 2, :block], f, 0, False).reshape(-1)
    qkv_full = qkv_all.reshape(width, -1)
    out_full = out_all.reshape(width, -1)
    dy_all = dy_all.reshape(-1, width)

    normed_one, inv_one, low_one = rms_forward(hidden, scale_one)
    qkv = dot(low_one, qkv_full, ((1,), (0,)))
    query = qkv[:, :heads_width].reshape(block, heads_here, HD)
    own = qkv[:, heads_width:]
    cosine, sine = rope_tables(positions[0])
    query_low = cast(rotate(query, cosine[:, None, :], sine[:, None, :]) * HD ** (-0.5))
    own_low = cast(jnp.where(is_key, rotate(own, cosine, sine), own))
    keyval_all = tokens_to_all(own_low, ctx, ten, 2).reshape(ctx, ten, block, HD)
    keys_all = keyval_all[:, 0].reshape(-1, HD)
    values_all = keyval_all[:, 1].reshape(-1, HD)
    rows_index = context_index * block + jnp.arange(block, dtype=jnp.int32)
    cols_index = jnp.arange(keys_all.shape[0], dtype=jnp.int32)
    allowed = (rows_index[:, None] >= cols_index[None, :]) & (
        segment_ids[0].astype(single)[:, None] == seg_all[None, :]
    )
    scores = jnp.einsum("bhd,jd->hbj", query_low, keys_all, preferred_element_type=single)
    masked = jnp.where(allowed, scores, masked_value)
    top = jnp.max(masked, axis=-1, keepdims=True)
    total = jnp.sum(jnp.where(allowed, jnp.exp(masked - top), 0.0), axis=-1, keepdims=True)
    lse = top + jnp.log(total)
    prob = jnp.where(allowed, jnp.exp(masked - lse), 0.0)
    prob_low = cast(prob)
    att_low = cast(
        jnp.einsum("hbj,jd->bhd", prob_low, values_all, preferred_element_type=single)
    )
    att_flat = att_low.reshape(block, heads_width)
    attn_part = dot(att_flat, out_full, ((1,), (1,)))
    attn_half = swap(cast(attn_part).reshape(ten, half_rows, width), ten, 3)
    mid_half = hidden_half + jnp.sum(attn_half.astype(single), axis=0)

    normed_two, inv_two, low_two = rms_forward(mid_half, scale_two)
    gate_slice, up_slice, down_slice, low_all = spread(
        [
            own_columns(gate_weight, ctx),
            own_columns(up_weight, ctx),
            own_columns(down_weight.T, ctx),
        ],
        (True, True, True),
        low_two,
        fs,
        ctx,
        ten,
        4,
    )
    gate_slice, up_slice, down_slice = (
        s.reshape(width, -1) for s in (gate_slice, up_slice, down_slice)
    )
    low_all = low_all.reshape(-1, width)
    gate = dot(low_all, gate_slice, ((1,), (0,)))
    upper = dot(low_all, up_slice, ((1,), (0,)))
    dhid = dot(dy_all, down_slice, ((1,), (0,)))
    gelu_gate, gelu_back = jax.vjp(gelu_tanh, gate)
    hid_low = cast(gelu_gate * upper)
    dgate_low = cast(gelu_back(dhid * upper)[0])
    dup_low = cast(dhid * gelu_gate)
    dnorm_part = cast(
        dot(dgate_low, gate_slice, ((1,), (1,))) + dot(dup_low, up_slice, ((1,), (1,)))
    )
    mlp_part = cast(dot(hid_low, down_slice, ((1,), (1,))))
    token_blocks = (ctx, ten, half_rows, width)
    row_blocks = (fs, ctx, rows, -1)
    dnorm_two, mlp_half, grad_wd, grad_wg, grad_wu = mlp_back(
        low_all.T.reshape(row_blocks),
        dy_all.T.reshape(row_blocks),
        hid_low,
        dgate_low,
        dup_low,
        dnorm_part.reshape(token_blocks),
        mlp_part.reshape(token_blocks),
        fs,
        ctx,
        ten,
        5,
    )
    dmid_norm, terms_two = rms_backward(dnorm_two, normed_two, inv_two, scale_two)
    dmid_half = cot_half + dmid_norm

    dmid_low = swap(
        jnp.broadcast_to(cast(dmid_half)[None], (ten, half_rows, width)), ten, 6
    ).reshape(block, width)
    datt_low = cast(dot(dmid_low, out_full, ((1,), (0,)))).reshape(block, heads_here, HD)
    delta = jnp.einsum("bhd,bhd->hb", datt_low, att_low, preferred_element_type=single)
    dprob = jnp.einsum("bhd,jd->hbj", datt_low, values_all, preferred_element_type=single)
    dscore_low = cast(prob * (dprob - delta[..., None]))
    dquery = jnp.einsum("hbj,jd->bhd", dscore_low, keys_all, preferred_element_type=single)
    dkey_part = jnp.einsum("hbj,bhd->jd", dscore_low, query_low, preferred_element_type=single)
    dvalue_part = jnp.einsum("hbj,bhd->jd", prob_low, datt_low, preferred_element_type=single)
    own_part = jnp.stack(
        [cast(part).reshape(ctx, block, HD) for part in (dkey_part, dvalue_part)], axis=1
    )
    down_own = sum_tokens(own_part.reshape(-1, HD), ctx, ten, 7)
    dquery_low = cast(
        unrotate(dquery, cosine[:, None, :], sine[:, None, :]) * HD ** (-0.5)
    ).reshape(block, heads_width)
    down_own = cast(jnp.where(is_key, unrotate(down_own, cosine, sine), down_own))
    d_qkv = jnp.concatenate([dquery_low, down_own], axis=1)
    dnorm_one = dot(d_qkv, qkv_full, ((1,), (1,)))
    dnorm_one = swap(cast(dnorm_one).reshape(ten, half_rows, width), ten, 8)
    dnorm_one = jnp.sum(dnorm_one.astype(single), axis=0)
    normed_half = lax.dynamic_slice_in_dim(normed_one, x * half_rows, half_rows, 0)
    inv_half = lax.dynamic_slice_in_dim(inv_one, x * half_rows, half_rows, 0)
    dinput_norm, terms_one = rms_backward(dnorm_one, normed_half, inv_half, scale_one)
    terms = jnp.stack([jnp.sum(terms_one, axis=0), jnp.sum(terms_two, axis=0)])
    terms = terms.reshape(2, fs, ctx, rows).transpose(1, 2, 0, 3)
    terms = jnp.pad(terms, ((0, 0), (0, 0), (0, 6), (0, -rows % 128)))
    give = cast(jnp.stack([mid_half + mlp_half, dmid_half + dinput_norm]))
    grad_wq, grad_wo, grad_s, grad_wkv, outs = attn_back(
        low_one.T.reshape(row_blocks),
        dmid_low.T.reshape(row_blocks),
        d_qkv,
        att_flat,
        terms,
        give,
        heads_width,
        fs,
        ctx,
        ten,
        9,
    )
    outs = outs.transpose(1, 0, 2, 3).reshape(2, 1, block, width).astype(single)

    def joined(grad):
        return grad.transpose(1, 0, 2).reshape(rows, -1).astype(single)

    grads = (
        grad_s[0, :rows],
        grad_wq,
        grad_wkv,
        grad_wo.T,
        grad_s[1, :rows],
        joined(grad_wg),
        joined(grad_wu),
        joined(grad_wd).T,
    )
    results = [
        adamw(weight, grad, first, second)
        for weight, grad, first, second in zip(masters, grads, firsts, seconds)
    ]
    return (
        outs[0],
        outs[1],
        *grads,
        *(entry[0] for entry in results),
        *(entry[1] for entry in results),
        *(entry[2] for entry in results),
    )


def solution(mesh):
    both = ("fsdp", "context")
    tokens = P("fsdp", "context", None)
    weights = (
        P(both),
        P(both, "tensor"),
        P(both, None),
        P("tensor", both),
        P(both),
        P(both, "tensor"),
        P(both, "tensor"),
        P("tensor", both),
    )
    return jax.shard_map(
        on_device,
        mesh=mesh,
        in_specs=(tokens, tokens, P("fsdp", "context"), P("fsdp", "context"), *(weights * 3)),
        out_specs=(tokens, tokens, *(weights * 4)),
        check_vma=False,
    )
```

```python
import functools

import jax
import jax.numpy as jnp
from jax import lax
from jax.experimental import pallas as pl
from jax.experimental.pallas import tpu as pltpu
from jax.sharding import PartitionSpec as P

HD = 256


norm_eps = 1e-06
beta_one = 0.9
beta_two = 0.999
adam_eps = 1e-08
learn_rate = 0.03
decay_rate = 0.1
adam_step = 4.0
rope_base = 10000.0
masked_value = -1e30

single = jnp.float32
half_type = jnp.bfloat16


def gelu_tanh(values):
    return jax.nn.gelu(values, approximate=True)


def rope_tables(positions):
    half = HD // 2
    freq = rope_base ** (-2.0 * jnp.arange(half).astype(jnp.float32) / HD)
    angle = positions.astype(jnp.float32)[..., None] * freq
    return (jnp.cos(angle), jnp.sin(angle))


def rotate(values, cosine, sine):
    half = values.shape[-1] // 2
    first = values[..., :half]
    second = values[..., half:]
    return jnp.concatenate(
        [first * cosine - second * sine, second * cosine + first * sine], axis=-1
    )


def unrotate(values, cosine, sine):
    half = values.shape[-1] // 2
    first = values[..., :half]
    second = values[..., half:]
    return jnp.concatenate(
        [first * cosine + second * sine, second * cosine - first * sine], axis=-1
    )


def rms_forward(values, scale):
    inverse = lax.rsqrt(jnp.mean(values * values, axis=-1, keepdims=True) + norm_eps)
    normed = values * inverse
    return (normed, inverse, (normed * (1.0 + scale)).astype(jnp.bfloat16))


def rms_backward(dnorm, normed, inverse, scale):
    dnormed = dnorm * (1.0 + scale)
    dvalues = inverse * (dnormed - normed * jnp.mean(dnormed * normed, axis=-1, keepdims=True))
    return (dvalues, dnorm * normed)


def adamw(weight, grad, first, second):
    first_new = beta_one * first + (1.0 - beta_one) * grad
    second_new = beta_two * second + (1.0 - beta_two) * grad * grad
    fix_one = 1.0 - beta_one**adam_step
    fix_two = 1.0 - beta_two**adam_step
    update = first_new / fix_one / (jnp.sqrt(second_new / fix_two) + adam_eps)
    return (weight - learn_rate * (update + decay_rate * weight), first_new, second_new)


def dot(a, b, dims):
    return lax.dot_general(a, b, (dims, ((), ())), preferred_element_type=single)


MESH = pl.DeviceIdType.MESH
ANY = pl.BlockSpec(memory_space=pl.ANY)
VMEM = pl.BlockSpec(memory_space=pltpu.VMEM)


def greet(peers):
    barrier = pltpu.get_barrier_semaphore()
    for peer in peers:
        pl.semaphore_signal(barrier, inc=1, device_id=peer, device_id_type=MESH)
    pl.semaphore_wait(barrier, len(peers))


def remote(src, dst, send, recv, peer):
    return pltpu.make_async_remote_copy(
        src_ref=src, dst_ref=dst, send_sem=send, recv_sem=recv, device_id=peer, device_id_type=MESH
    )


def arrived(dst, recv, peer):
    remote(dst, dst, recv, recv, peer).wait_recv()


def fsdp_place(fs):
    f = lax.axis_index("fsdp")
    core = lax.rem(f, 2)
    y = lax.div(f, 2)
    twin = {"fsdp": f + 1 - 2 * core}
    across = [{"fsdp": lax.rem(y + d, fs // 2) * 2 + core} for d in range(1, fs // 2)]
    return f, y, core, twin, across


class Sends:
    def __init__(self, send):
        self.send, self.made = send, []

    def push(self, src, dst, recv, peer, *conditions):
        copy = remote(src, dst, self.send.at[len(self.made)], recv, peer)
        self.made.append((copy, conditions))
        under(conditions, copy.start)

    def drain(self):
        for copy, conditions in self.made:
            under(conditions, copy.wait_send)


def under(conditions, action):
    if not conditions:
        action()
        return
    holds = conditions[0]
    for more in conditions[1:]:
        holds = jnp.logical_and(holds, more)
    pl.when(holds)(action)


def line_steps(z, ctx):
    for s in range(1, ctx):
        yield z - s, z >= s, z + 1, z + 1 < ctx
        yield z + s, z + s < ctx, z - 1, z >= 1


def tokens_kernel(ctx, ten, src, out, local, send, recv):
    z, x = lax.axis_index("context"), lax.axis_index("tensor")
    around = [lax.rem(z + d, ctx) for d in range(ctx)]
    across = [{"tensor": lax.rem(x + d, ten)} for d in range(1, ten)]
    greet([{"context": k} for k in around[1:]] + across)
    sends = []

    def push(ref, source, peer):
        copy = remote(ref, out.at[source, x], send.at[len(sends)], recv.at[source, x], peer)
        copy.start()
        sends.append(copy)

    for d in range(1, ctx):
        push(src, z, {"context": around[d]})
    for peer in across:
        push(src, z, peer)
    keep = pltpu.make_async_copy(src, out.at[z, x], local)
    keep.start()
    back = [lax.rem(z + ctx - d, ctx) for d in range(ctx)]
    for d in range(1, ctx):
        arrived(out.at[back[d], x], recv.at[back[d], x], {"context": back[d]})
        for peer in across:
            push(out.at[back[d], x], back[d], peer)
    for d in range(ctx):
        for peer in across:
            other = peer["tensor"]
            arrived(out.at[back[d], other], recv.at[back[d], other], peer)
    keep.wait()
    for copy in sends:
        copy.wait_send()


def tokens_to_all(block, ctx, ten, ident):
    sends = (ctx - 1) + ctx * (ten - 1)
    out = pl.pallas_call(
        functools.partial(tokens_kernel, ctx, ten),
        out_shape=jax.ShapeDtypeStruct((ctx, ten, *block.shape), block.dtype),
        in_specs=[VMEM],
        out_specs=VMEM,
        scratch_shapes=[
            pltpu.SemaphoreType.DMA(()),
            pltpu.SemaphoreType.DMA((sends,)),
            pltpu.SemaphoreType.DMA((ctx, ten)),
        ],
        compiler_params=pltpu.CompilerParams(collective_id=ident, has_side_effects=True),
        name=f"tokens_{ident}",
    )(block)
    return out.reshape(-1, block.shape[-1])


VMEM_ALL = 67043328


def cast(v):
    return v.astype(half_type)


def fill_product(dw, left, right, owner, ctx):
    def one(k, carry):
        dw[owner, k] = cast(
            lax.dot_general(
                left[owner, k], right[...], (((1,), (0,)), ((), ())), preferred_element_type=single
            )
        )
        return carry

    lax.fori_loop(0, ctx, one, 0)


def split_columns(ctx, weights, parts, wide, packed, small, load, store):
    columns = small.shape[-1]
    fetches = [pltpu.make_async_copy(weights[w], wide.at[w], load.at[w]) for w in range(3)]
    for fetch in fetches:
        fetch.start()
    for w in range(3):
        fetches[w].wait()
        for k in range(ctx):
            piece = cast(wide[w, :, k * columns : (k + 1) * columns])
            if w < 2:
                packed[k, :, w * columns : (w + 1) * columns] = piece
            else:
                small[k] = piece
    puts = [pltpu.make_async_copy(v, parts[j], store.at[j]) for j, v in enumerate((packed, small))]
    for put in puts:
        put.start()
    for put in puts:
        put.wait()


def first_kernel(fs, ctx, ten, count, *refs):
    srcs, weights = refs[: count + 1], refs[count + 1 : count + 4]
    refs = refs[count + 4 :]
    outs, parts = refs[: count + 1], refs[count + 1 : count + 3]
    wide, packed, small, load, store, local, send, recv, recv_t = refs[count + 3 :]
    f, y, core, twin, across = fsdp_place(fs)
    z, x = lax.axis_index("context"), lax.axis_index("tensor")
    beside = [{"tensor": lax.rem(x + d, ten)} for d in range(1, ten)]
    back = [lax.rem(z + ctx - d, ctx) for d in range(ctx)]
    up, down = {"context": z + 1}, {"context": z - 1}
    nxt, prv = lax.rem(z + 1, ctx), back[1]
    greet([{"context": nxt}, {"context": prv}] + across + [twin] + beside)
    out = Sends(send)
    keeps = []

    def where(w, source):
        if w == count:
            return outs[w].at[source, x], recv_t.at[source, x], beside
        return outs[w].at[f, source], recv.at[w, f, source], across + [twin]

    for w in range(count + 1):
        mine, sem, peers = where(w, z)
        out.push(srcs[w], mine, sem, up, z + 1 < ctx)
        out.push(srcs[w], mine, sem, down, z >= 1)
        for peer in peers:
            out.push(srcs[w], mine, sem, peer)
        keeps.append(pltpu.make_async_copy(srcs[w], mine, local.at[w]))
        keeps[-1].start()
    split_columns(ctx, weights, parts, wide, packed, small, load, store)
    for source, exists, onward, more in line_steps(z, ctx):
        for w in range(count + 1):
            block, sem, peers = where(w, source)
            under((exists,), lambda: arrived(block, sem, twin))
            out.push(block, block, sem, {"context": onward}, exists, more)
            for peer in peers:
                out.push(block, block, sem, peer, exists)
    chain = [(z, ())] + [(source, (exists,)) for source, exists, _, _ in line_steps(z, ctx)]
    for source, when in chain:
        for w in range(count):
            for peer in across:
                owner = peer["fsdp"]
                block, sem = outs[w].at[owner, source], recv.at[w, owner, source]
                under(when, lambda: arrived(block, sem, twin))
                out.push(block, block, sem, twin, *when)
    for source in back:
        for w in range(count):
            for step in range(fs // 2):
                owner = lax.rem(y + step, fs // 2) * 2 + 1 - core
                arrived(outs[w].at[owner, source], recv.at[w, owner, source], twin)
        for peer in beside:
            arrived(outs[count].at[source, peer["tensor"]], recv_t.at[source, peer["tensor"]], twin)
    for keep in keeps:
        keep.wait()
    out.drain()


def spread(blocks, tokens, weights, fs, ctx, ten, ident):
    count = len(blocks)
    chips = fs // 2
    lines = 2 + 2 * (ctx - 1)
    sends = count * (lines + (2 * ctx - 1) * (2 * chips - 1)) + lines + (2 * ctx - 1) * (ten - 1)
    rows, wide = weights[0].shape
    part = (ctx, rows, wide // ctx)
    pair = (ctx, rows, 2 * (wide // ctx))
    dma = pltpu.SemaphoreType.DMA
    return pl.pallas_call(
        functools.partial(first_kernel, fs, ctx, ten, count),
        out_shape=[jax.ShapeDtypeStruct((fs, ctx, *b.shape), b.dtype) for b in blocks]
        + [jax.ShapeDtypeStruct((ctx, ten, *tokens.shape), tokens.dtype)]
        + [jax.ShapeDtypeStruct(pair, half_type), jax.ShapeDtypeStruct(part, half_type)],
        in_specs=[ANY] * (count + 4),
        out_specs=[ANY] * (count + 3),
        scratch_shapes=[
            pltpu.VMEM((3, rows, wide), single),
            pltpu.VMEM(pair, half_type),
            pltpu.VMEM(part, half_type),
            dma((3,)),
            dma((2,)),
            dma((count + 1,)),
            dma((sends,)),
            dma((count, fs, ctx)),
            dma((ctx, ten)),
        ],
        compiler_params=pltpu.CompilerParams(
            collective_id=ident, has_side_effects=True, vmem_limit_bytes=VMEM_ALL
        ),
        name=f"spread_{ident}",
    )(*blocks, tokens, *weights)


def line_sum(z, ctx, owner, gathered, mine, slots, sem, out, kind, done):
    @pl.when(z == owner)
    def _():
        done(gathered())

    for toward, at, edge, past in (
        ({"context": z + 1}, owner + 1, z == 0, z < owner),
        ({"context": z - 1}, owner, z == ctx - 1, z > owner),
    ):

        @pl.when(jnp.logical_and(past, edge))
        def _():
            mine[...] = kind(gathered())

        @pl.when(jnp.logical_and(past, jnp.logical_not(edge)))
        def _():
            arrived(slots.at[at], sem.at[at], toward)
            mine[...] = kind(gathered() + slots[at].astype(single))

        out.push(mine, slots.at[at], sem.at[at], toward, past)


def line_end(z, ctx, slots, sem, add):
    for at, edge in ((z + 1, z == 0), (z, z == ctx - 1)):

        @pl.when(jnp.logical_not(edge))
        def _():
            arrived(slots.at[at], sem.at[at], {"context": z})
            add(slots[at].astype(single))


def ends_first(ctx):
    order = []
    for k in range((ctx + 1) // 2):
        order += [ctx - 1 - k] + ([k] if k != ctx - 1 - k else [])
    return order


def chip_tiles(weight, held, load, use):
    chips = weight.shape[0] // 2

    def fetch(k, slot):
        return pltpu.make_async_copy(weight.at[pl.ds(2 * k, 2)], held.at[slot], load.at[slot])

    fetch(0, 0).start()

    def step(k, carry):
        slot = lax.rem(k, 2)
        fetch(k, slot).wait()

        @pl.when(k + 1 < chips)
        def _():
            fetch(k + 1, 1 - slot).start()

        use(k, held[slot].reshape(-1, held.shape[-1]))
        return carry

    lax.fori_loop(0, chips, step, 0)


def forward_kernel(fs, ctx, ten, *refs):
    attn, hidden, scale, dy, part_p, part_d = refs[:6]
    slice_p, slice_d, hid, dpair, low_t, dy_t, mid, low = refs[6:14]
    low_all, take, held_p, held_d, sums_p, sums_d = refs[14:20]
    load, local, send, recv_p, recv_d, recv_t, recv_x = refs[20:]
    f, y, core, twin, across = fsdp_place(fs)
    z, x = lax.axis_index("context"), lax.axis_index("tensor")
    rows, columns = part_d.shape[1:]
    width = low.shape[1]
    count = hid.shape[0]
    beside = [{"tensor": lax.rem(x + d, ten)} for d in range(1, ten)]
    around = [lax.rem(z + d, ctx) for d in range(ctx)]
    back = [lax.rem(z + ctx - d, ctx) for d in range(ctx)]
    greet([{"context": k} for k in around[1:]] + across + [twin] + beside)
    out = Sends(send)
    parts, slices, recvs = (part_d, part_p), (slice_d, slice_p), (recv_d, recv_p)
    for peer in beside:
        out.push(attn.at[peer["tensor"]], take.at[x], recv_x.at[x], peer)

    def block(w, owner, source):
        return slices[w].at[owner, source], recvs[w].at[owner, source]

    def to_context(w, d):
        dst, sem = block(w, f, z)
        out.push(parts[w].at[around[d]], dst, sem, {"context": around[d]})

    def from_context(w, d):
        dst, sem = block(w, f, back[d])
        arrived(dst, sem, twin)
        for peer in across + [twin]:
            out.push(dst, dst, sem, peer)

    def from_chips(w):
        for d in range(ctx):
            for peer in across:
                dst, sem = block(w, peer["fsdp"], back[d])
                arrived(dst, sem, twin)
                out.push(dst, dst, sem, twin)

    def from_twin(w):
        for d in range(ctx):
            for step in range(fs // 2):
                dst, sem = block(w, lax.rem(y + step, fs // 2) * 2 + 1 - core, back[d])
                arrived(dst, sem, twin)

    to_context(0, 1)
    keeps = []
    for w in range(2):
        dst, sem = block(w, f, z)
        for peer in across + [twin]:
            out.push(parts[w].at[z], dst, sem, peer)
        keeps.append(pltpu.make_async_copy(parts[w].at[z], dst, local.at[w]))
        keeps[-1].start()
    total = hidden[...] + attn[x].astype(single)
    for peer in beside:
        other = peer["tensor"]
        arrived(take.at[other], recv_x.at[other], twin)
        total = total + take[other].astype(single)
    mid[...] = total
    inverse = lax.rsqrt(jnp.mean(total * total, axis=-1, keepdims=True) + norm_eps)
    low_all[z, x] = cast(total * inverse * (1.0 + scale[...]))
    mine = low_all.at[z, x]
    out.push(mine, mine, recv_t.at[z, x], {"context": z + 1}, z + 1 < ctx)
    out.push(mine, mine, recv_t.at[z, x], {"context": z - 1}, z >= 1)
    for peer in beside:
        out.push(mine, mine, recv_t.at[z, x], peer)
    later = [(0, d) for d in range(2, ctx)] + [(1, d) for d in range(1, ctx)]
    for step, (source, exists, onward, more) in enumerate(line_steps(z, ctx)):
        if step % 2 == 0:
            to_context(*later.pop(0))
            from_context(0, step // 2 + 1)
        here, sem = low_all.at[source, x], recv_t.at[source, x]
        under((exists,), lambda: arrived(here, sem, twin))
        out.push(here, here, sem, {"context": onward}, exists, more)
        for peer in beside:
            out.push(here, here, sem, peer, exists)
    for more in later:
        to_context(*more)

    def turned(dst, src):
        for j in range(fs * ctx):
            piece = src[:, :, :, j * rows : (j + 1) * rows].reshape(count, rows)
            dst[j // ctx, j % ctx] = piece.T

    def product(weight, held, left, sums):
        deep = width // (fs // 2)

        def use(k, tile):
            lanes = pl.ds(pl.multiple_of(k * deep, deep), deep)
            add = jnp.dot(
                left[:, :, :, lanes].reshape(count, deep), tile, preferred_element_type=single
            )

            @pl.when(k == 0)
            def _():
                sums[...] = add

            @pl.when(k > 0)
            def _():
                sums[...] += add

        chip_tiles(weight, held, load, use)

    from_chips(0)
    turned(dy_t, dy)
    from_context(1, 1)
    for source in back:
        for peer in beside:
            other = peer["tensor"]
            arrived(low_all.at[source, other], recv_t.at[source, other], twin)
    from_twin(0)
    keeps[0].wait()
    product(slice_d, held_d, dy, sums_d)
    for d in range(2, ctx):
        from_context(1, d)
    turned(low_t, low_all)
    from_chips(1)
    from_twin(1)
    keeps[1].wait()
    product(slice_p, held_p, low_all, sums_p)
    low[...] = low_all[z, x]
    root = (2.0 / jnp.pi) ** 0.5
    part = count // ctx

    def finish(k, carry):
        here = pl.ds(pl.multiple_of(k * part, part), part)
        pair, dhid = sums_p[here, :], sums_d[here, :]
        gate, upper = pair[:, :columns], pair[:, columns:]
        square = gate * gate
        tanh = jnp.tanh(root * gate * (1.0 + 0.044715 * square))
        gelu = 0.5 * gate * (1.0 + tanh)
        slope = 0.5 * (1.0 + tanh) + 0.5 * gate * (1.0 - tanh * tanh) * root * (
            1.0 + 3.0 * 0.044715 * square
        )
        hid[here, :] = cast(gelu * upper)
        dpair[here, :columns] = cast(dhid * upper * slope)
        dpair[here, columns:] = cast(dhid * gelu)
        return carry

    lax.fori_loop(0, ctx, finish, 0)
    out.drain()


def mlp_forward(attn, hidden, scale, dy_all, part_p, part_d, fs, ctx, ten, ident):
    rows, columns = part_d.shape[1:]
    t_rows, width = hidden.shape
    count = ctx * ten * t_rows
    chips = fs // 2
    sends = 2 * (ten - 1) + 2 * ctx + 2 * (ctx - 1) * (ten - 1) + 2 * (3 * ctx - 1 + 3 * ctx * chips)
    dma = pltpu.SemaphoreType.DMA
    shape = jax.ShapeDtypeStruct
    return pl.pallas_call(
        functools.partial(forward_kernel, fs, ctx, ten),
        out_shape=[
            shape((fs, ctx, rows, 2 * columns), half_type),
            shape((fs, ctx, rows, columns), half_type),
            shape((count, columns), half_type),
            shape((count, 2 * columns), half_type),
            shape((fs, ctx, rows, count), half_type),
            shape((fs, ctx, rows, count), half_type),
            shape((t_rows, width), single),
            shape((t_rows, width), half_type),
        ],
        in_specs=[VMEM] * 4 + [ANY] * 2,
        out_specs=[ANY] * 2 + [VMEM] * 6,
        scratch_shapes=[
            pltpu.VMEM((ctx, ten, t_rows, width), half_type),
            pltpu.VMEM((ten, t_rows, width), half_type),
            pltpu.VMEM((2, 2, ctx, rows, 2 * columns), half_type),
            pltpu.VMEM((2, 2, ctx, rows, columns), half_type),
            pltpu.VMEM((count, 2 * columns), single),
            pltpu.VMEM((count, columns), single),
            dma((2,)),
            dma((2,)),
            dma((sends,)),
            dma((fs, ctx)),
            dma((fs, ctx)),
            dma((ctx, ten)),
            dma((ten,)),
        ],
        compiler_params=pltpu.CompilerParams(
            collective_id=ident, has_side_effects=True, vmem_limit_bytes=VMEM_ALL
        ),
        name=f"mlp_forward_{ident}",
    )(attn, hidden, scale, dy_all, part_p, part_d)


def token_products(source, left, weight, held, load):
    def use(k, tile):
        term = lax.dot_general(
            left[...], tile, (((1,), (1,)), ((), ())), preferred_element_type=single
        )
        deep = tile.shape[0]
        lanes = pl.ds(pl.multiple_of(k * deep, deep), deep)
        source[:, :, :, lanes] = cast(term).reshape(*source.shape[:3], deep)

    chip_tiles(weight, held, load, use)


def token_start(source, first, recv, out, beside, order):
    for owner in order:
        for k, other in enumerate(beside):
            out.push(
                source.at[owner, other], first.at[k, owner], recv.at[k, owner], {"tensor": other}
            )


def token_step(owner, source, first, recv, slots, sems, z, x, ctx, out, done):
    for k in range(first.shape[0]):
        arrived(first.at[k, owner], recv.at[k, owner], {"tensor": x})

    def gathered():
        total = source[owner, x].astype(single)
        for k in range(first.shape[0]):
            total = total + first[k, owner].astype(single)
        return total

    line_sum(z, ctx, owner, gathered, source.at[owner, x], slots, sems, out, cast, done)


def back_kernel(fs, ctx, ten, *refs):
    low_t, dy_t, hid, dpair, mid, cot, scale, slice_p = refs[:8]
    dmid, dmid_all, terms, out_p, out_d = refs[8:13]
    dws, nears, fars = refs[13:15], refs[15:17], refs[17:19]
    source, first, line, held = refs[19:23]
    load, local, send, recv_c, recv_y, recv_z, recv_tx, recv_t, recv_x = refs[23:]
    f, y, core, twin, across = fsdp_place(fs)
    z, x = lax.axis_index("context"), lax.axis_index("tensor")
    chips = fs // 2
    around = [lax.rem(z + d, ctx) for d in range(ctx)]
    beside = [lax.rem(x + d, ten) for d in range(1, ten)]
    rows_of = [lax.rem(y + d, chips) for d in range(chips)]
    chip_order = rows_of[1:] + rows_of[:1]
    order = around[1:] + around[:1]
    greet([{"context": k} for k in around[1:]] + across + [twin] + [{"tensor": k} for k in beside])
    out = Sends(send)
    outs = (out_d, out_p)
    keeps = []

    def products(w):
        left, right = (dy_t, low_t)[w], (hid, dpair)[w]
        for row in chip_order:
            fill_product(dws[w], left, right, row * 2 + 1 - core, ctx)
            out.push(dws[w].at[row * 2 + 1 - core], nears[w].at[row], recv_c.at[w, row], twin)
        for row in chip_order:
            fill_product(dws[w], left, right, row * 2 + core, ctx)

    def over_chips(w):
        for k, row in enumerate(rows_of[1:]):
            arrived(nears[w].at[row], recv_c.at[w, row], twin)
            for d, owner in enumerate(order):
                mine = dws[w].at[row * 2 + core, owner]
                mine[...] = cast(mine[...].astype(single) + nears[w][row, owner].astype(single))
                out.push(mine, fars[w].at[k, d], recv_y.at[w, k, d], across[k])

    def over_context(w, d):
        if d == 0:
            arrived(nears[w].at[y], recv_c.at[w, y], twin)
        owner = order[d]
        mine = dws[w].at[f, owner]
        total = mine[...].astype(single) + nears[w][y, owner].astype(single)
        for k in range(chips - 1):
            arrived(fars[w].at[k, d], recv_y.at[w, k, d], twin)
            total = total + fars[w][k, d].astype(single)
        mine[...] = cast(total)
        if d < ctx - 1:
            out.push(mine, outs[w].at[z], recv_z.at[w, z], {"context": owner})
        else:
            keep = pltpu.make_async_copy(mine, outs[w].at[z], local.at[w])
            keep.start()
            keeps.append(keep)

    def keep_sum(v):
        dmid[...] = v

    def add_sum(v):
        dmid[...] += v

    token_products(source, dpair, slice_p, held, load)
    ends = ends_first(ctx)
    token_start(source, first, recv_tx, out, beside, ends)
    products(0)
    over_chips(0)
    products(1)
    over_chips(1)
    for d, owner in enumerate(ends):
        token_step(owner, source, first, recv_tx, line, recv_t, z, x, ctx, out, keep_sum)
        over_context(0, d)
    line_end(z, ctx, line, recv_t, add_sum)
    dnorm = dmid[...]
    values = mid[...]
    inverse = lax.rsqrt(jnp.mean(values * values, axis=-1, keepdims=True) + norm_eps)
    normed = values * inverse
    dnormed = dnorm * (1.0 + scale[...])
    terms[...] = jnp.sum(dnorm * normed, axis=0, keepdims=True)
    total = cot[...] + inverse * (
        dnormed - normed * jnp.mean(dnormed * normed, axis=-1, keepdims=True)
    )
    dmid[...] = total
    dmid_all[x] = cast(total)
    for other in beside:
        out.push(dmid_all.at[x], dmid_all.at[x], recv_x.at[x], {"tensor": other})
    for d in range(ctx):
        over_context(1, d)
    for other in beside:
        arrived(dmid_all.at[other], recv_x.at[other], twin)
    for w in range(2):
        for k in around[1:]:
            arrived(outs[w].at[k], recv_z.at[w, k], twin)
    for keep in keeps:
        keep.wait()
    out.drain()


def mlp_back(low_t, dy_t, hid, dpair, mid, cot, scale, slice_p, fs, ctx, ten, ident):
    rows, columns = low_t.shape[2], hid.shape[1]
    t_rows, width = mid.shape
    chips = fs // 2
    blocks = [(rows, columns), (rows, 2 * columns)]
    sends = ctx * (ten - 1) + 2 * ctx + 2 * (chips + (chips - 1) * ctx + ctx - 1) + ten - 1
    dma = pltpu.SemaphoreType.DMA
    shape = jax.ShapeDtypeStruct
    return pl.pallas_call(
        functools.partial(back_kernel, fs, ctx, ten),
        out_shape=[
            shape((t_rows, width), single),
            shape((ten, t_rows, width), half_type),
            shape((1, width), single),
            shape((ctx, rows, 2 * columns), half_type),
            shape((ctx, rows, columns), half_type),
        ],
        in_specs=[VMEM] * 7 + [ANY],
        out_specs=[VMEM] * 3 + [ANY] * 2,
        scratch_shapes=[pltpu.VMEM((fs, ctx, *b), half_type) for b in blocks]
        + [pltpu.VMEM((chips, ctx, *b), half_type) for b in blocks]
        + [pltpu.VMEM((chips - 1, ctx, *b), half_type) for b in blocks]
        + [
            pltpu.VMEM((ctx, ten, t_rows, width), half_type),
            pltpu.VMEM((ten - 1, ctx, t_rows, width), half_type),
            pltpu.VMEM((ctx + 1, t_rows, width), half_type),
            pltpu.VMEM((2, 2, ctx, rows, 2 * columns), half_type),
            dma((2,)),
            dma((2,)),
            dma((sends,)),
            dma((2, chips)),
            dma((2, chips - 1, ctx)),
            dma((2, ctx)),
            dma((ten - 1, ctx)),
            dma((ctx + 1,)),
            dma((ten,)),
        ],
        compiler_params=pltpu.CompilerParams(
            collective_id=ident, has_side_effects=True, vmem_limit_bytes=VMEM_ALL
        ),
        name=f"mlp_back_{ident}",
    )(low_t, dy_t, hid, dpair, mid, cot, scale, slice_p)


def update_kernel(at, parts, weight, first, second, grad_out, weight_out, first_out, second_out):
    columns = weight.shape[1] // parts.shape[0]
    for k in range(parts.shape[0]):
        grad = parts[k, :, at * columns : (at + 1) * columns].astype(single)
        here = (slice(None), slice(k * columns, (k + 1) * columns))
        grad_out[here] = grad
        weight_out[here], first_out[here], second_out[here] = adamw(
            weight[here], grad, first[here], second[here]
        )


def update(parts, at, weight, first, second, ident):
    ctx, rows, columns = parts.shape
    step = 32 if rows % 32 == 0 else 8
    spec = pl.BlockSpec((step, weight.shape[1]), lambda i: (i, 0))
    part = pl.BlockSpec((ctx, step, columns), lambda i: (0, i, 0))
    return pl.pallas_call(
        functools.partial(update_kernel, at),
        grid=(rows // step,),
        out_shape=[jax.ShapeDtypeStruct(weight.shape, single)] * 4,
        in_specs=[part, spec, spec, spec],
        out_specs=[spec] * 4,
        compiler_params=pltpu.CompilerParams(vmem_limit_bytes=VMEM_ALL),
        name=f"update_{ident}",
    )(parts, weight, first, second)


def attn_kernel(fs, ctx, ten, *refs):
    low_t, dmid_t, d_query, att, own, cosine, sine, hidden, mid, dmid, scale, terms = refs[:12]
    hid, slice_d, slice_q = refs[12:15]
    out_q, out_o, out_s, out_kv, tokens = refs[15:20]
    dws, nears, fars, lines = refs[20:23], refs[23:26], refs[26:29], refs[29:32]
    source, first, line, first_k, line_k, sum_k, d_qkv, dnorm, take = refs[32:41]
    held_d, held_q, tail, pool, total_m, own_sums = refs[41:47]
    load, send, recv_c, recv_y, recv_z, recv_tx, recv_t, recv_kx, recv_k, recv_n, recv_x = refs[47:]
    f, y, core, twin, across = fsdp_place(fs)
    z, x = lax.axis_index("context"), lax.axis_index("tensor")
    chips = fs // 2
    rows = low_t.shape[2]
    beside = [lax.rem(x + d, ten) for d in range(1, ten)]
    rows_of = [lax.rem(y + d, chips) for d in range(chips)]
    chip_order = rows_of[1:] + rows_of[:1]
    nxt, prv = lax.rem(z + 1, ctx), lax.rem(z + ctx - 1, ctx)
    greet([{"context": nxt}, {"context": prv}] + across + [twin] + [{"tensor": k} for k in beside])
    out = Sends(send)
    order = ends_first(ctx)
    kinds = (cast, cast, lambda v: v)
    heads = d_query.shape[1]
    rights = (d_qkv, att)
    lefts = (low_t, dmid_t)

    def start(w):
        for row in chip_order:
            owner = row * 2 + 1 - core
            if w < 2:
                fill_product(dws[w], lefts[w], rights[w], owner, ctx)
            out.push(dws[w].at[owner], nears[w].at[row], recv_c.at[w, row], twin)
        if w < 2:
            for row in chip_order:
                fill_product(dws[w], lefts[w], rights[w], row * 2 + core, ctx)

    def over_chips(w):
        for k, row in enumerate(rows_of[1:]):
            arrived(nears[w].at[row], recv_c.at[w, row], twin)
            for owner in order:
                mine = dws[w].at[row * 2 + core, owner]
                mine[...] = kinds[w](mine[...].astype(single) + nears[w][row, owner].astype(single))
                out.push(mine, fars[w].at[k, owner], recv_y.at[w, k, owner], across[k])

    def over_context(w, d):
        if d == 0:
            arrived(nears[w].at[y], recv_c.at[w, y], twin)
        owner = order[d]
        mine = dws[w].at[f, owner]
        for k in range(chips - 1):
            arrived(fars[w].at[k, owner], recv_y.at[w, k, owner], twin)

        def gathered():
            total = mine[...].astype(single) + nears[w][y, owner].astype(single)
            for k in range(chips - 1):
                total = total + fars[w][k, owner].astype(single)
            return total

        def done(v):
            mine[...] = kinds[w](v)

        line_sum(
            z, ctx, owner, gathered, mine, lines[w], recv_z.at[w], out, kinds[w], done
        )

    def finish(w):
        def add(v):
            dws[w][f, z] = kinds[w](dws[w][f, z].astype(single) + v)

        line_end(z, ctx, lines[w], recv_z.at[w], add)
        return dws[w][f, z]

    own_sums[...] = own[...]
    token_start(own_sums, first_k, recv_kx, out, beside, order)
    start(1)
    token_products(source, hid, slice_d, held_d, load)
    token_start(source, first, recv_tx, out, beside, order)
    over_chips(1)

    def keep_k(v):
        sum_k[...] = v

    def add_k(v):
        sum_k[...] += v

    for owner in order:
        token_step(owner, own_sums, first_k, recv_kx, line_k, recv_k, z, x, ctx, out, keep_k)
    line_end(z, ctx, line_k, recv_k, add_k)
    summed = sum_k[...]
    half = summed.shape[1] // 2
    a, b = summed[:, :half], summed[:, half:]
    c, s = cosine[...], sine[...]
    is_key = x == 0
    d_qkv[:, :heads] = d_query[...]
    d_qkv[:, heads : heads + half] = cast(jnp.where(is_key, a * c + b * s, a))
    d_qkv[:, heads + half :] = cast(jnp.where(is_key, b * c - a * s, b))
    start(0)
    over_chips(0)
    token_products(dnorm, d_qkv, slice_q, held_q, load)
    for other in beside:
        out.push(dnorm.at[0, other], take.at[x], recv_n.at[x], {"tensor": other})

    def keep_m(v):
        total_m[...] = v

    def add_m(v):
        total_m[...] += v

    for d, owner in enumerate(order):
        token_step(owner, source, first, recv_tx, line, recv_t, z, x, ctx, out, keep_m)
        over_context(1, d)
    dnorm_one = dnorm[0, x].astype(single)
    for other in beside:
        arrived(take.at[other], recv_n.at[other], twin)
        dnorm_one = dnorm_one + take[other].astype(single)
    values = hidden[...]
    inverse = lax.rsqrt(jnp.mean(values * values, axis=-1, keepdims=True) + norm_eps)
    normed = values * inverse
    dnormed = dnorm_one * (1.0 + scale[...])
    tokens[x, 1] = cast(
        dmid[...]
        + inverse * (dnormed - normed * jnp.mean(dnormed * normed, axis=-1, keepdims=True))
    )
    sums = jnp.sum(dnorm_one * normed, axis=0, keepdims=True)
    dws[2][...] = jnp.zeros_like(dws[2])
    for j in range(fs * ctx):
        at = slice(j * rows, (j + 1) * rows)
        dws[2][j // ctx, j % ctx, 0:1, :rows] = sums[:, at]
        dws[2][j // ctx, j % ctx, 1:2, :rows] = terms[:, at]
    start(2)
    line_end(z, ctx, line, recv_t, add_m)
    tokens[x, 0] = cast(mid[...] + total_m[...])
    for other in beside:
        out.push(tokens.at[x], tokens.at[x], recv_x.at[0, x], {"tensor": other})
    over_chips(2)
    for d in range(ctx):
        over_context(2, d)
        over_context(0, d)
    pool[x] = finish(2)
    for other in beside:
        out.push(pool.at[x], pool.at[x], recv_x.at[1, x], {"tensor": other})
    grad = finish(0)
    out_q[...] = grad[:, :heads].astype(single)
    tail[x] = grad[:, heads:]
    for other in beside:
        out.push(tail.at[x], tail.at[x], recv_x.at[2, x], {"tensor": other})
    out_o[...] = finish(1).astype(single)
    for other in beside:
        arrived(tokens.at[other], recv_x.at[0, other], twin)
        arrived(pool.at[other], recv_x.at[1, other], twin)
        arrived(tail.at[other], recv_x.at[2, other], twin)
    total = pool[0]
    for k in range(1, ten):
        total = total + pool[k]
    out_s[...] = total
    columns = tail.shape[-1]
    for k in range(ten):
        out_kv[:, k * columns : (k + 1) * columns] = tail[k].astype(single)
    out.drain()


def attn_back(
    low_t, dmid_t, d_query, att, own, cosine, sine, hidden, mid, dmid, scale, terms, hid, slice_d, slice_q,
    fs, ctx, ten, ident,
):
    rows = low_t.shape[2]
    t_rows, width = mid.shape
    chips = fs // 2
    heads = d_query.shape[1]
    count, tail = own.shape[2:]
    lanes = -(-rows // 128) * 128
    both = [
        ((rows, heads + tail), half_type),
        ((rows, att.shape[1]), half_type),
        ((8, lanes), single),
    ]
    sends = (
        2 * (ctx * (ten - 1) + 2 * ctx)
        + 4 * (ten - 1)
        + 3 * (chips + (chips - 1) * ctx + 2 * ctx)
    )
    dma = pltpu.SemaphoreType.DMA
    shape = jax.ShapeDtypeStruct
    return pl.pallas_call(
        functools.partial(attn_kernel, fs, ctx, ten),
        out_shape=[
            shape((rows, heads), single),
            shape((rows, att.shape[1]), single),
            shape((8, lanes), single),
            shape((rows, ten * tail), single),
            shape((ten, 2, t_rows, width), half_type),
        ],
        in_specs=[VMEM] * 13 + [ANY] * 2,
        out_specs=[VMEM] * 5,
        scratch_shapes=[pltpu.VMEM((fs, ctx, *b), t) for b, t in both]
        + [pltpu.VMEM((chips, ctx, *b), t) for b, t in both]
        + [pltpu.VMEM((chips - 1, ctx, *b), t) for b, t in both]
        + [pltpu.VMEM((ctx + 1, *b), t) for b, t in both]
        + [
            pltpu.VMEM((ctx, ten, t_rows, width), half_type),
            pltpu.VMEM((ten - 1, ctx, t_rows, width), half_type),
            pltpu.VMEM((ctx + 1, t_rows, width), half_type),
            pltpu.VMEM((ten - 1, ctx, count, tail), half_type),
            pltpu.VMEM((ctx + 1, count, tail), half_type),
            pltpu.VMEM((count, tail), single),
            pltpu.VMEM((count, heads + tail), half_type),
            pltpu.VMEM((1, ten, t_rows, width), half_type),
            pltpu.VMEM((ten, t_rows, width), half_type),
            pltpu.VMEM((2, 2, ctx, *slice_d.shape[2:]), half_type),
            pltpu.VMEM((2, 2, ctx, *slice_q.shape[2:]), half_type),
            pltpu.VMEM((ten, rows, tail), half_type),
            pltpu.VMEM((ten, 8, lanes), single),
            pltpu.VMEM((t_rows, width), single),
            pltpu.VMEM(own.shape, half_type),
            dma((2,)),
            dma((sends,)),
            dma((3, chips)),
            dma((3, chips - 1, ctx)),
            dma((3, ctx + 1)),
            dma((ten - 1, ctx)),
            dma((ctx + 1,)),
            dma((ten - 1, ctx)),
            dma((ctx + 1,)),
            dma((ten,)),
            dma((3, ten)),
        ],
        compiler_params=pltpu.CompilerParams(
            collective_id=ident, has_side_effects=True, vmem_limit_bytes=VMEM_ALL
        ),
        name=f"attn_back_{ident}",
    )(low_t, dmid_t, d_query, att, own, cosine, sine, hidden, mid, dmid, scale, terms, hid, slice_d, slice_q)


def on_device(hidden_in, cotangent, segment_ids, positions, *params):
    masters, firsts, seconds = params[:8], params[8:16], params[16:]
    (
        attn_scale,
        query_weight,
        keyval_weight,
        output_weight,
        mlp_scale,
        gate_weight,
        up_weight,
        down_weight,
    ) = masters
    fs, ctx, ten = (lax.axis_size(name) for name in ("fsdp", "context", "tensor"))
    x = lax.axis_index("tensor")
    context_index = lax.axis_index("context")
    block, width = hidden_in.shape[1:]
    rows = query_weight.shape[0]
    half_rows = block // ten
    heads_width = query_weight.shape[1]
    heads_here = heads_width // HD
    hidden = hidden_in[0]
    cot = cotangent[0]
    hidden_half = lax.dynamic_slice_in_dim(hidden, x * half_rows, half_rows, 0)
    cot_half = lax.dynamic_slice_in_dim(cot, x * half_rows, half_rows, 0)
    is_key = x == 0

    qkv_block = jnp.concatenate(
        [
            cast(query_weight),
            cast(lax.dynamic_slice_in_dim(keyval_weight, x * HD, HD, 1)),
        ],
        axis=1,
    )
    lanes = -(-max(rows, block) // 128) * 128
    wide = [
        jnp.pad(v, (0, lanes - v.shape[0]))
        for v in (attn_scale, mlp_scale, segment_ids[0].astype(single))
    ]
    small = jnp.stack(wide + [jnp.zeros((lanes,), single)] * 5)
    small_all, qkv_all, out_all, dy_all, part_p, part_d = spread(
        [small, qkv_block, cast(output_weight.T)],
        cast(cot_half),
        [gate_weight, up_weight, down_weight.T],
        fs,
        ctx,
        ten,
        1,
    )
    scale_one = cast(small_all[:, :, 0, :rows].reshape(-1)).astype(single)
    scale_two = cast(small_all[:, :, 1, :rows].reshape(-1)).astype(single)
    f = lax.axis_index("fsdp")
    seg_all = lax.dynamic_index_in_dim(small_all[:, :, 2, :block], f, 0, False).reshape(-1)
    qkv_full = qkv_all.reshape(width, -1)
    out_full = out_all.reshape(width, -1)

    _, _, low_one = rms_forward(hidden, scale_one)
    qkv = dot(low_one, qkv_full, ((1,), (0,)))
    query = qkv[:, :heads_width].reshape(block, heads_here, HD)
    own = qkv[:, heads_width:]
    cosine, sine = rope_tables(positions[0])
    query_low = cast(rotate(query, cosine[:, None, :], sine[:, None, :]) * HD ** (-0.5))
    own_low = cast(jnp.where(is_key, rotate(own, cosine, sine), own))
    keyval_all = tokens_to_all(own_low, ctx, ten, 2).reshape(ctx, ten, block, HD)
    keys_all = keyval_all[:, 0].reshape(-1, HD)
    values_all = keyval_all[:, 1].reshape(-1, HD)
    rows_index = context_index * block + jnp.arange(block, dtype=jnp.int32)
    cols_index = jnp.arange(keys_all.shape[0], dtype=jnp.int32)
    allowed = (rows_index[:, None] >= cols_index[None, :]) & (
        segment_ids[0].astype(single)[:, None] == seg_all[None, :]
    )
    scores = jnp.einsum("bhd,jd->hbj", query_low, keys_all, preferred_element_type=single)
    masked = jnp.where(allowed, scores, masked_value)
    top = jnp.max(masked, axis=-1, keepdims=True)
    total = jnp.sum(jnp.where(allowed, jnp.exp(masked - top), 0.0), axis=-1, keepdims=True)
    lse = top + jnp.log(total)
    prob = jnp.where(allowed, jnp.exp(masked - lse), 0.0)
    prob_low = cast(prob)
    att_low = cast(
        jnp.einsum("hbj,jd->bhd", prob_low, values_all, preferred_element_type=single)
    )
    att_flat = att_low.reshape(block, heads_width)
    attn_part = dot(att_flat, out_full, ((1,), (1,)))
    slice_p, slice_d, hid, dpair, low_t, dy_t, mid_half, _ = mlp_forward(
        cast(attn_part).reshape(ten, half_rows, width),
        hidden_half,
        scale_two[None],
        dy_all,
        part_p,
        part_d,
        fs,
        ctx,
        ten,
        4,
    )
    dmid_half, dmid_low, terms_two, part_p, part_d = mlp_back(
        low_t, dy_t, hid, dpair, mid_half, cot_half, scale_two[None], slice_p, fs, ctx, ten, 5
    )

    dmid_low = dmid_low.reshape(block, width)
    datt_low = cast(dot(dmid_low, out_full, ((1,), (0,)))).reshape(block, heads_here, HD)
    delta = jnp.einsum("bhd,bhd->hb", datt_low, att_low, preferred_element_type=single)
    dprob = jnp.einsum("bhd,jd->hbj", datt_low, values_all, preferred_element_type=single)
    dscore_low = cast(prob * (dprob - delta[..., None]))
    dquery = jnp.einsum("hbj,jd->bhd", dscore_low, keys_all, preferred_element_type=single)
    dkey_part = jnp.einsum("hbj,bhd->jd", dscore_low, query_low, preferred_element_type=single)
    dvalue_part = jnp.einsum("hbj,bhd->jd", prob_low, datt_low, preferred_element_type=single)
    own_part = jnp.stack(
        [cast(part).reshape(ctx, block, HD) for part in (dkey_part, dvalue_part)], axis=1
    )
    dquery_low = cast(
        unrotate(dquery, cosine[:, None, :], sine[:, None, :]) * HD ** (-0.5)
    ).reshape(block, heads_width)
    row_blocks = (fs, ctx, rows, -1)
    grad_wq, grad_wo, grad_s, grad_wkv, outs = attn_back(
        low_one.T.reshape(row_blocks),
        dmid_low.T.reshape(row_blocks),
        dquery_low,
        att_flat,
        own_part,
        cosine,
        sine,
        hidden_half,
        mid_half,
        dmid_half,
        scale_one[None],
        terms_two,
        hid,
        slice_d,
        qkv_all,
        fs,
        ctx,
        ten,
        9,
    )
    outs = outs.transpose(1, 0, 2, 3).reshape(2, 1, block, width).astype(single)

    grads = (grad_s[0, :rows], grad_wq, grad_wkv, grad_wo.T, grad_s[1, :rows])
    results = [
        (grad, *adamw(weight, grad, first, second))
        for weight, grad, first, second in zip(masters, grads, firsts, seconds)
    ]
    results += [
        update(part_p, 0, gate_weight, firsts[5], seconds[5], 5),
        update(part_p, 1, up_weight, firsts[6], seconds[6], 6),
        [v.T for v in update(part_d, 0, down_weight.T, firsts[7].T, seconds[7].T, 7)],
    ]
    return (
        outs[0],
        outs[1],
        *(entry[0] for entry in results),
        *(entry[1] for entry in results),
        *(entry[2] for entry in results),
        *(entry[3] for entry in results),
    )


def solution(mesh):
    both = ("fsdp", "context")
    tokens = P("fsdp", "context", None)
    weights = (
        P(both),
        P(both, "tensor"),
        P(both, None),
        P("tensor", both),
        P(both),
        P(both, "tensor"),
        P(both, "tensor"),
        P("tensor", both),
    )
    return jax.shard_map(
        on_device,
        mesh=mesh,
        in_specs=(tokens, tokens, P("fsdp", "context"), P("fsdp", "context"), *(weights * 3)),
        out_specs=(tokens, tokens, *(weights * 4)),
        check_vma=False,
    )
```

```python
import functools

import jax
import jax.numpy as jnp
from jax import lax
from jax.experimental import pallas as pl
from jax.experimental.pallas import tpu as pltpu
from jax.sharding import PartitionSpec as P

HD = 256


norm_eps = 1e-06
beta_one = 0.9
beta_two = 0.999
adam_eps = 1e-08
learn_rate = 0.03
decay_rate = 0.1
adam_step = 4.0
rope_base = 10000.0
masked_value = -1e30

single = jnp.float32
half_type = jnp.bfloat16


def gelu_tanh(values):
    return jax.nn.gelu(values, approximate=True)


def rope_tables(positions):
    half = HD // 2
    freq = rope_base ** (-2.0 * jnp.arange(half).astype(jnp.float32) / HD)
    angle = positions.astype(jnp.float32)[..., None] * freq
    return (jnp.cos(angle), jnp.sin(angle))


def rotate(values, cosine, sine):
    half = values.shape[-1] // 2
    first = values[..., :half]
    second = values[..., half:]
    return jnp.concatenate(
        [first * cosine - second * sine, second * cosine + first * sine], axis=-1
    )


def unrotate(values, cosine, sine):
    half = values.shape[-1] // 2
    first = values[..., :half]
    second = values[..., half:]
    return jnp.concatenate(
        [first * cosine + second * sine, second * cosine - first * sine], axis=-1
    )


def rms_forward(values, scale):
    inverse = lax.rsqrt(jnp.mean(values * values, axis=-1, keepdims=True) + norm_eps)
    normed = values * inverse
    return (normed, inverse, (normed * (1.0 + scale)).astype(jnp.bfloat16))


def rms_backward(dnorm, normed, inverse, scale):
    dnormed = dnorm * (1.0 + scale)
    dvalues = inverse * (dnormed - normed * jnp.mean(dnormed * normed, axis=-1, keepdims=True))
    return (dvalues, dnorm * normed)


def adamw(weight, grad, first, second):
    first_new = beta_one * first + (1.0 - beta_one) * grad
    second_new = beta_two * second + (1.0 - beta_two) * grad * grad
    fix_one = 1.0 - beta_one**adam_step
    fix_two = 1.0 - beta_two**adam_step
    update = first_new / fix_one / (jnp.sqrt(second_new / fix_two) + adam_eps)
    return (weight - learn_rate * (update + decay_rate * weight), first_new, second_new)


def dot(a, b, dims):
    return lax.dot_general(a, b, (dims, ((), ())), preferred_element_type=single)


MESH = pl.DeviceIdType.MESH
ANY = pl.BlockSpec(memory_space=pl.ANY)
VMEM = pl.BlockSpec(memory_space=pltpu.VMEM)


def greet(peers):
    barrier = pltpu.get_barrier_semaphore()
    for peer in peers:
        pl.semaphore_signal(barrier, inc=1, device_id=peer, device_id_type=MESH)
    pl.semaphore_wait(barrier, len(peers))


def remote(src, dst, send, recv, peer):
    return pltpu.make_async_remote_copy(
        src_ref=src, dst_ref=dst, send_sem=send, recv_sem=recv, device_id=peer, device_id_type=MESH
    )


def arrived(dst, recv, peer):
    remote(dst, dst, recv, recv, peer).wait_recv()


def fsdp_place(fs):
    f = lax.axis_index("fsdp")
    core = lax.rem(f, 2)
    y = lax.div(f, 2)
    twin = {"fsdp": f + 1 - 2 * core}
    across = [{"fsdp": lax.rem(y + d, fs // 2) * 2 + core} for d in range(1, fs // 2)]
    return f, y, core, twin, across


class Sends:
    def __init__(self, send):
        self.send, self.made = send, []

    def push(self, src, dst, recv, peer, *conditions):
        copy = remote(src, dst, self.send.at[len(self.made)], recv, peer)
        self.made.append((copy, conditions))
        under(conditions, copy.start)

    def drain(self):
        for copy, conditions in self.made:
            under(conditions, copy.wait_send)


def under(conditions, action):
    if not conditions:
        action()
        return
    holds = conditions[0]
    for more in conditions[1:]:
        holds = jnp.logical_and(holds, more)
    pl.when(holds)(action)


def line_steps(z, ctx):
    for s in range(1, ctx):
        yield z - s, z >= s, z + 1, z + 1 < ctx
        yield z + s, z + s < ctx, z - 1, z >= 1


def tokens_kernel(ctx, ten, src, out, local, send, recv):
    z, x = lax.axis_index("context"), lax.axis_index("tensor")
    around = [lax.rem(z + d, ctx) for d in range(ctx)]
    across = [{"tensor": lax.rem(x + d, ten)} for d in range(1, ten)]
    greet([{"context": k} for k in around[1:]] + across)
    sends = []

    def push(ref, source, peer):
        copy = remote(ref, out.at[source, x], send.at[len(sends)], recv.at[source, x], peer)
        copy.start()
        sends.append(copy)

    for d in range(1, ctx):
        push(src, z, {"context": around[d]})
    for peer in across:
        push(src, z, peer)
    keep = pltpu.make_async_copy(src, out.at[z, x], local)
    keep.start()
    back = [lax.rem(z + ctx - d, ctx) for d in range(ctx)]
    for d in range(1, ctx):
        arrived(out.at[back[d], x], recv.at[back[d], x], {"context": back[d]})
        for peer in across:
            push(out.at[back[d], x], back[d], peer)
    for d in range(ctx):
        for peer in across:
            other = peer["tensor"]
            arrived(out.at[back[d], other], recv.at[back[d], other], peer)
    keep.wait()
    for copy in sends:
        copy.wait_send()


def tokens_to_all(block, ctx, ten, ident):
    sends = (ctx - 1) + ctx * (ten - 1)
    out = pl.pallas_call(
        functools.partial(tokens_kernel, ctx, ten),
        out_shape=jax.ShapeDtypeStruct((ctx, ten, *block.shape), block.dtype),
        in_specs=[VMEM],
        out_specs=VMEM,
        scratch_shapes=[
            pltpu.SemaphoreType.DMA(()),
            pltpu.SemaphoreType.DMA((sends,)),
            pltpu.SemaphoreType.DMA((ctx, ten)),
        ],
        compiler_params=pltpu.CompilerParams(collective_id=ident, has_side_effects=True),
        name=f"tokens_{ident}",
    )(block)
    return out.reshape(-1, block.shape[-1])


VMEM_ALL = 67043328


def cast(v):
    return v.astype(half_type)


def fill_product(dw, left, right, owner, ctx):
    def one(k, carry):
        dw[owner, k] = cast(
            lax.dot_general(
                left[owner, k], right[...], (((1,), (0,)), ((), ())), preferred_element_type=single
            )
        )
        return carry

    lax.fori_loop(0, ctx, one, 0)


def split_columns(ctx, weights, parts, wide, packed, small, load, store):
    columns = small.shape[-1]
    fetches = [pltpu.make_async_copy(weights[w], wide.at[w], load.at[w]) for w in range(3)]
    for fetch in fetches:
        fetch.start()
    for w in range(3):
        fetches[w].wait()
        for k in range(ctx):
            piece = cast(wide[w, :, k * columns : (k + 1) * columns])
            if w < 2:
                packed[k, :, w * columns : (w + 1) * columns] = piece
            else:
                small[k] = piece
    puts = [pltpu.make_async_copy(v, parts[j], store.at[j]) for j, v in enumerate((packed, small))]
    for put in puts:
        put.start()
    for put in puts:
        put.wait()


def first_kernel(fs, ctx, ten, count, *refs):
    srcs, weights = refs[: count + 1], refs[count + 1 : count + 4]
    refs = refs[count + 4 :]
    outs, parts = refs[: count + 1], refs[count + 1 : count + 3]
    wide, packed, small, load, store, local, send, recv, recv_t = refs[count + 3 :]
    f, y, core, twin, across = fsdp_place(fs)
    z, x = lax.axis_index("context"), lax.axis_index("tensor")
    beside = [{"tensor": lax.rem(x + d, ten)} for d in range(1, ten)]
    back = [lax.rem(z + ctx - d, ctx) for d in range(ctx)]
    up, down = {"context": z + 1}, {"context": z - 1}
    nxt, prv = lax.rem(z + 1, ctx), back[1]
    greet([{"context": nxt}, {"context": prv}] + across + [twin] + beside)
    out = Sends(send)
    keeps = []

    def where(w, source):
        if w == count:
            return outs[w].at[source, x], recv_t.at[source, x], beside
        return outs[w].at[f, source], recv.at[w, f, source], across + [twin]

    for w in range(count + 1):
        mine, sem, peers = where(w, z)
        out.push(srcs[w], mine, sem, up, z + 1 < ctx)
        out.push(srcs[w], mine, sem, down, z >= 1)
        for peer in peers:
            out.push(srcs[w], mine, sem, peer)
        keeps.append(pltpu.make_async_copy(srcs[w], mine, local.at[w]))
        keeps[-1].start()
    split_columns(ctx, weights, parts, wide, packed, small, load, store)
    for source, exists, onward, more in line_steps(z, ctx):
        for w in range(count + 1):
            block, sem, peers = where(w, source)
            under((exists,), lambda: arrived(block, sem, twin))
            out.push(block, block, sem, {"context": onward}, exists, more)
            for peer in peers:
                out.push(block, block, sem, peer, exists)
    chain = [(z, ())] + [(source, (exists,)) for source, exists, _, _ in line_steps(z, ctx)]
    for source, when in chain:
        for w in range(count):
            for peer in across:
                owner = peer["fsdp"]
                block, sem = outs[w].at[owner, source], recv.at[w, owner, source]
                under(when, lambda: arrived(block, sem, twin))
                out.push(block, block, sem, twin, *when)
    for source in back:
        for w in range(count):
            for step in range(fs // 2):
                owner = lax.rem(y + step, fs // 2) * 2 + 1 - core
                arrived(outs[w].at[owner, source], recv.at[w, owner, source], twin)
        for peer in beside:
            arrived(outs[count].at[source, peer["tensor"]], recv_t.at[source, peer["tensor"]], twin)
    for keep in keeps:
        keep.wait()
    out.drain()


def spread(blocks, tokens, weights, fs, ctx, ten, ident):
    count = len(blocks)
    chips = fs // 2
    lines = 2 + 2 * (ctx - 1)
    sends = count * (lines + (2 * ctx - 1) * (2 * chips - 1)) + lines + (2 * ctx - 1) * (ten - 1)
    rows, wide = weights[0].shape
    part = (ctx, rows, wide // ctx)
    pair = (ctx, rows, 2 * (wide // ctx))
    dma = pltpu.SemaphoreType.DMA
    return pl.pallas_call(
        functools.partial(first_kernel, fs, ctx, ten, count),
        out_shape=[jax.ShapeDtypeStruct((fs, ctx, *b.shape), b.dtype) for b in blocks]
        + [jax.ShapeDtypeStruct((ctx, ten, *tokens.shape), tokens.dtype)]
        + [jax.ShapeDtypeStruct(pair, half_type), jax.ShapeDtypeStruct(part, half_type)],
        in_specs=[ANY] * (count + 4),
        out_specs=[ANY] * (count + 3),
        scratch_shapes=[
            pltpu.VMEM((3, rows, wide), single),
            pltpu.VMEM(pair, half_type),
            pltpu.VMEM(part, half_type),
            dma((3,)),
            dma((2,)),
            dma((count + 1,)),
            dma((sends,)),
            dma((count, fs, ctx)),
            dma((ctx, ten)),
        ],
        compiler_params=pltpu.CompilerParams(
            collective_id=ident, has_side_effects=True, vmem_limit_bytes=VMEM_ALL
        ),
        name=f"spread_{ident}",
    )(*blocks, tokens, *weights)


def flip(k, bit):
    return k + bit - 2 * bit * lax.rem(lax.div(k, bit), 2)


def halving(z, ctx):
    sends, seen, base, bit = [], [], 0, 1
    while bit < ctx:
        count = ctx // (2 * bit)
        for u in range(count):
            owner = flip(z, bit) - 2 * bit * lax.div(z, 2 * bit) + 2 * bit * u
            sends.append((owner, flip(z, bit), base + u, [at + lax.div(owner, d) for at, d in seen]))
        seen.append((base, 2 * bit))
        base, bit = base + count, 2 * bit
    return sends, [at + lax.div(z, d) for at, d in seen]


def doubling(z, ctx):
    steps, held, bit = [], [z], ctx // 2
    while bit:
        got = [flip(k, bit) for k in held]
        steps.append((flip(z, bit), list(held), got))
        held, bit = held + got, bit // 2
    return steps


def collect(total, slots, sem, places, peer):
    for at in places:
        arrived(slots.at[at], sem.at[at], peer)
        total = total + slots[at].astype(single)
    return total


def chip_tiles(weight, held, load, use):
    chips = weight.shape[0] // 2

    def fetch(k, slot):
        return pltpu.make_async_copy(weight.at[pl.ds(2 * k, 2)], held.at[slot], load.at[slot])

    fetch(0, 0).start()

    def step(k, carry):
        slot = lax.rem(k, 2)
        fetch(k, slot).wait()

        @pl.when(k + 1 < chips)
        def _():
            fetch(k + 1, 1 - slot).start()

        use(k, held[slot].reshape(-1, held.shape[-1]))
        return carry

    lax.fori_loop(0, chips, step, 0)


def forward_kernel(fs, ctx, ten, *refs):
    attn, hidden, scale, dy, part_p, part_d = refs[:6]
    slice_p, slice_d, hid, dpair, low_t, dy_t, mid, low = refs[6:14]
    low_all, take, held_p, held_d, sums_p, sums_d = refs[14:20]
    load, local, send, recv_p, recv_d, recv_t, recv_x = refs[20:]
    f, y, core, twin, across = fsdp_place(fs)
    z, x = lax.axis_index("context"), lax.axis_index("tensor")
    rows, columns = part_d.shape[1:]
    width = low.shape[1]
    count = hid.shape[0]
    beside = [{"tensor": lax.rem(x + d, ten)} for d in range(1, ten)]
    around = [lax.rem(z + d, ctx) for d in range(ctx)]
    back = [lax.rem(z + ctx - d, ctx) for d in range(ctx)]
    greet([{"context": k} for k in around[1:]] + across + [twin] + beside)
    out = Sends(send)
    parts, slices, recvs = (part_p, part_d), (slice_p, slice_d), (recv_p, recv_d)
    for peer in beside:
        out.push(attn.at[peer["tensor"]], take.at[x], recv_x.at[x], peer)

    def block(w, owner, source):
        return slices[w].at[owner, source], recvs[w].at[owner, source]

    def to_context(w, d):
        dst, sem = block(w, f, z)
        out.push(parts[w].at[around[d]], dst, sem, {"context": around[d]})

    def from_context(w, d):
        dst, sem = block(w, f, back[d])
        arrived(dst, sem, twin)
        for peer in across + [twin]:
            out.push(dst, dst, sem, peer)

    def from_chips(w):
        for d in range(ctx):
            for peer in across:
                dst, sem = block(w, peer["fsdp"], back[d])
                arrived(dst, sem, twin)
                out.push(dst, dst, sem, twin)

    def from_twin(w):
        for d in range(ctx):
            for step in range(fs // 2):
                dst, sem = block(w, lax.rem(y + step, fs // 2) * 2 + 1 - core, back[d])
                arrived(dst, sem, twin)

    to_context(0, 1)
    keeps = []
    for w in range(2):
        dst, sem = block(w, f, z)
        for peer in across + [twin]:
            out.push(parts[w].at[z], dst, sem, peer)
        keeps.append(pltpu.make_async_copy(parts[w].at[z], dst, local.at[w]))
        keeps[-1].start()
    total = hidden[...] + attn[x].astype(single)
    for peer in beside:
        other = peer["tensor"]
        arrived(take.at[other], recv_x.at[other], twin)
        total = total + take[other].astype(single)
    mid[...] = total
    inverse = lax.rsqrt(jnp.mean(total * total, axis=-1, keepdims=True) + norm_eps)
    low_all[z, x] = cast(total * inverse * (1.0 + scale[...]))
    mine = low_all.at[z, x]
    later = [(0, d) for d in range(2, ctx)] + [(1, d) for d in range(1, ctx)]
    early = [d for d in range(1, ctx)]
    steps = doubling(z, ctx)
    for partner, _, _ in steps:
        out.push(mine, mine, recv_t.at[z, x], {"context": partner})
    for peer in beside:
        out.push(mine, mine, recv_t.at[z, x], peer)
    to_context(*later.pop(0))
    for step, (partner, _, got) in enumerate(steps):
        for source in got:
            here, sem = low_all.at[source, x], recv_t.at[source, x]
            arrived(here, sem, twin)
            for further, _, _ in steps[step + 1 :]:
                out.push(here, here, sem, {"context": further})
            for peer in beside:
                out.push(here, here, sem, peer)
            if early:
                from_context(0, early.pop(0))
            if later:
                to_context(*later.pop(0))
    while later:
        to_context(*later.pop(0))
    while early:
        from_context(0, early.pop(0))

    def turned(dst, src):
        for j in range(fs * ctx):
            piece = src[:, :, :, j * rows : (j + 1) * rows].reshape(count, rows)
            dst[j // ctx, j % ctx] = piece.T

    def product(weight, held, left, sums):
        deep = width // (fs // 2)

        def use(k, tile):
            lanes = pl.ds(pl.multiple_of(k * deep, deep), deep)
            add = jnp.dot(
                left[:, :, :, lanes].reshape(count, deep), tile, preferred_element_type=single
            )

            @pl.when(k == 0)
            def _():
                sums[...] = add

            @pl.when(k > 0)
            def _():
                sums[...] += add

        chip_tiles(weight, held, load, use)

    from_chips(0)
    turned(dy_t, dy)
    from_context(1, 1)
    for source in back:
        for peer in beside:
            other = peer["tensor"]
            arrived(low_all.at[source, other], recv_t.at[source, other], twin)
    from_twin(0)
    keeps[0].wait()
    turned(low_t, low_all)
    for d in range(2, ctx):
        from_context(1, d)
    product(slice_p, held_p, low_all, sums_p)
    from_chips(1)
    from_twin(1)
    keeps[1].wait()
    product(slice_d, held_d, dy, sums_d)
    low[...] = low_all[z, x]
    root = (2.0 / jnp.pi) ** 0.5
    part = count // ctx

    def finish(k, carry):
        here = pl.ds(pl.multiple_of(k * part, part), part)
        pair, dhid = sums_p[here, :], sums_d[here, :]
        gate, upper = pair[:, :columns], pair[:, columns:]
        square = gate * gate
        tanh = jnp.tanh(root * gate * (1.0 + 0.044715 * square))
        gelu = 0.5 * gate * (1.0 + tanh)
        slope = 0.5 * (1.0 + tanh) + 0.5 * gate * (1.0 - tanh * tanh) * root * (
            1.0 + 3.0 * 0.044715 * square
        )
        hid[here, :] = cast(gelu * upper)
        dpair[here, :columns] = cast(dhid * upper * slope)
        dpair[here, columns:] = cast(dhid * gelu)
        return carry

    lax.fori_loop(0, ctx, finish, 0)
    out.drain()


def mlp_forward(attn, hidden, scale, dy_all, part_p, part_d, fs, ctx, ten, ident):
    rows, columns = part_d.shape[1:]
    t_rows, width = hidden.shape
    count = ctx * ten * t_rows
    chips = fs // 2
    sends = 2 * (ten - 1) + 2 * ctx + 2 * (ctx - 1) * (ten - 1) + 2 * (3 * ctx - 1 + 3 * ctx * chips)
    dma = pltpu.SemaphoreType.DMA
    shape = jax.ShapeDtypeStruct
    return pl.pallas_call(
        functools.partial(forward_kernel, fs, ctx, ten),
        out_shape=[
            shape((fs, ctx, rows, 2 * columns), half_type),
            shape((fs, ctx, rows, columns), half_type),
            shape((count, columns), half_type),
            shape((count, 2 * columns), half_type),
            shape((fs, ctx, rows, count), half_type),
            shape((fs, ctx, rows, count), half_type),
            shape((t_rows, width), single),
            shape((t_rows, width), half_type),
        ],
        in_specs=[VMEM] * 4 + [ANY] * 2,
        out_specs=[ANY] * 2 + [VMEM] * 6,
        scratch_shapes=[
            pltpu.VMEM((ctx, ten, t_rows, width), half_type),
            pltpu.VMEM((ten, t_rows, width), half_type),
            pltpu.VMEM((2, 2, ctx, rows, 2 * columns), half_type),
            pltpu.VMEM((2, 2, ctx, rows, columns), half_type),
            pltpu.VMEM((count, 2 * columns), single),
            pltpu.VMEM((count, columns), single),
            dma((2,)),
            dma((2,)),
            dma((sends,)),
            dma((fs, ctx)),
            dma((fs, ctx)),
            dma((ctx, ten)),
            dma((ten,)),
        ],
        compiler_params=pltpu.CompilerParams(
            collective_id=ident, has_side_effects=True, vmem_limit_bytes=VMEM_ALL
        ),
        name=f"mlp_forward_{ident}",
    )(attn, hidden, scale, dy_all, part_p, part_d)


def token_products(source, left, weight, held, load):
    def use(k, tile):
        term = lax.dot_general(
            left[...], tile, (((1,), (1,)), ((), ())), preferred_element_type=single
        )
        deep = tile.shape[0]
        lanes = pl.ds(pl.multiple_of(k * deep, deep), deep)
        source[:, :, :, lanes] = cast(term).reshape(*source.shape[:3], deep)

    chip_tiles(weight, held, load, use)


def token_start(source, first, recv, out, beside, order):
    for owner in order:
        for k, other in enumerate(beside):
            out.push(
                source.at[owner, other], first.at[k, owner], recv.at[k, owner], {"tensor": other}
            )


def token_sum(owner, places, source, first, recv, slots, sem, x):
    total = source[owner, x].astype(single)
    for k in range(first.shape[0]):
        arrived(first.at[k, owner], recv.at[k, owner], {"tensor": x})
        total = total + first[k, owner].astype(single)
    return collect(total, slots, sem, places, {"tensor": x})


def token_send(send, source, first, recv, slots, sem, x, out):
    owner, partner, slot, places = send
    mine = source.at[owner, x]
    mine[...] = cast(token_sum(owner, places, source, first, recv, slots, sem, x))
    out.push(mine, slots.at[slot], sem.at[slot], {"context": partner})


def back_kernel(fs, ctx, ten, *refs):
    low_t, dy_t, hid, dpair, mid, cot, scale, slice_p = refs[:8]
    dmid, dmid_all, terms, out_p, out_d = refs[8:13]
    dws, nears, fars = refs[13:15], refs[15:17], refs[17:19]
    source, first, line, held = refs[19:23]
    load, local, send, recv_c, recv_y, recv_z, recv_tx, recv_t, recv_x = refs[23:]
    f, y, core, twin, across = fsdp_place(fs)
    z, x = lax.axis_index("context"), lax.axis_index("tensor")
    chips = fs // 2
    around = [lax.rem(z + d, ctx) for d in range(ctx)]
    beside = [lax.rem(x + d, ten) for d in range(1, ten)]
    rows_of = [lax.rem(y + d, chips) for d in range(chips)]
    chip_order = rows_of[1:] + rows_of[:1]
    order = around[1:] + around[:1]
    greet([{"context": k} for k in around[1:]] + across + [twin] + [{"tensor": k} for k in beside])
    out = Sends(send)
    outs = (out_d, out_p)
    keeps = []

    def products(w):
        left, right = (dy_t, low_t)[w], (hid, dpair)[w]
        for row in chip_order:
            fill_product(dws[w], left, right, row * 2 + 1 - core, ctx)
            out.push(dws[w].at[row * 2 + 1 - core], nears[w].at[row], recv_c.at[w, row], twin)
        for row in chip_order:
            fill_product(dws[w], left, right, row * 2 + core, ctx)

    def over_chips(w):
        for k, row in enumerate(rows_of[1:]):
            arrived(nears[w].at[row], recv_c.at[w, row], twin)
            for d, owner in enumerate(order):
                mine = dws[w].at[row * 2 + core, owner]
                mine[...] = cast(mine[...].astype(single) + nears[w][row, owner].astype(single))
                out.push(mine, fars[w].at[k, d], recv_y.at[w, k, d], across[k])

    def over_context(w, d):
        if d == 0:
            arrived(nears[w].at[y], recv_c.at[w, y], twin)
        owner = order[d]
        mine = dws[w].at[f, owner]
        total = mine[...].astype(single) + nears[w][y, owner].astype(single)
        for k in range(chips - 1):
            arrived(fars[w].at[k, d], recv_y.at[w, k, d], twin)
            total = total + fars[w][k, d].astype(single)
        mine[...] = cast(total)
        if d < ctx - 1:
            out.push(mine, outs[w].at[z], recv_z.at[w, z], {"context": owner})
        else:
            keep = pltpu.make_async_copy(mine, outs[w].at[z], local.at[w])
            keep.start()
            keeps.append(keep)

    sends, own_slots = halving(z, ctx)
    owners = [send[0] for send in sends] + [z]
    products(0)
    over_chips(0)
    token_products(source, dpair, slice_p, held, load)
    token_start(source, first, recv_tx, out, beside, owners)
    products(1)
    over_chips(1)
    for d, send_z in enumerate(sends):
        token_send(send_z, source, first, recv_tx, line, recv_t, x, out)
        over_context(0, d)
    over_context(0, ctx - 1)
    dnorm = token_sum(z, own_slots, source, first, recv_tx, line, recv_t, x)
    values = mid[...]
    inverse = lax.rsqrt(jnp.mean(values * values, axis=-1, keepdims=True) + norm_eps)
    normed = values * inverse
    dnormed = dnorm * (1.0 + scale[...])
    terms[...] = jnp.sum(dnorm * normed, axis=0, keepdims=True)
    total = cot[...] + inverse * (
        dnormed - normed * jnp.mean(dnormed * normed, axis=-1, keepdims=True)
    )
    dmid[...] = total
    dmid_all[x] = cast(total)
    for other in beside:
        out.push(dmid_all.at[x], dmid_all.at[x], recv_x.at[x], {"tensor": other})
    for d in range(ctx):
        over_context(1, d)
    for other in beside:
        arrived(dmid_all.at[other], recv_x.at[other], twin)
    for w in range(2):
        for k in around[1:]:
            arrived(outs[w].at[k], recv_z.at[w, k], twin)
    for keep in keeps:
        keep.wait()
    out.drain()


def mlp_back(low_t, dy_t, hid, dpair, mid, cot, scale, slice_p, fs, ctx, ten, ident):
    rows, columns = low_t.shape[2], hid.shape[1]
    t_rows, width = mid.shape
    chips = fs // 2
    blocks = [(rows, columns), (rows, 2 * columns)]
    sends = ctx * (ten - 1) + 2 * ctx + 2 * (chips + (chips - 1) * ctx + ctx - 1) + ten - 1
    dma = pltpu.SemaphoreType.DMA
    shape = jax.ShapeDtypeStruct
    return pl.pallas_call(
        functools.partial(back_kernel, fs, ctx, ten),
        out_shape=[
            shape((t_rows, width), single),
            shape((ten, t_rows, width), half_type),
            shape((1, width), single),
            shape((ctx, rows, 2 * columns), half_type),
            shape((ctx, rows, columns), half_type),
        ],
        in_specs=[VMEM] * 7 + [ANY],
        out_specs=[VMEM] * 3 + [ANY] * 2,
        scratch_shapes=[pltpu.VMEM((fs, ctx, *b), half_type) for b in blocks]
        + [pltpu.VMEM((chips, ctx, *b), half_type) for b in blocks]
        + [pltpu.VMEM((chips - 1, ctx, *b), half_type) for b in blocks]
        + [
            pltpu.VMEM((ctx, ten, t_rows, width), half_type),
            pltpu.VMEM((ten - 1, ctx, t_rows, width), half_type),
            pltpu.VMEM((ctx + 1, t_rows, width), half_type),
            pltpu.VMEM((2, 2, ctx, rows, 2 * columns), half_type),
            dma((2,)),
            dma((2,)),
            dma((sends,)),
            dma((2, chips)),
            dma((2, chips - 1, ctx)),
            dma((2, ctx)),
            dma((ten - 1, ctx)),
            dma((ctx + 1,)),
            dma((ten,)),
        ],
        compiler_params=pltpu.CompilerParams(
            collective_id=ident, has_side_effects=True, vmem_limit_bytes=VMEM_ALL
        ),
        name=f"mlp_back_{ident}",
    )(low_t, dy_t, hid, dpair, mid, cot, scale, slice_p)


def update_kernel(parts, *refs):
    count = len(refs) // 7
    for w in range(count):
        weight, first, second = refs[3 * w : 3 * w + 3]
        outs = refs[3 * count + 4 * w : 3 * count + 4 * w + 4]
        columns = weight.shape[1] // parts.shape[0]
        for k in range(parts.shape[0]):
            grad = parts[k, :, w * columns : (w + 1) * columns].astype(single)
            here = (slice(None), slice(k * columns, (k + 1) * columns))
            values = (grad, *adamw(weight[here], grad, first[here], second[here]))
            for out, value in zip(outs, values):
                out[here] = value


def update(parts, weights, ident):
    ctx, rows, columns = parts.shape
    step = 32 if rows % 32 == 0 else 8
    wide = weights[0][0].shape[1]
    spec = pl.BlockSpec((step, wide), lambda i: (i, 0))
    part = pl.BlockSpec((ctx, step, columns), lambda i: (0, i, 0))
    count = len(weights)
    outs = pl.pallas_call(
        update_kernel,
        grid=(rows // step,),
        out_shape=[jax.ShapeDtypeStruct((rows, wide), single)] * (4 * count),
        in_specs=[part] + [spec] * (3 * count),
        out_specs=[spec] * (4 * count),
        compiler_params=pltpu.CompilerParams(vmem_limit_bytes=VMEM_ALL),
        name=f"update_{ident}",
    )(parts, *(v for group in weights for v in group))
    return [outs[4 * w : 4 * w + 4] for w in range(count)]


def attn_kernel(fs, ctx, ten, *refs):
    low_t, dmid_t, d_query, att, own, cosine, sine, hidden, mid, dmid, scale, terms = refs[:12]
    hid, slice_d, slice_q = refs[12:15]
    out_q, out_o, out_s, out_kv, tokens = refs[15:20]
    dws, nears, fars, lines = refs[20:25], refs[25:30], refs[30:35], refs[35:40]
    source, first, line, first_k, line_k, d_qkv, dnorm, take = refs[40:48]
    held_d, held_q, tail, pool, own_sums = refs[48:53]
    load, send, recv_c, recv_y, recv_z, recv_tx, recv_t, recv_kx, recv_k, recv_n, recv_x = refs[53:]
    f, y, core, twin, across = fsdp_place(fs)
    z, x = lax.axis_index("context"), lax.axis_index("tensor")
    chips = fs // 2
    rows = low_t.shape[2]
    beside = [lax.rem(x + d, ten) for d in range(1, ten)]
    rows_of = [lax.rem(y + d, chips) for d in range(chips)]
    chip_order = rows_of[1:] + rows_of[:1]
    partners = [{"context": partner} for partner, _, _ in doubling(z, ctx)]
    greet(partners + across + [twin] + [{"tensor": k} for k in beside])
    out = Sends(send)
    sends, own_slots = halving(z, ctx)
    order = [send_z[0] for send_z in sends] + [z]
    kinds = (cast, cast, cast, cast, lambda v: v)
    heads = d_query.shape[1]
    widths = [dw.shape[-1] for dw in dws[:4]]
    rights = (
        d_qkv.at[:, : widths[0]],
        d_qkv.at[:, widths[0] :],
        att.at[:, : widths[2]],
        att.at[:, widths[2] :],
    )
    lefts = (low_t, low_t, dmid_t, dmid_t)

    def start(w):
        for row in chip_order:
            owner = row * 2 + 1 - core
            if w < 4:
                fill_product(dws[w], lefts[w], rights[w], owner, ctx)
            out.push(dws[w].at[owner], nears[w].at[row], recv_c.at[w, row], twin)
        if w < 4:
            for row in chip_order:
                fill_product(dws[w], lefts[w], rights[w], row * 2 + core, ctx)

    def over_chips(w):
        for k, row in enumerate(rows_of[1:]):
            arrived(nears[w].at[row], recv_c.at[w, row], twin)
            for owner in order:
                mine = dws[w].at[row * 2 + core, owner]
                mine[...] = kinds[w](mine[...].astype(single) + nears[w][row, owner].astype(single))
                out.push(mine, fars[w].at[k, owner], recv_y.at[w, k, owner], across[k])

    def summed_block(w, owner, places):
        total = dws[w][f, owner].astype(single) + nears[w][y, owner].astype(single)
        for k in range(chips - 1):
            arrived(fars[w].at[k, owner], recv_y.at[w, k, owner], twin)
            total = total + fars[w][k, owner].astype(single)
        return collect(total, lines[w], recv_z.at[w], places, twin)

    def over_context(w, d):
        if d == 0:
            arrived(nears[w].at[y], recv_c.at[w, y], twin)
        owner, partner, slot, places = sends[d]
        mine = dws[w].at[f, owner]
        mine[...] = kinds[w](summed_block(w, owner, places))
        out.push(mine, lines[w].at[slot], recv_z.at[w, slot], {"context": partner})

    def finish(w):
        return summed_block(w, z, own_slots)

    own_sums[...] = own[...]
    token_start(own_sums, first_k, recv_kx, out, beside, order)
    start(2)
    over_chips(2)
    start(3)
    over_chips(3)
    for d, send_z in enumerate(sends):
        token_send(send_z, own_sums, first_k, recv_kx, line_k, recv_k, x, out)
        over_context(2, d)
    summed = token_sum(z, own_slots, own_sums, first_k, recv_kx, line_k, recv_k, x)
    half = summed.shape[1] // 2
    a, b = summed[:, :half], summed[:, half:]
    c, s = cosine[...], sine[...]
    is_key = x == 0
    d_qkv[:, :heads] = d_query[...]
    d_qkv[:, heads : heads + half] = cast(jnp.where(is_key, a * c + b * s, a))
    d_qkv[:, heads + half :] = cast(jnp.where(is_key, b * c - a * s, b))
    token_products(dnorm, d_qkv, slice_q, held_q, load)
    for other in beside:
        out.push(dnorm.at[0, other], take.at[x], recv_n.at[x], {"tensor": other})
    start(0)
    over_chips(0)
    token_products(source, hid, slice_d, held_d, load)
    token_start(source, first, recv_tx, out, beside, order)
    for d in range(ctx - 1):
        over_context(3, d)
    dnorm_one = dnorm[0, x].astype(single)
    for other in beside:
        arrived(take.at[other], recv_n.at[other], twin)
        dnorm_one = dnorm_one + take[other].astype(single)
    values = hidden[...]
    inverse = lax.rsqrt(jnp.mean(values * values, axis=-1, keepdims=True) + norm_eps)
    normed = values * inverse
    dnormed = dnorm_one * (1.0 + scale[...])
    tokens[x, 1] = cast(
        dmid[...]
        + inverse * (dnormed - normed * jnp.mean(dnormed * normed, axis=-1, keepdims=True))
    )
    sums = jnp.sum(dnorm_one * normed, axis=0, keepdims=True)
    dws[4][...] = jnp.zeros_like(dws[4])
    for j in range(fs * ctx):
        at = slice(j * rows, (j + 1) * rows)
        dws[4][j // ctx, j % ctx, 0:1, :rows] = sums[:, at]
        dws[4][j // ctx, j % ctx, 1:2, :rows] = terms[:, at]
    start(4)
    start(1)
    over_chips(4)
    over_chips(1)

    def hand_over(t):
        for other in beside:
            out.push(tokens.at[x, t], tokens.at[x, t], recv_x.at[2 + t, x], {"tensor": other})

    hand_over(1)
    for d, send_z in enumerate(sends):
        token_send(send_z, source, first, recv_tx, line, recv_t, x, out)
        over_context(0, d)
    for d in range(ctx - 1):
        over_context(4, d)
    for d in range(ctx - 1):
        over_context(1, d)
        if d == 0:
            tokens[x, 0] = cast(
                mid[...] + token_sum(z, own_slots, source, first, recv_tx, line, recv_t, x)
            )
            hand_over(0)
    pool[x] = finish(4)
    for other in beside:
        out.push(pool.at[x], pool.at[x], recv_x.at[0, x], {"tensor": other})
    out_o[:, : widths[2]] = finish(2)
    out_o[:, widths[2] :] = finish(3)
    out_q[:, : widths[0]] = finish(0)
    grad = finish(1)
    out_q[:, widths[0] :] = grad[:, : heads - widths[0]]
    tail[x] = cast(grad[:, heads - widths[0] :])
    for other in beside:
        out.push(tail.at[x], tail.at[x], recv_x.at[1, x], {"tensor": other})
    for other in beside:
        arrived(pool.at[other], recv_x.at[0, other], twin)
        arrived(tail.at[other], recv_x.at[1, other], twin)
        for t in range(2):
            arrived(tokens.at[other, t], recv_x.at[2 + t, other], twin)
    total = pool[0]
    for k in range(1, ten):
        total = total + pool[k]
    out_s[...] = total
    columns = tail.shape[-1]
    for k in range(ten):
        out_kv[:, k * columns : (k + 1) * columns] = tail[k].astype(single)
    out.drain()


def attn_back(
    low_t, dmid_t, d_query, att, own, cosine, sine, hidden, mid, dmid, scale, terms, hid, slice_d, slice_q,
    fs, ctx, ten, ident,
):
    rows = low_t.shape[2]
    t_rows, width = mid.shape
    chips = fs // 2
    heads = d_query.shape[1]
    count, tail = own.shape[2:]
    lanes = -(-rows // 128) * 128
    cuts = [-(-total // 256) * 128 for total in (heads + tail, att.shape[1])]
    both = [
        ((rows, cuts[0]), half_type),
        ((rows, heads + tail - cuts[0]), half_type),
        ((rows, cuts[1]), half_type),
        ((rows, att.shape[1] - cuts[1]), half_type),
        ((8, lanes), single),
    ]
    sends = (
        2 * (ctx * (ten - 1) + 2 * ctx)
        + 5 * (ten - 1)
        + 5 * (chips + (chips - 1) * ctx + 2 * ctx)
    )
    dma = pltpu.SemaphoreType.DMA
    shape = jax.ShapeDtypeStruct
    return pl.pallas_call(
        functools.partial(attn_kernel, fs, ctx, ten),
        out_shape=[
            shape((rows, heads), single),
            shape((rows, att.shape[1]), single),
            shape((8, lanes), single),
            shape((rows, ten * tail), single),
            shape((ten, 2, t_rows, width), half_type),
        ],
        in_specs=[VMEM] * 13 + [ANY] * 2,
        out_specs=[VMEM] * 5,
        scratch_shapes=[pltpu.VMEM((fs, ctx, *b), t) for b, t in both]
        + [pltpu.VMEM((chips, ctx, *b), t) for b, t in both]
        + [pltpu.VMEM((chips - 1, ctx, *b), t) for b, t in both]
        + [pltpu.VMEM((ctx + 1, *b), t) for b, t in both]
        + [
            pltpu.VMEM((ctx, ten, t_rows, width), half_type),
            pltpu.VMEM((ten - 1, ctx, t_rows, width), half_type),
            pltpu.VMEM((ctx + 1, t_rows, width), half_type),
            pltpu.VMEM((ten - 1, ctx, count, tail), half_type),
            pltpu.VMEM((ctx + 1, count, tail), half_type),
            pltpu.VMEM((count, heads + tail), half_type),
            pltpu.VMEM((1, ten, t_rows, width), half_type),
            pltpu.VMEM((ten, t_rows, width), half_type),
            pltpu.VMEM((2, 2, ctx, *slice_d.shape[2:]), half_type),
            pltpu.VMEM((2, 2, ctx, *slice_q.shape[2:]), half_type),
            pltpu.VMEM((ten, rows, tail), half_type),
            pltpu.VMEM((ten, 8, lanes), single),
            pltpu.VMEM(own.shape, half_type),
            dma((2,)),
            dma((sends,)),
            dma((5, chips)),
            dma((5, chips - 1, ctx)),
            dma((5, ctx + 1)),
            dma((ten - 1, ctx)),
            dma((ctx + 1,)),
            dma((ten - 1, ctx)),
            dma((ctx + 1,)),
            dma((ten,)),
            dma((4, ten)),
        ],
        compiler_params=pltpu.CompilerParams(
            collective_id=ident, has_side_effects=True, vmem_limit_bytes=VMEM_ALL
        ),
        name=f"attn_back_{ident}",
    )(low_t, dmid_t, d_query, att, own, cosine, sine, hidden, mid, dmid, scale, terms, hid, slice_d, slice_q)


def on_device(hidden_in, cotangent, segment_ids, positions, *params):
    masters, firsts, seconds = params[:8], params[8:16], params[16:]
    (
        attn_scale,
        query_weight,
        keyval_weight,
        output_weight,
        mlp_scale,
        gate_weight,
        up_weight,
        down_weight,
    ) = masters
    fs, ctx, ten = (lax.axis_size(name) for name in ("fsdp", "context", "tensor"))
    x = lax.axis_index("tensor")
    context_index = lax.axis_index("context")
    block, width = hidden_in.shape[1:]
    rows = query_weight.shape[0]
    half_rows = block // ten
    heads_width = query_weight.shape[1]
    heads_here = heads_width // HD
    hidden = hidden_in[0]
    cot = cotangent[0]
    hidden_half = lax.dynamic_slice_in_dim(hidden, x * half_rows, half_rows, 0)
    cot_half = lax.dynamic_slice_in_dim(cot, x * half_rows, half_rows, 0)
    is_key = x == 0

    qkv_block = jnp.concatenate(
        [
            cast(query_weight),
            cast(lax.dynamic_slice_in_dim(keyval_weight, x * HD, HD, 1)),
        ],
        axis=1,
    )
    lanes = -(-max(rows, block) // 128) * 128
    wide = [
        jnp.pad(v, (0, lanes - v.shape[0]))
        for v in (attn_scale, mlp_scale, segment_ids[0].astype(single))
    ]
    small = jnp.stack(wide + [jnp.zeros((lanes,), single)] * 5)
    small_all, qkv_all, out_all, dy_all, part_p, part_d = spread(
        [small, qkv_block, cast(output_weight.T)],
        cast(cot_half),
        [gate_weight, up_weight, down_weight.T],
        fs,
        ctx,
        ten,
        1,
    )
    scale_one = cast(small_all[:, :, 0, :rows].reshape(-1)).astype(single)
    scale_two = cast(small_all[:, :, 1, :rows].reshape(-1)).astype(single)
    f = lax.axis_index("fsdp")
    seg_all = lax.dynamic_index_in_dim(small_all[:, :, 2, :block], f, 0, False).reshape(-1)
    qkv_full = qkv_all.reshape(width, -1)
    out_full = out_all.reshape(width, -1)

    _, _, low_one = rms_forward(hidden, scale_one)
    qkv = dot(low_one, qkv_full, ((1,), (0,)))
    query = qkv[:, :heads_width].reshape(block, heads_here, HD)
    own = qkv[:, heads_width:]
    cosine, sine = rope_tables(positions[0])
    query_low = cast(rotate(query, cosine[:, None, :], sine[:, None, :]) * HD ** (-0.5))
    own_low = cast(jnp.where(is_key, rotate(own, cosine, sine), own))
    keyval_all = tokens_to_all(own_low, ctx, ten, 2).reshape(ctx, ten, block, HD)
    keys_all = keyval_all[:, 0].reshape(-1, HD)
    values_all = keyval_all[:, 1].reshape(-1, HD)
    rows_index = context_index * block + jnp.arange(block, dtype=jnp.int32)
    cols_index = jnp.arange(keys_all.shape[0], dtype=jnp.int32)
    allowed = (rows_index[:, None] >= cols_index[None, :]) & (
        segment_ids[0].astype(single)[:, None] == seg_all[None, :]
    )
    scores = jnp.einsum("bhd,jd->hbj", query_low, keys_all, preferred_element_type=single)
    masked = jnp.where(allowed, scores, masked_value)
    top = jnp.max(masked, axis=-1, keepdims=True)
    total = jnp.sum(jnp.where(allowed, jnp.exp(masked - top), 0.0), axis=-1, keepdims=True)
    lse = top + jnp.log(total)
    prob = jnp.where(allowed, jnp.exp(masked - lse), 0.0)
    prob_low = cast(prob)
    att_low = cast(
        jnp.einsum("hbj,jd->bhd", prob_low, values_all, preferred_element_type=single)
    )
    att_flat = att_low.reshape(block, heads_width)
    attn_part = dot(att_flat, out_full, ((1,), (1,)))
    slice_p, slice_d, hid, dpair, low_t, dy_t, mid_half, _ = mlp_forward(
        cast(attn_part).reshape(ten, half_rows, width),
        hidden_half,
        scale_two[None],
        dy_all,
        part_p,
        part_d,
        fs,
        ctx,
        ten,
        4,
    )
    dmid_half, dmid_low, terms_two, part_p, part_d = mlp_back(
        low_t, dy_t, hid, dpair, mid_half, cot_half, scale_two[None], slice_p, fs, ctx, ten, 5
    )

    dmid_low = dmid_low.reshape(block, width)
    datt_low = cast(dot(dmid_low, out_full, ((1,), (0,)))).reshape(block, heads_here, HD)
    delta = jnp.einsum("bhd,bhd->hb", datt_low, att_low, preferred_element_type=single)
    dprob = jnp.einsum("bhd,jd->hbj", datt_low, values_all, preferred_element_type=single)
    dscore_low = cast(prob * (dprob - delta[..., None]))
    dquery = jnp.einsum("hbj,jd->bhd", dscore_low, keys_all, preferred_element_type=single)
    dkey_part = jnp.einsum("hbj,bhd->jd", dscore_low, query_low, preferred_element_type=single)
    dvalue_part = jnp.einsum("hbj,bhd->jd", prob_low, datt_low, preferred_element_type=single)
    own_part = jnp.stack(
        [cast(part).reshape(ctx, block, HD) for part in (dkey_part, dvalue_part)], axis=1
    )
    dquery_low = cast(
        unrotate(dquery, cosine[:, None, :], sine[:, None, :]) * HD ** (-0.5)
    ).reshape(block, heads_width)
    row_blocks = (fs, ctx, rows, -1)
    grad_wq, grad_wo, grad_s, grad_wkv, outs = attn_back(
        low_one.T.reshape(row_blocks),
        dmid_low.T.reshape(row_blocks),
        dquery_low,
        att_flat,
        own_part,
        cosine,
        sine,
        hidden_half,
        mid_half,
        dmid_half,
        scale_one[None],
        terms_two,
        hid,
        slice_d,
        qkv_all,
        fs,
        ctx,
        ten,
        9,
    )
    outs = outs.transpose(1, 0, 2, 3).reshape(2, 1, block, width).astype(single)

    grads = (grad_s[0, :rows], grad_wq, grad_wkv, grad_wo.T, grad_s[1, :rows])
    results = [
        (grad, *adamw(weight, grad, first, second))
        for weight, grad, first, second in zip(masters, grads, firsts, seconds)
    ]
    groups = list(zip(masters, firsts, seconds))
    results += update(part_p, groups[5:7], 5)
    results += [[v.T for v in update(part_d, [[v.T for v in groups[7]]], 7)[0]]]
    return (
        outs[0],
        outs[1],
        *(entry[0] for entry in results),
        *(entry[1] for entry in results),
        *(entry[2] for entry in results),
        *(entry[3] for entry in results),
    )


def solution(mesh):
    both = ("fsdp", "context")
    tokens = P("fsdp", "context", None)
    weights = (
        P(both),
        P(both, "tensor"),
        P(both, None),
        P("tensor", both),
        P(both),
        P(both, "tensor"),
        P(both, "tensor"),
        P("tensor", both),
    )
    return jax.shard_map(
        on_device,
        mesh=mesh,
        in_specs=(tokens, tokens, P("fsdp", "context"), P("fsdp", "context"), *(weights * 3)),
        out_specs=(tokens, tokens, *(weights * 4)),
        check_vma=False,
    )
```

```python
import functools

import jax
import jax.numpy as jnp
from jax import lax
from jax.experimental import pallas as pl
from jax.experimental.pallas import tpu as pltpu
from jax.sharding import PartitionSpec as P

HD = 256


norm_eps = 1e-06
beta_one = 0.9
beta_two = 0.999
adam_eps = 1e-08
learn_rate = 0.03
decay_rate = 0.1
adam_step = 4.0
rope_base = 10000.0
masked_value = -1e30

single = jnp.float32
half_type = jnp.bfloat16


def gelu_tanh(values):
    return jax.nn.gelu(values, approximate=True)


def rope_tables(positions):
    half = HD // 2
    freq = rope_base ** (-2.0 * jnp.arange(half).astype(jnp.float32) / HD)
    angle = positions.astype(jnp.float32)[..., None] * freq
    return (jnp.cos(angle), jnp.sin(angle))


def rotate(values, cosine, sine):
    half = values.shape[-1] // 2
    first = values[..., :half]
    second = values[..., half:]
    return jnp.concatenate(
        [first * cosine - second * sine, second * cosine + first * sine], axis=-1
    )


def unrotate(values, cosine, sine):
    half = values.shape[-1] // 2
    first = values[..., :half]
    second = values[..., half:]
    return jnp.concatenate(
        [first * cosine + second * sine, second * cosine - first * sine], axis=-1
    )


def rms_forward(values, scale):
    inverse = lax.rsqrt(jnp.mean(values * values, axis=-1, keepdims=True) + norm_eps)
    normed = values * inverse
    return (normed, inverse, (normed * (1.0 + scale)).astype(jnp.bfloat16))


def rms_backward(dnorm, normed, inverse, scale):
    dnormed = dnorm * (1.0 + scale)
    dvalues = inverse * (dnormed - normed * jnp.mean(dnormed * normed, axis=-1, keepdims=True))
    return (dvalues, dnorm * normed)


def adamw(weight, grad, first, second):
    first_new = beta_one * first + (1.0 - beta_one) * grad
    second_new = beta_two * second + (1.0 - beta_two) * grad * grad
    fix_one = 1.0 - beta_one**adam_step
    fix_two = 1.0 - beta_two**adam_step
    update = first_new / fix_one / (jnp.sqrt(second_new / fix_two) + adam_eps)
    return (weight - learn_rate * (update + decay_rate * weight), first_new, second_new)


def dot(a, b, dims):
    return lax.dot_general(a, b, (dims, ((), ())), preferred_element_type=single)


MESH = pl.DeviceIdType.MESH
ANY = pl.BlockSpec(memory_space=pl.ANY)
VMEM = pl.BlockSpec(memory_space=pltpu.VMEM)


def greet(peers):
    barrier = pltpu.get_barrier_semaphore()
    for peer in peers:
        pl.semaphore_signal(barrier, inc=1, device_id=peer, device_id_type=MESH)
    pl.semaphore_wait(barrier, len(peers))


def remote(src, dst, send, recv, peer):
    return pltpu.make_async_remote_copy(
        src_ref=src, dst_ref=dst, send_sem=send, recv_sem=recv, device_id=peer, device_id_type=MESH
    )


def arrived(dst, recv, peer):
    remote(dst, dst, recv, recv, peer).wait_recv()


def fsdp_place(fs):
    f = lax.axis_index("fsdp")
    core = lax.rem(f, 2)
    y = lax.div(f, 2)
    twin = {"fsdp": f + 1 - 2 * core}
    across = [{"fsdp": lax.rem(y + d, fs // 2) * 2 + core} for d in range(1, fs // 2)]
    return f, y, core, twin, across


class Sends:
    def __init__(self, send):
        self.send, self.made = send, []

    def push(self, src, dst, recv, peer, *conditions):
        copy = remote(src, dst, self.send.at[len(self.made)], recv, peer)
        self.made.append((copy, conditions))
        under(conditions, copy.start)

    def drain(self):
        for copy, conditions in self.made:
            under(conditions, copy.wait_send)


def under(conditions, action):
    if not conditions:
        action()
        return
    holds = conditions[0]
    for more in conditions[1:]:
        holds = jnp.logical_and(holds, more)
    pl.when(holds)(action)


def line_steps(z, ctx):
    for s in range(1, ctx):
        yield z - s, z >= s, z + 1, z + 1 < ctx
        yield z + s, z + s < ctx, z - 1, z >= 1


def tokens_kernel(ctx, ten, src, out, local, send, recv):
    z, x = lax.axis_index("context"), lax.axis_index("tensor")
    around = [lax.rem(z + d, ctx) for d in range(ctx)]
    across = [{"tensor": lax.rem(x + d, ten)} for d in range(1, ten)]
    greet([{"context": k} for k in around[1:]] + across)
    sends = []

    def push(ref, source, peer):
        copy = remote(ref, out.at[source, x], send.at[len(sends)], recv.at[source, x], peer)
        copy.start()
        sends.append(copy)

    for d in range(1, ctx):
        push(src, z, {"context": around[d]})
    for peer in across:
        push(src, z, peer)
    keep = pltpu.make_async_copy(src, out.at[z, x], local)
    keep.start()
    back = [lax.rem(z + ctx - d, ctx) for d in range(ctx)]
    for d in range(1, ctx):
        arrived(out.at[back[d], x], recv.at[back[d], x], {"context": back[d]})
        for peer in across:
            push(out.at[back[d], x], back[d], peer)
    for d in range(ctx):
        for peer in across:
            other = peer["tensor"]
            arrived(out.at[back[d], other], recv.at[back[d], other], peer)
    keep.wait()
    for copy in sends:
        copy.wait_send()


def tokens_to_all(block, ctx, ten, ident):
    sends = (ctx - 1) + ctx * (ten - 1)
    out = pl.pallas_call(
        functools.partial(tokens_kernel, ctx, ten),
        out_shape=jax.ShapeDtypeStruct((ctx, ten, *block.shape), block.dtype),
        in_specs=[VMEM],
        out_specs=VMEM,
        scratch_shapes=[
            pltpu.SemaphoreType.DMA(()),
            pltpu.SemaphoreType.DMA((sends,)),
            pltpu.SemaphoreType.DMA((ctx, ten)),
        ],
        compiler_params=pltpu.CompilerParams(collective_id=ident, has_side_effects=True),
        name=f"tokens_{ident}",
    )(block)
    return out.reshape(-1, block.shape[-1])


VMEM_ALL = 67043328


def cast(v):
    return v.astype(half_type)


def fill_product(dw, left, right, owner, ctx):
    def one(k, carry):
        dw[owner, k] = cast(
            lax.dot_general(
                left[owner, k], right[...], (((1,), (0,)), ((), ())), preferred_element_type=single
            )
        )
        return carry

    lax.fori_loop(0, ctx, one, 0)


def split_columns(ctx, weights, parts, wide, packed, small, load, store):
    columns = small.shape[-1]
    fetches = [pltpu.make_async_copy(weights[w], wide.at[w], load.at[w]) for w in range(3)]
    for fetch in fetches:
        fetch.start()
    for w in range(3):
        fetches[w].wait()
        for k in range(ctx):
            piece = cast(wide[w, :, k * columns : (k + 1) * columns])
            if w < 2:
                packed[k, :, w * columns : (w + 1) * columns] = piece
            else:
                small[k] = piece
    puts = [pltpu.make_async_copy(v, parts[j], store.at[j]) for j, v in enumerate((packed, small))]
    for put in puts:
        put.start()
    for put in puts:
        put.wait()


def first_kernel(fs, ctx, ten, count, *refs):
    srcs, weights = refs[: count + 1], refs[count + 1 : count + 4]
    refs = refs[count + 4 :]
    outs, parts = refs[: count + 1], refs[count + 1 : count + 3]
    wide, packed, small, load, store, local, send, recv, recv_t = refs[count + 3 :]
    f, y, core, twin, across = fsdp_place(fs)
    z, x = lax.axis_index("context"), lax.axis_index("tensor")
    beside = [{"tensor": lax.rem(x + d, ten)} for d in range(1, ten)]
    back = [lax.rem(z + ctx - d, ctx) for d in range(ctx)]
    up, down = {"context": z + 1}, {"context": z - 1}
    nxt, prv = lax.rem(z + 1, ctx), back[1]
    greet([{"context": nxt}, {"context": prv}] + across + [twin] + beside)
    out = Sends(send)
    keeps = []

    def where(w, source):
        if w == count:
            return outs[w].at[source, x], recv_t.at[source, x], beside
        return outs[w].at[f, source], recv.at[w, f, source], across + [twin]

    for w in range(count + 1):
        mine, sem, peers = where(w, z)
        out.push(srcs[w], mine, sem, up, z + 1 < ctx)
        out.push(srcs[w], mine, sem, down, z >= 1)
        for peer in peers:
            out.push(srcs[w], mine, sem, peer)
        keeps.append(pltpu.make_async_copy(srcs[w], mine, local.at[w]))
        keeps[-1].start()
    split_columns(ctx, weights, parts, wide, packed, small, load, store)
    for source, exists, onward, more in line_steps(z, ctx):
        for w in range(count + 1):
            block, sem, peers = where(w, source)
            under((exists,), lambda: arrived(block, sem, twin))
            out.push(block, block, sem, {"context": onward}, exists, more)
            for peer in peers:
                out.push(block, block, sem, peer, exists)
    chain = [(z, ())] + [(source, (exists,)) for source, exists, _, _ in line_steps(z, ctx)]
    for source, when in chain:
        for w in range(count):
            for peer in across:
                owner = peer["fsdp"]
                block, sem = outs[w].at[owner, source], recv.at[w, owner, source]
                under(when, lambda: arrived(block, sem, twin))
                out.push(block, block, sem, twin, *when)
    for source in back:
        for w in range(count):
            for step in range(fs // 2):
                owner = lax.rem(y + step, fs // 2) * 2 + 1 - core
                arrived(outs[w].at[owner, source], recv.at[w, owner, source], twin)
        for peer in beside:
            arrived(outs[count].at[source, peer["tensor"]], recv_t.at[source, peer["tensor"]], twin)
    for keep in keeps:
        keep.wait()
    out.drain()


def spread(blocks, tokens, weights, fs, ctx, ten, ident):
    count = len(blocks)
    chips = fs // 2
    lines = 2 + 2 * (ctx - 1)
    sends = count * (lines + (2 * ctx - 1) * (2 * chips - 1)) + lines + (2 * ctx - 1) * (ten - 1)
    rows, wide = weights[0].shape
    part = (ctx, rows, wide // ctx)
    pair = (ctx, rows, 2 * (wide // ctx))
    dma = pltpu.SemaphoreType.DMA
    return pl.pallas_call(
        functools.partial(first_kernel, fs, ctx, ten, count),
        out_shape=[jax.ShapeDtypeStruct((fs, ctx, *b.shape), b.dtype) for b in blocks]
        + [jax.ShapeDtypeStruct((ctx, ten, *tokens.shape), tokens.dtype)]
        + [jax.ShapeDtypeStruct(pair, half_type), jax.ShapeDtypeStruct(part, half_type)],
        in_specs=[ANY] * (count + 4),
        out_specs=[ANY] * (count + 3),
        scratch_shapes=[
            pltpu.VMEM((3, rows, wide), single),
            pltpu.VMEM(pair, half_type),
            pltpu.VMEM(part, half_type),
            dma((3,)),
            dma((2,)),
            dma((count + 1,)),
            dma((sends,)),
            dma((count, fs, ctx)),
            dma((ctx, ten)),
        ],
        compiler_params=pltpu.CompilerParams(
            collective_id=ident, has_side_effects=True, vmem_limit_bytes=VMEM_ALL
        ),
        name=f"spread_{ident}",
    )(*blocks, tokens, *weights)


def flip(k, bit):
    return k + bit - 2 * bit * lax.rem(lax.div(k, bit), 2)


def halving(z, ctx):
    sends, seen, base, bit = [], [], 0, 1
    while bit < ctx:
        count = ctx // (2 * bit)
        for u in range(count):
            owner = flip(z, bit) - 2 * bit * lax.div(z, 2 * bit) + 2 * bit * u
            sends.append((owner, flip(z, bit), base + u, [at + lax.div(owner, d) for at, d in seen]))
        seen.append((base, 2 * bit))
        base, bit = base + count, 2 * bit
    return sends, [at + lax.div(z, d) for at, d in seen]


def doubling(z, ctx):
    steps, held, bit = [], [z], ctx // 2
    while bit:
        got = [flip(k, bit) for k in held]
        steps.append((flip(z, bit), list(held), got))
        held, bit = held + got, bit // 2
    return steps


def collect(total, slots, sem, places, peer):
    for at in places:
        arrived(slots.at[at], sem.at[at], peer)
        total = total + slots[at].astype(single)
    return total


def chip_tiles(weight, held, load, use):
    chips = weight.shape[0] // 2

    def fetch(k, slot):
        return pltpu.make_async_copy(weight.at[pl.ds(2 * k, 2)], held.at[slot], load.at[slot])

    fetch(0, 0).start()

    def step(k, carry):
        slot = lax.rem(k, 2)
        fetch(k, slot).wait()

        @pl.when(k + 1 < chips)
        def _():
            fetch(k + 1, 1 - slot).start()

        use(k, held[slot].reshape(-1, held.shape[-1]))
        return carry

    lax.fori_loop(0, chips, step, 0)


def forward_kernel(fs, ctx, ten, *refs):
    att, hidden, scale, dy, part_p, part_d, slice_o = refs[:7]
    slice_p, slice_d, hid, dpair, low_t, dy_t, mid = refs[7:14]
    low_all, attn, take, held_o, held_p, held_d, sums_p, sums_d = refs[14:22]
    load, local, send, recv_p, recv_d, recv_t, recv_x = refs[22:]
    f, y, core, twin, across = fsdp_place(fs)
    z, x = lax.axis_index("context"), lax.axis_index("tensor")
    rows, columns = part_d.shape[1:]
    width = hidden.shape[1]
    count = hid.shape[0]
    beside = [{"tensor": lax.rem(x + d, ten)} for d in range(1, ten)]
    around = [lax.rem(z + d, ctx) for d in range(ctx)]
    back = [lax.rem(z + ctx - d, ctx) for d in range(ctx)]
    greet([{"context": k} for k in around[1:]] + across + [twin] + beside)
    out = Sends(send)
    parts, slices, recvs = (part_p, part_d), (slice_p, slice_d), (recv_p, recv_d)

    def block(w, owner, source):
        return slices[w].at[owner, source], recvs[w].at[owner, source]

    def to_context(w, d):
        dst, sem = block(w, f, z)
        out.push(parts[w].at[around[d]], dst, sem, {"context": around[d]})

    def from_context(w, d):
        dst, sem = block(w, f, back[d])
        arrived(dst, sem, twin)
        for peer in across + [twin]:
            out.push(dst, dst, sem, peer)

    def from_chips(w):
        for d in range(ctx):
            for peer in across:
                dst, sem = block(w, peer["fsdp"], back[d])
                arrived(dst, sem, twin)
                out.push(dst, dst, sem, twin)

    def from_twin(w):
        for d in range(ctx):
            for step in range(fs // 2):
                dst, sem = block(w, lax.rem(y + step, fs // 2) * 2 + 1 - core, back[d])
                arrived(dst, sem, twin)

    to_context(0, 1)
    keeps = []
    for w in range(2):
        dst, sem = block(w, f, z)
        for peer in across + [twin]:
            out.push(parts[w].at[z], dst, sem, peer)
        keeps.append(pltpu.make_async_copy(parts[w].at[z], dst, local.at[w]))
        keeps[-1].start()
    token_products(attn, att, slice_o, held_o, load)
    for peer in beside:
        out.push(attn.at[0, peer["tensor"]], take.at[x], recv_x.at[x], peer)
    total = hidden[...] + attn[0, x].astype(single)
    for peer in beside:
        other = peer["tensor"]
        arrived(take.at[other], recv_x.at[other], twin)
        total = total + take[other].astype(single)
    mid[...] = total
    inverse = lax.rsqrt(jnp.mean(total * total, axis=-1, keepdims=True) + norm_eps)
    low_all[z, x] = cast(total * inverse * (1.0 + scale[...]))
    mine = low_all.at[z, x]
    later = [(0, d) for d in range(2, ctx)] + [(1, d) for d in range(1, ctx)]
    early = [d for d in range(1, ctx)]
    steps = doubling(z, ctx)
    for partner, _, _ in steps:
        out.push(mine, mine, recv_t.at[z, x], {"context": partner})
    for peer in beside:
        out.push(mine, mine, recv_t.at[z, x], peer)
    to_context(*later.pop(0))
    from_context(0, early.pop(0))
    for step, (partner, _, got) in enumerate(steps):
        for source in got:
            here, sem = low_all.at[source, x], recv_t.at[source, x]
            arrived(here, sem, twin)
            for further, _, _ in steps[step + 1 :]:
                out.push(here, here, sem, {"context": further})
            for peer in beside:
                out.push(here, here, sem, peer)
            if early:
                from_context(0, early.pop(0))
            if later:
                to_context(*later.pop(0))
    while later:
        to_context(*later.pop(0))
    while early:
        from_context(0, early.pop(0))

    def turned(dst, src):
        for j in range(fs * ctx):
            piece = src[:, :, :, j * rows : (j + 1) * rows].reshape(count, rows)
            dst[j // ctx, j % ctx] = piece.T

    def product(weight, held, left, sums):
        deep = width // (fs // 2)

        def use(k, tile):
            lanes = pl.ds(pl.multiple_of(k * deep, deep), deep)
            add = jnp.dot(
                left[:, :, :, lanes].reshape(count, deep), tile, preferred_element_type=single
            )

            @pl.when(k == 0)
            def _():
                sums[...] = add

            @pl.when(k > 0)
            def _():
                sums[...] += add

        chip_tiles(weight, held, load, use)

    from_chips(0)
    turned(dy_t, dy)
    from_context(1, 1)
    for source in back:
        for peer in beside:
            other = peer["tensor"]
            arrived(low_all.at[source, other], recv_t.at[source, other], twin)
    from_twin(0)
    keeps[0].wait()
    turned(low_t, low_all)
    for d in range(2, ctx):
        from_context(1, d)
    product(slice_p, held_p, low_all, sums_p)
    from_chips(1)
    from_twin(1)
    keeps[1].wait()
    product(slice_d, held_d, dy, sums_d)
    root = (2.0 / jnp.pi) ** 0.5
    part = count // ctx

    def finish(k, carry):
        here = pl.ds(pl.multiple_of(k * part, part), part)
        pair, dhid = sums_p[here, :], sums_d[here, :]
        gate, upper = pair[:, :columns], pair[:, columns:]
        square = gate * gate
        tanh = jnp.tanh(root * gate * (1.0 + 0.044715 * square))
        gelu = 0.5 * gate * (1.0 + tanh)
        slope = 0.5 * (1.0 + tanh) + 0.5 * gate * (1.0 - tanh * tanh) * root * (
            1.0 + 3.0 * 0.044715 * square
        )
        hid[here, :] = cast(gelu * upper)
        dpair[here, :columns] = cast(dhid * upper * slope)
        dpair[here, columns:] = cast(dhid * gelu)
        return carry

    lax.fori_loop(0, ctx, finish, 0)
    out.drain()


def mlp_forward(att, hidden, scale, dy_all, part_p, part_d, slice_o, fs, ctx, ten, ident):
    rows, columns = part_d.shape[1:]
    t_rows, width = hidden.shape
    count = ctx * ten * t_rows
    chips = fs // 2
    sends = 2 * (ten - 1) + 2 * ctx + 2 * (ctx - 1) * (ten - 1) + 2 * (3 * ctx - 1 + 3 * ctx * chips)
    dma = pltpu.SemaphoreType.DMA
    shape = jax.ShapeDtypeStruct
    return pl.pallas_call(
        functools.partial(forward_kernel, fs, ctx, ten),
        out_shape=[
            shape((fs, ctx, rows, 2 * columns), half_type),
            shape((fs, ctx, rows, columns), half_type),
            shape((count, columns), half_type),
            shape((count, 2 * columns), half_type),
            shape((fs, ctx, rows, count), half_type),
            shape((fs, ctx, rows, count), half_type),
            shape((t_rows, width), single),
        ],
        in_specs=[VMEM] * 4 + [ANY] * 3,
        out_specs=[ANY] * 2 + [VMEM] * 5,
        scratch_shapes=[
            pltpu.VMEM((ctx, ten, t_rows, width), half_type),
            pltpu.VMEM((1, ten, t_rows, width), half_type),
            pltpu.VMEM((ten, t_rows, width), half_type),
            pltpu.VMEM((2, 2, ctx, *slice_o.shape[2:]), half_type),
            pltpu.VMEM((2, 2, ctx, rows, 2 * columns), half_type),
            pltpu.VMEM((2, 2, ctx, rows, columns), half_type),
            pltpu.VMEM((count, 2 * columns), single),
            pltpu.VMEM((count, columns), single),
            dma((2,)),
            dma((2,)),
            dma((sends,)),
            dma((fs, ctx)),
            dma((fs, ctx)),
            dma((ctx, ten)),
            dma((ten,)),
        ],
        compiler_params=pltpu.CompilerParams(
            collective_id=ident, has_side_effects=True, vmem_limit_bytes=VMEM_ALL
        ),
        name=f"mlp_forward_{ident}",
    )(att, hidden, scale, dy_all, part_p, part_d, slice_o)


def token_products(source, left, weight, held, load):
    def use(k, tile):
        term = lax.dot_general(
            left[...], tile, (((1,), (1,)), ((), ())), preferred_element_type=single
        )
        deep = tile.shape[0]
        lanes = pl.ds(pl.multiple_of(k * deep, deep), deep)
        source[:, :, :, lanes] = cast(term).reshape(*source.shape[:3], deep)

    chip_tiles(weight, held, load, use)


def token_start(source, first, recv, out, beside, order):
    for owner in order:
        for k, other in enumerate(beside):
            out.push(
                source.at[owner, other], first.at[k, owner], recv.at[k, owner], {"tensor": other}
            )


def token_sum(owner, places, source, first, recv, slots, sem, x):
    total = source[owner, x].astype(single)
    for k in range(first.shape[0]):
        arrived(first.at[k, owner], recv.at[k, owner], {"tensor": x})
        total = total + first[k, owner].astype(single)
    return collect(total, slots, sem, places, {"tensor": x})


def token_send(send, source, first, recv, slots, sem, x, out):
    owner, partner, slot, places = send
    mine = source.at[owner, x]
    mine[...] = cast(token_sum(owner, places, source, first, recv, slots, sem, x))
    out.push(mine, slots.at[slot], sem.at[slot], {"context": partner})


def back_kernel(fs, ctx, ten, *refs):
    low_t, dy_t, hid, dpair, mid, cot, scale, slice_p, slice_o = refs[:9]
    dmid, dmid_all, datt, terms, out_p, out_d = refs[9:15]
    dws, nears, fars = refs[15:17], refs[17:19], refs[19:21]
    source, first, line, held, held_o, sums = refs[21:27]
    load, local, send, recv_c, recv_y, recv_z, recv_tx, recv_t, recv_x = refs[27:]
    f, y, core, twin, across = fsdp_place(fs)
    z, x = lax.axis_index("context"), lax.axis_index("tensor")
    chips = fs // 2
    around = [lax.rem(z + d, ctx) for d in range(ctx)]
    beside = [lax.rem(x + d, ten) for d in range(1, ten)]
    rows_of = [lax.rem(y + d, chips) for d in range(chips)]
    chip_order = rows_of[1:] + rows_of[:1]
    order = around[1:] + around[:1]
    greet([{"context": k} for k in around[1:]] + across + [twin] + [{"tensor": k} for k in beside])
    out = Sends(send)
    outs = (out_d, out_p)
    keeps = []

    def products(w):
        left, right = (dy_t, low_t)[w], (hid, dpair)[w]
        for row in chip_order:
            fill_product(dws[w], left, right, row * 2 + 1 - core, ctx)
            out.push(dws[w].at[row * 2 + 1 - core], nears[w].at[row], recv_c.at[w, row], twin)
        for row in chip_order:
            fill_product(dws[w], left, right, row * 2 + core, ctx)

    def over_chips(w):
        for k, row in enumerate(rows_of[1:]):
            arrived(nears[w].at[row], recv_c.at[w, row], twin)
            for d, owner in enumerate(order):
                mine = dws[w].at[row * 2 + core, owner]
                mine[...] = cast(mine[...].astype(single) + nears[w][row, owner].astype(single))
                out.push(mine, fars[w].at[k, d], recv_y.at[w, k, d], across[k])

    def over_context(w, d):
        if d == 0:
            arrived(nears[w].at[y], recv_c.at[w, y], twin)
        owner = order[d]
        mine = dws[w].at[f, owner]
        total = mine[...].astype(single) + nears[w][y, owner].astype(single)
        for k in range(chips - 1):
            arrived(fars[w].at[k, d], recv_y.at[w, k, d], twin)
            total = total + fars[w][k, d].astype(single)
        mine[...] = cast(total)
        if d < ctx - 1:
            out.push(mine, outs[w].at[z], recv_z.at[w, z], {"context": owner})
        else:
            keep = pltpu.make_async_copy(mine, outs[w].at[z], local.at[w])
            keep.start()
            keeps.append(keep)

    sends, own_slots = halving(z, ctx)
    owners = [send[0] for send in sends] + [z]
    products(0)
    over_chips(0)
    token_products(source, dpair, slice_p, held, load)
    token_start(source, first, recv_tx, out, beside, owners)
    over_context(0, 0)
    products(1)
    over_chips(1)
    for d, send_z in enumerate(sends):
        token_send(send_z, source, first, recv_tx, line, recv_t, x, out)
        over_context(0, d + 1)
    dnorm = token_sum(z, own_slots, source, first, recv_tx, line, recv_t, x)
    values = mid[...]
    inverse = lax.rsqrt(jnp.mean(values * values, axis=-1, keepdims=True) + norm_eps)
    normed = values * inverse
    dnormed = dnorm * (1.0 + scale[...])
    terms[...] = jnp.sum(dnorm * normed, axis=0, keepdims=True)
    total = cot[...] + inverse * (
        dnormed - normed * jnp.mean(dnormed * normed, axis=-1, keepdims=True)
    )
    dmid[...] = total
    dmid_all[x] = cast(total)
    for other in beside:
        out.push(dmid_all.at[x], dmid_all.at[x], recv_x.at[x], {"tensor": other})
    for d in range(ctx):
        over_context(1, d)
    for other in beside:
        arrived(dmid_all.at[other], recv_x.at[other], twin)
    count, width = dmid_all.shape[0] * dmid_all.shape[1], dmid_all.shape[2]
    deep = width // chips

    def use(k, tile):
        lanes = pl.ds(pl.multiple_of(k * deep, deep), deep)
        add = jnp.dot(
            dmid_all[:, :, lanes].reshape(count, deep), tile, preferred_element_type=single
        )

        @pl.when(k == 0)
        def _():
            sums[...] = add

        @pl.when(k > 0)
        def _():
            sums[...] += add

    chip_tiles(slice_o, held_o, load, use)
    datt[...] = cast(sums[...])
    for w in range(2):
        for k in around[1:]:
            arrived(outs[w].at[k], recv_z.at[w, k], twin)
    for keep in keeps:
        keep.wait()
    out.drain()


def mlp_back(low_t, dy_t, hid, dpair, mid, cot, scale, slice_p, slice_o, fs, ctx, ten, ident):
    rows, columns = low_t.shape[2], hid.shape[1]
    t_rows, width = mid.shape
    chips = fs // 2
    blocks = [(rows, columns), (rows, 2 * columns)]
    sends = ctx * (ten - 1) + 2 * ctx + 2 * (chips + (chips - 1) * ctx + ctx - 1) + ten - 1
    dma = pltpu.SemaphoreType.DMA
    shape = jax.ShapeDtypeStruct
    return pl.pallas_call(
        functools.partial(back_kernel, fs, ctx, ten),
        out_shape=[
            shape((t_rows, width), single),
            shape((ten, t_rows, width), half_type),
            shape((ten * t_rows, slice_o.shape[3]), half_type),
            shape((1, width), single),
            shape((ctx, rows, 2 * columns), half_type),
            shape((ctx, rows, columns), half_type),
        ],
        in_specs=[VMEM] * 7 + [ANY] * 2,
        out_specs=[VMEM] * 4 + [ANY] * 2,
        scratch_shapes=[pltpu.VMEM((fs, ctx, *b), half_type) for b in blocks]
        + [pltpu.VMEM((chips, ctx, *b), half_type) for b in blocks]
        + [pltpu.VMEM((chips - 1, ctx, *b), half_type) for b in blocks]
        + [
            pltpu.VMEM((ctx, ten, t_rows, width), half_type),
            pltpu.VMEM((ten - 1, ctx, t_rows, width), half_type),
            pltpu.VMEM((ctx, t_rows, width), half_type),
            pltpu.VMEM((2, 2, ctx, rows, 2 * columns), half_type),
            pltpu.VMEM((2, 2, ctx, *slice_o.shape[2:]), half_type),
            pltpu.VMEM((ten * t_rows, slice_o.shape[3]), single),
            dma((2,)),
            dma((2,)),
            dma((sends,)),
            dma((2, chips)),
            dma((2, chips - 1, ctx)),
            dma((2, ctx)),
            dma((ten - 1, ctx)),
            dma((ctx + 1,)),
            dma((ten,)),
        ],
        compiler_params=pltpu.CompilerParams(
            collective_id=ident, has_side_effects=True, vmem_limit_bytes=VMEM_ALL
        ),
        name=f"mlp_back_{ident}",
    )(low_t, dy_t, hid, dpair, mid, cot, scale, slice_p, slice_o)


def update_kernel(parts, *refs):
    count = len(refs) // 7
    for w in range(count):
        weight, first, second = refs[3 * w : 3 * w + 3]
        outs = refs[3 * count + 4 * w : 3 * count + 4 * w + 4]
        columns = weight.shape[1] // parts.shape[0]
        for k in range(parts.shape[0]):
            grad = parts[k, :, w * columns : (w + 1) * columns].astype(single)
            here = (slice(None), slice(k * columns, (k + 1) * columns))
            values = (grad, *adamw(weight[here], grad, first[here], second[here]))
            for out, value in zip(outs, values):
                out[here] = value


def update(parts, weights, ident):
    ctx, rows, columns = parts.shape
    step = 32 if rows % 32 == 0 else 8
    wide = weights[0][0].shape[1]
    spec = pl.BlockSpec((step, wide), lambda i: (i, 0))
    part = pl.BlockSpec((ctx, step, columns), lambda i: (0, i, 0))
    count = len(weights)
    outs = pl.pallas_call(
        update_kernel,
        grid=(rows // step,),
        out_shape=[jax.ShapeDtypeStruct((rows, wide), single)] * (4 * count),
        in_specs=[part] + [spec] * (3 * count),
        out_specs=[spec] * (4 * count),
        compiler_params=pltpu.CompilerParams(vmem_limit_bytes=VMEM_ALL),
        name=f"update_{ident}",
    )(parts, *(v for group in weights for v in group))
    return [outs[4 * w : 4 * w + 4] for w in range(count)]


def attn_kernel(fs, ctx, ten, *refs):
    low_t, dmid_t, d_query, att, own, cosine, sine, hidden, mid, dmid, scale, terms = refs[:12]
    hid, slice_d, slice_q = refs[12:15]
    out_q, out_o, out_s, out_kv, tokens = refs[15:20]
    dws, nears, fars, lines = refs[20:25], refs[25:30], refs[30:35], refs[35:40]
    source, first, line, first_k, line_k, d_qkv, dnorm, take = refs[40:48]
    held_d, held_q, tail, pool, own_sums = refs[48:53]
    load, send, recv_c, recv_y, recv_z, recv_tx, recv_t, recv_kx, recv_k, recv_n, recv_x = refs[53:]
    f, y, core, twin, across = fsdp_place(fs)
    z, x = lax.axis_index("context"), lax.axis_index("tensor")
    chips = fs // 2
    rows = low_t.shape[2]
    beside = [lax.rem(x + d, ten) for d in range(1, ten)]
    rows_of = [lax.rem(y + d, chips) for d in range(chips)]
    chip_order = rows_of[1:] + rows_of[:1]
    partners = [{"context": partner} for partner, _, _ in doubling(z, ctx)]
    greet(partners + across + [twin] + [{"tensor": k} for k in beside])
    out = Sends(send)
    sends, own_slots = halving(z, ctx)
    order = [send_z[0] for send_z in sends] + [z]
    kinds = (cast, cast, cast, cast, lambda v: v)
    heads = d_query.shape[1]
    widths = [dw.shape[-1] for dw in dws[:4]]
    rights = (
        d_qkv.at[:, : widths[0]],
        d_qkv.at[:, widths[0] :],
        att.at[:, : widths[2]],
        att.at[:, widths[2] :],
    )
    lefts = (low_t, low_t, dmid_t, dmid_t)

    def start(w):
        for row in chip_order:
            owner = row * 2 + 1 - core
            if w < 4:
                fill_product(dws[w], lefts[w], rights[w], owner, ctx)
            out.push(dws[w].at[owner], nears[w].at[row], recv_c.at[w, row], twin)
        if w < 4:
            for row in chip_order:
                fill_product(dws[w], lefts[w], rights[w], row * 2 + core, ctx)

    def over_chips(w):
        for k, row in enumerate(rows_of[1:]):
            arrived(nears[w].at[row], recv_c.at[w, row], twin)
            for owner in order:
                mine = dws[w].at[row * 2 + core, owner]
                mine[...] = kinds[w](mine[...].astype(single) + nears[w][row, owner].astype(single))
                out.push(mine, fars[w].at[k, owner], recv_y.at[w, k, owner], across[k])

    def summed_block(w, owner, places):
        total = dws[w][f, owner].astype(single) + nears[w][y, owner].astype(single)
        for k in range(chips - 1):
            arrived(fars[w].at[k, owner], recv_y.at[w, k, owner], twin)
            total = total + fars[w][k, owner].astype(single)
        return collect(total, lines[w], recv_z.at[w], places, twin)

    def over_context(w, d):
        if d == 0:
            arrived(nears[w].at[y], recv_c.at[w, y], twin)
        owner, partner, slot, places = sends[d]
        mine = dws[w].at[f, owner]
        mine[...] = kinds[w](summed_block(w, owner, places))
        out.push(mine, lines[w].at[slot], recv_z.at[w, slot], {"context": partner})

    def finish(w):
        return summed_block(w, z, own_slots)

    own_sums[...] = own[...]
    token_start(own_sums, first_k, recv_kx, out, beside, order)
    start(2)
    over_chips(2)
    token_products(source, hid, slice_d, held_d, load)
    token_start(source, first, recv_tx, out, beside, order)
    start(3)
    over_chips(3)
    early, late = range(ctx // 2), range(ctx // 2, ctx - 1)
    for d in early:
        token_send(sends[d], own_sums, first_k, recv_kx, line_k, recv_k, x, out)
    for d in early:
        over_context(2, d)
    for d in late:
        token_send(sends[d], own_sums, first_k, recv_kx, line_k, recv_k, x, out)
    summed = token_sum(z, own_slots, own_sums, first_k, recv_kx, line_k, recv_k, x)
    half = summed.shape[1] // 2
    a, b = summed[:, :half], summed[:, half:]
    c, s = cosine[...], sine[...]
    is_key = x == 0
    d_qkv[:, :heads] = d_query[...]
    d_qkv[:, heads : heads + half] = cast(jnp.where(is_key, a * c + b * s, a))
    d_qkv[:, heads + half :] = cast(jnp.where(is_key, b * c - a * s, b))
    start(0)
    over_chips(0)
    for d in late:
        over_context(2, d)
    token_products(dnorm, d_qkv, slice_q, held_q, load)
    for other in beside:
        out.push(dnorm.at[0, other], take.at[x], recv_n.at[x], {"tensor": other})
    for d in early:
        token_send(sends[d], source, first, recv_tx, line, recv_t, x, out)
    for d in early:
        over_context(3, d)
    start(1)
    for d in late:
        token_send(sends[d], source, first, recv_tx, line, recv_t, x, out)
    for d in late:
        over_context(3, d)
    dnorm_one = dnorm[0, x].astype(single)
    for other in beside:
        arrived(take.at[other], recv_n.at[other], twin)
        dnorm_one = dnorm_one + take[other].astype(single)
    values = hidden[...]
    inverse = lax.rsqrt(jnp.mean(values * values, axis=-1, keepdims=True) + norm_eps)
    normed = values * inverse
    dnormed = dnorm_one * (1.0 + scale[...])
    tokens[x, 1] = cast(
        dmid[...]
        + inverse * (dnormed - normed * jnp.mean(dnormed * normed, axis=-1, keepdims=True))
    )
    sums = jnp.sum(dnorm_one * normed, axis=0, keepdims=True)
    dws[4][...] = jnp.zeros_like(dws[4])
    for j in range(fs * ctx):
        at = slice(j * rows, (j + 1) * rows)
        dws[4][j // ctx, j % ctx, 0:1, :rows] = sums[:, at]
        dws[4][j // ctx, j % ctx, 1:2, :rows] = terms[:, at]
    start(4)
    over_chips(4)
    over_chips(1)

    def hand_over(t):
        for other in beside:
            out.push(tokens.at[x, t], tokens.at[x, t], recv_x.at[2 + t, x], {"tensor": other})

    hand_over(1)
    for d in early:
        over_context(0, d)
    tokens[x, 0] = cast(
        mid[...] + token_sum(z, own_slots, source, first, recv_tx, line, recv_t, x)
    )
    hand_over(0)
    for d in early:
        over_context(4, d)
    for d in late:
        over_context(0, d)
    for d in early:
        over_context(1, d)
    for w in (4, 1):
        for d in late:
            over_context(w, d)
    pool[x] = finish(4)
    for other in beside:
        out.push(pool.at[x], pool.at[x], recv_x.at[0, x], {"tensor": other})
    out_o[:, : widths[2]] = finish(2)
    out_o[:, widths[2] :] = finish(3)
    out_q[:, : widths[0]] = finish(0)
    grad = finish(1)
    out_q[:, widths[0] :] = grad[:, : heads - widths[0]]
    tail[x] = cast(grad[:, heads - widths[0] :])
    for other in beside:
        out.push(tail.at[x], tail.at[x], recv_x.at[1, x], {"tensor": other})
    for other in beside:
        arrived(pool.at[other], recv_x.at[0, other], twin)
        arrived(tail.at[other], recv_x.at[1, other], twin)
        for t in range(2):
            arrived(tokens.at[other, t], recv_x.at[2 + t, other], twin)
    total = pool[0]
    for k in range(1, ten):
        total = total + pool[k]
    out_s[...] = total
    columns = tail.shape[-1]
    for k in range(ten):
        out_kv[:, k * columns : (k + 1) * columns] = tail[k].astype(single)
    out.drain()


def attn_back(
    low_t, dmid_t, d_query, att, own, cosine, sine, hidden, mid, dmid, scale, terms, hid, slice_d, slice_q,
    fs, ctx, ten, ident,
):
    rows = low_t.shape[2]
    t_rows, width = mid.shape
    chips = fs // 2
    heads = d_query.shape[1]
    count, tail = own.shape[2:]
    lanes = -(-rows // 128) * 128
    cuts = [-(-total // 256) * 128 for total in (heads + tail, att.shape[1])]
    both = [
        ((rows, cuts[0]), half_type),
        ((rows, heads + tail - cuts[0]), half_type),
        ((rows, cuts[1]), half_type),
        ((rows, att.shape[1] - cuts[1]), half_type),
        ((8, lanes), single),
    ]
    sends = (
        2 * (ctx * (ten - 1) + 2 * ctx)
        + 5 * (ten - 1)
        + 5 * (chips + (chips - 1) * ctx + 2 * ctx)
    )
    dma = pltpu.SemaphoreType.DMA
    shape = jax.ShapeDtypeStruct
    return pl.pallas_call(
        functools.partial(attn_kernel, fs, ctx, ten),
        out_shape=[
            shape((rows, heads), single),
            shape((rows, att.shape[1]), single),
            shape((8, lanes), single),
            shape((rows, ten * tail), single),
            shape((ten, 2, t_rows, width), half_type),
        ],
        in_specs=[VMEM] * 13 + [ANY] * 2,
        out_specs=[VMEM] * 5,
        scratch_shapes=[pltpu.VMEM((fs, ctx, *b), t) for b, t in both]
        + [pltpu.VMEM((chips, ctx, *b), t) for b, t in both]
        + [pltpu.VMEM((chips - 1, ctx, *b), t) for b, t in both]
        + [pltpu.VMEM((ctx + 1, *b), t) for b, t in both]
        + [
            pltpu.VMEM((ctx, ten, t_rows, width), half_type),
            pltpu.VMEM((ten - 1, ctx, t_rows, width), half_type),
            pltpu.VMEM((ctx + 1, t_rows, width), half_type),
            pltpu.VMEM((ten - 1, ctx, count, tail), half_type),
            pltpu.VMEM((ctx + 1, count, tail), half_type),
            pltpu.VMEM((count, heads + tail), half_type),
            pltpu.VMEM((1, ten, t_rows, width), half_type),
            pltpu.VMEM((ten, t_rows, width), half_type),
            pltpu.VMEM((2, 2, ctx, *slice_d.shape[2:]), half_type),
            pltpu.VMEM((2, 2, ctx, *slice_q.shape[2:]), half_type),
            pltpu.VMEM((ten, rows, tail), half_type),
            pltpu.VMEM((ten, 8, lanes), single),
            pltpu.VMEM(own.shape, half_type),
            dma((2,)),
            dma((sends,)),
            dma((5, chips)),
            dma((5, chips - 1, ctx)),
            dma((5, ctx + 1)),
            dma((ten - 1, ctx)),
            dma((ctx + 1,)),
            dma((ten - 1, ctx)),
            dma((ctx + 1,)),
            dma((ten,)),
            dma((4, ten)),
        ],
        compiler_params=pltpu.CompilerParams(
            collective_id=ident, has_side_effects=True, vmem_limit_bytes=VMEM_ALL
        ),
        name=f"attn_back_{ident}",
    )(low_t, dmid_t, d_query, att, own, cosine, sine, hidden, mid, dmid, scale, terms, hid, slice_d, slice_q)


def on_device(hidden_in, cotangent, segment_ids, positions, *params):
    masters, firsts, seconds = params[:8], params[8:16], params[16:]
    (
        attn_scale,
        query_weight,
        keyval_weight,
        output_weight,
        mlp_scale,
        gate_weight,
        up_weight,
        down_weight,
    ) = masters
    fs, ctx, ten = (lax.axis_size(name) for name in ("fsdp", "context", "tensor"))
    x = lax.axis_index("tensor")
    context_index = lax.axis_index("context")
    block, width = hidden_in.shape[1:]
    rows = query_weight.shape[0]
    half_rows = block // ten
    heads_width = query_weight.shape[1]
    heads_here = heads_width // HD
    hidden = hidden_in[0]
    cot = cotangent[0]
    hidden_half = lax.dynamic_slice_in_dim(hidden, x * half_rows, half_rows, 0)
    cot_half = lax.dynamic_slice_in_dim(cot, x * half_rows, half_rows, 0)
    is_key = x == 0

    qkv_block = jnp.concatenate(
        [
            cast(query_weight),
            cast(lax.dynamic_slice_in_dim(keyval_weight, x * HD, HD, 1)),
        ],
        axis=1,
    )
    lanes = -(-max(rows, block) // 128) * 128
    wide = [
        jnp.pad(v, (0, lanes - v.shape[0]))
        for v in (attn_scale, mlp_scale, segment_ids[0].astype(single))
    ]
    small = jnp.stack(wide + [jnp.zeros((lanes,), single)] * 5)
    small_all, qkv_all, out_all, dy_all, part_p, part_d = spread(
        [small, qkv_block, cast(output_weight.T)],
        cast(cot_half),
        [gate_weight, up_weight, down_weight.T],
        fs,
        ctx,
        ten,
        1,
    )
    scale_one = cast(small_all[:, :, 0, :rows].reshape(-1)).astype(single)
    scale_two = cast(small_all[:, :, 1, :rows].reshape(-1)).astype(single)
    f = lax.axis_index("fsdp")
    seg_all = lax.dynamic_index_in_dim(small_all[:, :, 2, :block], f, 0, False).reshape(-1)
    qkv_full = qkv_all.reshape(width, -1)

    _, _, low_one = rms_forward(hidden, scale_one)
    qkv = dot(low_one, qkv_full, ((1,), (0,)))
    query = qkv[:, :heads_width].reshape(block, heads_here, HD)
    own = qkv[:, heads_width:]
    cosine, sine = rope_tables(positions[0])
    query_low = cast(rotate(query, cosine[:, None, :], sine[:, None, :]) * HD ** (-0.5))
    own_low = cast(jnp.where(is_key, rotate(own, cosine, sine), own))
    keyval_all = tokens_to_all(own_low, ctx, ten, 2).reshape(ctx, ten, block, HD)
    keys_all = keyval_all[:, 0].reshape(-1, HD)
    values_all = keyval_all[:, 1].reshape(-1, HD)
    rows_index = context_index * block + jnp.arange(block, dtype=jnp.int32)
    cols_index = jnp.arange(keys_all.shape[0], dtype=jnp.int32)
    allowed = (rows_index[:, None] >= cols_index[None, :]) & (
        segment_ids[0].astype(single)[:, None] == seg_all[None, :]
    )
    scores = jnp.einsum("bhd,jd->hbj", query_low, keys_all, preferred_element_type=single)
    masked = jnp.where(allowed, scores, masked_value)
    top = jnp.max(masked, axis=-1, keepdims=True)
    total = jnp.sum(jnp.where(allowed, jnp.exp(masked - top), 0.0), axis=-1, keepdims=True)
    lse = top + jnp.log(total)
    prob = jnp.where(allowed, jnp.exp(masked - lse), 0.0)
    prob_low = cast(prob)
    att_low = cast(
        jnp.einsum("hbj,jd->bhd", prob_low, values_all, preferred_element_type=single)
    )
    att_flat = att_low.reshape(block, heads_width)
    slice_p, slice_d, hid, dpair, low_t, dy_t, mid_half = mlp_forward(
        att_flat,
        hidden_half,
        scale_two[None],
        dy_all,
        part_p,
        part_d,
        out_all,
        fs,
        ctx,
        ten,
        4,
    )
    dmid_half, dmid_low, datt, terms_two, part_p, part_d = mlp_back(
        low_t, dy_t, hid, dpair, mid_half, cot_half, scale_two[None], slice_p, out_all, fs, ctx, ten, 5
    )

    dmid_low = dmid_low.reshape(block, width)
    datt_low = datt.reshape(block, heads_here, HD)
    delta = jnp.einsum("bhd,bhd->hb", datt_low, att_low, preferred_element_type=single)
    dprob = jnp.einsum("bhd,jd->hbj", datt_low, values_all, preferred_element_type=single)
    dscore_low = cast(prob * (dprob - delta[..., None]))
    dquery = jnp.einsum("hbj,jd->bhd", dscore_low, keys_all, preferred_element_type=single)
    dkey_part = jnp.einsum("hbj,bhd->jd", dscore_low, query_low, preferred_element_type=single)
    dvalue_part = jnp.einsum("hbj,bhd->jd", prob_low, datt_low, preferred_element_type=single)
    own_part = jnp.stack(
        [cast(part).reshape(ctx, block, HD) for part in (dkey_part, dvalue_part)], axis=1
    )
    dquery_low = cast(
        unrotate(dquery, cosine[:, None, :], sine[:, None, :]) * HD ** (-0.5)
    ).reshape(block, heads_width)
    row_blocks = (fs, ctx, rows, -1)
    grad_wq, grad_wo, grad_s, grad_wkv, outs = attn_back(
        low_one.T.reshape(row_blocks),
        dmid_low.T.reshape(row_blocks),
        dquery_low,
        att_flat,
        own_part,
        cosine,
        sine,
        hidden_half,
        mid_half,
        dmid_half,
        scale_one[None],
        terms_two,
        hid,
        slice_d,
        qkv_all,
        fs,
        ctx,
        ten,
        9,
    )
    outs = outs.transpose(1, 0, 2, 3).reshape(2, 1, block, width).astype(single)

    grads = (grad_s[0, :rows], grad_wq, grad_wkv, grad_wo.T, grad_s[1, :rows])
    results = [
        (grad, *adamw(weight, grad, first, second))
        for weight, grad, first, second in zip(masters, grads, firsts, seconds)
    ]
    groups = list(zip(masters, firsts, seconds))
    results += update(part_p, groups[5:7], 5)
    results += [[v.T for v in update(part_d, [[v.T for v in groups[7]]], 7)[0]]]
    return (
        outs[0],
        outs[1],
        *(entry[0] for entry in results),
        *(entry[1] for entry in results),
        *(entry[2] for entry in results),
        *(entry[3] for entry in results),
    )


def solution(mesh):
    both = ("fsdp", "context")
    tokens = P("fsdp", "context", None)
    weights = (
        P(both),
        P(both, "tensor"),
        P(both, None),
        P("tensor", both),
        P(both),
        P(both, "tensor"),
        P(both, "tensor"),
        P("tensor", both),
    )
    return jax.shard_map(
        on_device,
        mesh=mesh,
        in_specs=(tokens, tokens, P("fsdp", "context"), P("fsdp", "context"), *(weights * 3)),
        out_specs=(tokens, tokens, *(weights * 4)),
        check_vma=False,
    )
```

```python
import functools

import jax
import jax.numpy as jnp
from jax import lax
from jax.experimental import pallas as pl
from jax.experimental.pallas import tpu as pltpu
from jax.sharding import PartitionSpec as P

HD = 256


norm_eps = 1e-06
beta_one = 0.9
beta_two = 0.999
adam_eps = 1e-08
learn_rate = 0.03
decay_rate = 0.1
adam_step = 4.0
rope_base = 10000.0
masked_value = -1e30

single = jnp.float32
half_type = jnp.bfloat16


def gelu_tanh(values):
    return jax.nn.gelu(values, approximate=True)


def rope_tables(positions):
    half = HD // 2
    freq = rope_base ** (-2.0 * jnp.arange(half).astype(jnp.float32) / HD)
    angle = positions.astype(jnp.float32)[..., None] * freq
    return (jnp.cos(angle), jnp.sin(angle))


def rotate(values, cosine, sine):
    half = values.shape[-1] // 2
    first = values[..., :half]
    second = values[..., half:]
    return jnp.concatenate(
        [first * cosine - second * sine, second * cosine + first * sine], axis=-1
    )


def unrotate(values, cosine, sine):
    half = values.shape[-1] // 2
    first = values[..., :half]
    second = values[..., half:]
    return jnp.concatenate(
        [first * cosine + second * sine, second * cosine - first * sine], axis=-1
    )


def rms_forward(values, scale):
    inverse = lax.rsqrt(jnp.mean(values * values, axis=-1, keepdims=True) + norm_eps)
    normed = values * inverse
    return (normed, inverse, (normed * (1.0 + scale)).astype(jnp.bfloat16))


def rms_backward(dnorm, normed, inverse, scale):
    dnormed = dnorm * (1.0 + scale)
    dvalues = inverse * (dnormed - normed * jnp.mean(dnormed * normed, axis=-1, keepdims=True))
    return (dvalues, dnorm * normed)


def adamw(weight, grad, first, second):
    first_new = beta_one * first + (1.0 - beta_one) * grad
    second_new = beta_two * second + (1.0 - beta_two) * grad * grad
    fix_one = 1.0 - beta_one**adam_step
    fix_two = 1.0 - beta_two**adam_step
    update = first_new / fix_one / (jnp.sqrt(second_new / fix_two) + adam_eps)
    return (weight - learn_rate * (update + decay_rate * weight), first_new, second_new)


def dot(a, b, dims):
    return lax.dot_general(a, b, (dims, ((), ())), preferred_element_type=single)


MESH = pl.DeviceIdType.MESH
ANY = pl.BlockSpec(memory_space=pl.ANY)
VMEM = pl.BlockSpec(memory_space=pltpu.VMEM)


def greet(peers):
    barrier = pltpu.get_barrier_semaphore()
    for peer in peers:
        pl.semaphore_signal(barrier, inc=1, device_id=peer, device_id_type=MESH)
    pl.semaphore_wait(barrier, len(peers))


def remote(src, dst, send, recv, peer):
    return pltpu.make_async_remote_copy(
        src_ref=src, dst_ref=dst, send_sem=send, recv_sem=recv, device_id=peer, device_id_type=MESH
    )


def arrived(dst, recv, peer):
    remote(dst, dst, recv, recv, peer).wait_recv()


def fsdp_place(fs):
    f = lax.axis_index("fsdp")
    core = lax.rem(f, 2)
    y = lax.div(f, 2)
    twin = {"fsdp": f + 1 - 2 * core}
    across = [{"fsdp": lax.rem(y + d, fs // 2) * 2 + core} for d in range(1, fs // 2)]
    return f, y, core, twin, across


class Sends:
    def __init__(self, send):
        self.send, self.made = send, []

    def push(self, src, dst, recv, peer, *conditions):
        copy = remote(src, dst, self.send.at[len(self.made)], recv, peer)
        self.made.append((copy, conditions))
        under(conditions, copy.start)

    def drain(self):
        for copy, conditions in self.made:
            under(conditions, copy.wait_send)


def under(conditions, action):
    if not conditions:
        action()
        return
    holds = conditions[0]
    for more in conditions[1:]:
        holds = jnp.logical_and(holds, more)
    pl.when(holds)(action)


def line_steps(z, ctx):
    for s in range(1, ctx):
        yield z - s, z >= s, z + 1, z + 1 < ctx
        yield z + s, z + s < ctx, z - 1, z >= 1


def tokens_kernel(ctx, ten, src, out, local, send, recv):
    z, x = lax.axis_index("context"), lax.axis_index("tensor")
    around = [lax.rem(z + d, ctx) for d in range(ctx)]
    across = [{"tensor": lax.rem(x + d, ten)} for d in range(1, ten)]
    greet([{"context": k} for k in around[1:]] + across)
    sends = []

    def push(ref, source, peer):
        copy = remote(ref, out.at[source, x], send.at[len(sends)], recv.at[source, x], peer)
        copy.start()
        sends.append(copy)

    for d in range(1, ctx):
        push(src, z, {"context": around[d]})
    for peer in across:
        push(src, z, peer)
    keep = pltpu.make_async_copy(src, out.at[z, x], local)
    keep.start()
    back = [lax.rem(z + ctx - d, ctx) for d in range(ctx)]
    for d in range(1, ctx):
        arrived(out.at[back[d], x], recv.at[back[d], x], {"context": back[d]})
        for peer in across:
            push(out.at[back[d], x], back[d], peer)
    for d in range(ctx):
        for peer in across:
            other = peer["tensor"]
            arrived(out.at[back[d], other], recv.at[back[d], other], peer)
    keep.wait()
    for copy in sends:
        copy.wait_send()


def tokens_to_all(block, ctx, ten, ident):
    sends = (ctx - 1) + ctx * (ten - 1)
    out = pl.pallas_call(
        functools.partial(tokens_kernel, ctx, ten),
        out_shape=jax.ShapeDtypeStruct((ctx, ten, *block.shape), block.dtype),
        in_specs=[VMEM],
        out_specs=VMEM,
        scratch_shapes=[
            pltpu.SemaphoreType.DMA(()),
            pltpu.SemaphoreType.DMA((sends,)),
            pltpu.SemaphoreType.DMA((ctx, ten)),
        ],
        compiler_params=pltpu.CompilerParams(collective_id=ident, has_side_effects=True),
        name=f"tokens_{ident}",
    )(block)
    return out.reshape(-1, block.shape[-1])


VMEM_ALL = 67043328


def cast(v):
    return v.astype(half_type)


def fill_product(dw, left, right, owner, ctx):
    def one(k, carry):
        dw[owner, k] = cast(
            lax.dot_general(
                left[owner, k], right[...], (((1,), (0,)), ((), ())), preferred_element_type=single
            )
        )
        return carry

    lax.fori_loop(0, ctx, one, 0)


def split_columns(ctx, weights, parts, wide, packed, small, load, store):
    columns = small.shape[-1]
    fetches = [pltpu.make_async_copy(weights[w], wide.at[w], load.at[w]) for w in range(3)]
    for fetch in fetches:
        fetch.start()
    for w in range(3):
        fetches[w].wait()
        for k in range(ctx):
            piece = cast(wide[w, :, k * columns : (k + 1) * columns])
            if w < 2:
                packed[k, :, w * columns : (w + 1) * columns] = piece
            else:
                small[k] = piece
    puts = [pltpu.make_async_copy(v, parts[j], store.at[j]) for j, v in enumerate((packed, small))]
    for put in puts:
        put.start()
    for put in puts:
        put.wait()


def first_kernel(fs, ctx, ten, count, *refs):
    srcs, weights = refs[: count + 1], refs[count + 1 : count + 4]
    refs = refs[count + 4 :]
    outs, parts = refs[: count + 1], refs[count + 1 : count + 3]
    wide, packed, small, load, store, local, send, recv, recv_t = refs[count + 3 :]
    f, y, core, twin, across = fsdp_place(fs)
    z, x = lax.axis_index("context"), lax.axis_index("tensor")
    beside = [{"tensor": lax.rem(x + d, ten)} for d in range(1, ten)]
    back = [lax.rem(z + ctx - d, ctx) for d in range(ctx)]
    up, down = {"context": z + 1}, {"context": z - 1}
    nxt, prv = lax.rem(z + 1, ctx), back[1]
    greet([{"context": nxt}, {"context": prv}] + across + [twin] + beside)
    out = Sends(send)
    keeps = []

    def where(w, source):
        if w == count:
            return outs[w].at[source, x], recv_t.at[source, x], beside
        return outs[w].at[f, source], recv.at[w, f, source], across + [twin]

    for w in range(count + 1):
        mine, sem, peers = where(w, z)
        out.push(srcs[w], mine, sem, up, z + 1 < ctx)
        out.push(srcs[w], mine, sem, down, z >= 1)
        for peer in peers:
            out.push(srcs[w], mine, sem, peer)
        keeps.append(pltpu.make_async_copy(srcs[w], mine, local.at[w]))
        keeps[-1].start()
    split_columns(ctx, weights, parts, wide, packed, small, load, store)
    for source, exists, onward, more in line_steps(z, ctx):
        for w in range(count + 1):
            block, sem, peers = where(w, source)
            under((exists,), lambda: arrived(block, sem, twin))
            out.push(block, block, sem, {"context": onward}, exists, more)
            for peer in peers:
                out.push(block, block, sem, peer, exists)
    chain = [(z, ())] + [(source, (exists,)) for source, exists, _, _ in line_steps(z, ctx)]
    for source, when in chain:
        for w in range(count):
            for peer in across:
                owner = peer["fsdp"]
                block, sem = outs[w].at[owner, source], recv.at[w, owner, source]
                under(when, lambda: arrived(block, sem, twin))
                out.push(block, block, sem, twin, *when)
    for source in back:
        for w in range(count):
            for step in range(fs // 2):
                owner = lax.rem(y + step, fs // 2) * 2 + 1 - core
                arrived(outs[w].at[owner, source], recv.at[w, owner, source], twin)
        for peer in beside:
            arrived(outs[count].at[source, peer["tensor"]], recv_t.at[source, peer["tensor"]], twin)
    for keep in keeps:
        keep.wait()
    out.drain()


def spread(blocks, tokens, weights, fs, ctx, ten, ident):
    count = len(blocks)
    chips = fs // 2
    lines = 2 + 2 * (ctx - 1)
    sends = count * (lines + (2 * ctx - 1) * (2 * chips - 1)) + lines + (2 * ctx - 1) * (ten - 1)
    rows, wide = weights[0].shape
    part = (ctx, rows, wide // ctx)
    pair = (ctx, rows, 2 * (wide // ctx))
    dma = pltpu.SemaphoreType.DMA
    return pl.pallas_call(
        functools.partial(first_kernel, fs, ctx, ten, count),
        out_shape=[jax.ShapeDtypeStruct((fs, ctx, *b.shape), b.dtype) for b in blocks]
        + [jax.ShapeDtypeStruct((ctx, ten, *tokens.shape), tokens.dtype)]
        + [jax.ShapeDtypeStruct(pair, half_type), jax.ShapeDtypeStruct(part, half_type)],
        in_specs=[ANY] * (count + 4),
        out_specs=[ANY] * (count + 3),
        scratch_shapes=[
            pltpu.VMEM((3, rows, wide), single),
            pltpu.VMEM(pair, half_type),
            pltpu.VMEM(part, half_type),
            dma((3,)),
            dma((2,)),
            dma((count + 1,)),
            dma((sends,)),
            dma((count, fs, ctx)),
            dma((ctx, ten)),
        ],
        compiler_params=pltpu.CompilerParams(
            collective_id=ident, has_side_effects=True, vmem_limit_bytes=VMEM_ALL
        ),
        name=f"spread_{ident}",
    )(*blocks, tokens, *weights)


def flip(k, bit):
    return k + bit - 2 * bit * lax.rem(lax.div(k, bit), 2)


def halving(z, ctx):
    sends, seen, base, bit = [], [], 0, 1
    while bit < ctx:
        count = ctx // (2 * bit)
        for u in range(count):
            owner = flip(z, bit) - 2 * bit * lax.div(z, 2 * bit) + 2 * bit * u
            sends.append((owner, flip(z, bit), base + u, [at + lax.div(owner, d) for at, d in seen]))
        seen.append((base, 2 * bit))
        base, bit = base + count, 2 * bit
    return sends, [at + lax.div(z, d) for at, d in seen]


def doubling(z, ctx):
    steps, held, bit = [], [z], ctx // 2
    while bit:
        got = [flip(k, bit) for k in held]
        steps.append((flip(z, bit), list(held), got))
        held, bit = held + got, bit // 2
    return steps


def collect(total, slots, sem, places, peer):
    for at in places:
        arrived(slots.at[at], sem.at[at], peer)
        total = total + slots[at].astype(single)
    return total


def chip_tiles(weight, held, load, use):
    chips = weight.shape[0] // 2

    def fetch(k, slot):
        return pltpu.make_async_copy(weight.at[pl.ds(2 * k, 2)], held.at[slot], load.at[slot])

    fetch(0, 0).start()

    def step(k, carry):
        slot = lax.rem(k, 2)
        fetch(k, slot).wait()

        @pl.when(k + 1 < chips)
        def _():
            fetch(k + 1, 1 - slot).start()

        use(k, held[slot].reshape(-1, held.shape[-1]))
        return carry

    lax.fori_loop(0, chips, step, 0)


def forward_kernel(fs, ctx, ten, *refs):
    att, hidden, scale, dy, part_p, part_d, slice_o = refs[:7]
    slice_p, slice_d, hid, dpair, low_t, dy_t, mid = refs[7:14]
    low_all, attn, take, held_o, held_p, held_d, sums_p, sums_d = refs[14:22]
    load, local, send, recv_p, recv_d, recv_t, recv_x = refs[22:]
    f, y, core, twin, across = fsdp_place(fs)
    z, x = lax.axis_index("context"), lax.axis_index("tensor")
    rows, columns = part_d.shape[1:]
    width = hidden.shape[1]
    count = hid.shape[0]
    beside = [{"tensor": lax.rem(x + d, ten)} for d in range(1, ten)]
    shifts = sorted(range(ctx), key=lambda d: (min(d, ctx - d), d))
    around = [lax.rem(z + d, ctx) for d in shifts]
    back = [lax.rem(z + ctx - d, ctx) for d in shifts]
    greet([{"context": k} for k in around[1:]] + across + [twin] + beside)
    out = Sends(send)
    parts, slices, recvs = (part_p, part_d), (slice_p, slice_d), (recv_p, recv_d)

    def block(w, owner, source):
        return slices[w].at[owner, source], recvs[w].at[owner, source]

    def to_context(w, d):
        dst, sem = block(w, f, z)
        out.push(parts[w].at[around[d]], dst, sem, {"context": around[d]})

    def from_context(w, d):
        dst, sem = block(w, f, back[d])
        arrived(dst, sem, twin)
        for peer in across + [twin]:
            out.push(dst, dst, sem, peer)

    def from_chips(w):
        for d in range(ctx):
            for peer in across:
                dst, sem = block(w, peer["fsdp"], back[d])
                arrived(dst, sem, twin)
                out.push(dst, dst, sem, twin)

    def from_twin(w):
        for d in range(ctx):
            for step in range(fs // 2):
                dst, sem = block(w, lax.rem(y + step, fs // 2) * 2 + 1 - core, back[d])
                arrived(dst, sem, twin)

    to_context(0, 1)
    keeps = []
    for w in range(2):
        dst, sem = block(w, f, z)
        for peer in across + [twin]:
            out.push(parts[w].at[z], dst, sem, peer)
        keeps.append(pltpu.make_async_copy(parts[w].at[z], dst, local.at[w]))
        keeps[-1].start()
    token_products(attn, att, slice_o, held_o, load)
    for peer in beside:
        out.push(attn.at[0, peer["tensor"]], take.at[x], recv_x.at[x], peer)
    total = hidden[...] + attn[0, x].astype(single)
    for peer in beside:
        other = peer["tensor"]
        arrived(take.at[other], recv_x.at[other], twin)
        total = total + take[other].astype(single)
    mid[...] = total
    inverse = lax.rsqrt(jnp.mean(total * total, axis=-1, keepdims=True) + norm_eps)
    low_all[z, x] = cast(total * inverse * (1.0 + scale[...]))
    mine = low_all.at[z, x]
    later = [(0, d) for d in range(2, ctx)] + [(1, d) for d in range(1, ctx)]
    early = [d for d in range(1, ctx)]
    steps = doubling(z, ctx)
    for partner, _, _ in steps:
        out.push(mine, mine, recv_t.at[z, x], {"context": partner})
    for peer in beside:
        out.push(mine, mine, recv_t.at[z, x], peer)
    to_context(*later.pop(0))
    from_context(0, early.pop(0))
    for step, (partner, _, got) in enumerate(steps):
        for source in got:
            here, sem = low_all.at[source, x], recv_t.at[source, x]
            arrived(here, sem, twin)
            for further, _, _ in steps[step + 1 :]:
                out.push(here, here, sem, {"context": further})
            for peer in beside:
                out.push(here, here, sem, peer)
            if early:
                from_context(0, early.pop(0))
            if later:
                to_context(*later.pop(0))
    while later:
        to_context(*later.pop(0))
    while early:
        from_context(0, early.pop(0))

    def turned(dst, src):
        for j in range(fs * ctx):
            piece = src[:, :, :, j * rows : (j + 1) * rows].reshape(count, rows)
            dst[j // ctx, j % ctx] = piece.T

    def product(weight, held, left, sums):
        deep = width // (fs // 2)

        def use(k, tile):
            lanes = pl.ds(pl.multiple_of(k * deep, deep), deep)
            add = jnp.dot(
                left[:, :, :, lanes].reshape(count, deep), tile, preferred_element_type=single
            )

            @pl.when(k == 0)
            def _():
                sums[...] = add

            @pl.when(k > 0)
            def _():
                sums[...] += add

        chip_tiles(weight, held, load, use)

    from_chips(0)
    turned(dy_t, dy)
    from_context(1, 1)
    for source in back:
        for peer in beside:
            other = peer["tensor"]
            arrived(low_all.at[source, other], recv_t.at[source, other], twin)
    from_twin(0)
    keeps[0].wait()
    turned(low_t, low_all)
    for d in range(2, ctx):
        from_context(1, d)
    product(slice_p, held_p, low_all, sums_p)
    from_chips(1)
    from_twin(1)
    keeps[1].wait()
    product(slice_d, held_d, dy, sums_d)
    root = (2.0 / jnp.pi) ** 0.5
    part = count // ctx

    def finish(k, carry):
        here = pl.ds(pl.multiple_of(k * part, part), part)
        pair, dhid = sums_p[here, :], sums_d[here, :]
        gate, upper = pair[:, :columns], pair[:, columns:]
        square = gate * gate
        tanh = jnp.tanh(root * gate * (1.0 + 0.044715 * square))
        gelu = 0.5 * gate * (1.0 + tanh)
        slope = 0.5 * (1.0 + tanh) + 0.5 * gate * (1.0 - tanh * tanh) * root * (
            1.0 + 3.0 * 0.044715 * square
        )
        hid[here, :] = cast(gelu * upper)
        dpair[here, :columns] = cast(dhid * upper * slope)
        dpair[here, columns:] = cast(dhid * gelu)
        return carry

    lax.fori_loop(0, ctx, finish, 0)
    out.drain()


def mlp_forward(att, hidden, scale, dy_all, part_p, part_d, slice_o, fs, ctx, ten, ident):
    rows, columns = part_d.shape[1:]
    t_rows, width = hidden.shape
    count = ctx * ten * t_rows
    chips = fs // 2
    sends = 2 * (ten - 1) + 2 * ctx + 2 * (ctx - 1) * (ten - 1) + 2 * (3 * ctx - 1 + 3 * ctx * chips)
    dma = pltpu.SemaphoreType.DMA
    shape = jax.ShapeDtypeStruct
    return pl.pallas_call(
        functools.partial(forward_kernel, fs, ctx, ten),
        out_shape=[
            shape((fs, ctx, rows, 2 * columns), half_type),
            shape((fs, ctx, rows, columns), half_type),
            shape((count, columns), half_type),
            shape((count, 2 * columns), half_type),
            shape((fs, ctx, rows, count), half_type),
            shape((fs, ctx, rows, count), half_type),
            shape((t_rows, width), single),
        ],
        in_specs=[VMEM] * 4 + [ANY] * 3,
        out_specs=[ANY] * 2 + [VMEM] * 5,
        scratch_shapes=[
            pltpu.VMEM((ctx, ten, t_rows, width), half_type),
            pltpu.VMEM((1, ten, t_rows, width), half_type),
            pltpu.VMEM((ten, t_rows, width), half_type),
            pltpu.VMEM((2, 2, ctx, *slice_o.shape[2:]), half_type),
            pltpu.VMEM((2, 2, ctx, rows, 2 * columns), half_type),
            pltpu.VMEM((2, 2, ctx, rows, columns), half_type),
            pltpu.VMEM((count, 2 * columns), single),
            pltpu.VMEM((count, columns), single),
            dma((2,)),
            dma((2,)),
            dma((sends,)),
            dma((fs, ctx)),
            dma((fs, ctx)),
            dma((ctx, ten)),
            dma((ten,)),
        ],
        compiler_params=pltpu.CompilerParams(
            collective_id=ident, has_side_effects=True, vmem_limit_bytes=VMEM_ALL
        ),
        name=f"mlp_forward_{ident}",
    )(att, hidden, scale, dy_all, part_p, part_d, slice_o)


def token_products(source, left, weight, held, load):
    def use(k, tile):
        term = lax.dot_general(
            left[...], tile, (((1,), (1,)), ((), ())), preferred_element_type=single
        )
        deep = tile.shape[0]
        lanes = pl.ds(pl.multiple_of(k * deep, deep), deep)
        source[:, :, :, lanes] = cast(term).reshape(*source.shape[:3], deep)

    chip_tiles(weight, held, load, use)


def token_start(source, first, recv, out, beside, order):
    for owner in order:
        for k, other in enumerate(beside):
            out.push(
                source.at[owner, other], first.at[k, owner], recv.at[k, owner], {"tensor": other}
            )


def token_sum(owner, places, source, first, recv, slots, sem, x):
    total = source[owner, x].astype(single)
    for k in range(first.shape[0]):
        arrived(first.at[k, owner], recv.at[k, owner], {"tensor": x})
        total = total + first[k, owner].astype(single)
    return collect(total, slots, sem, places, {"tensor": x})


def token_send(send, source, first, recv, slots, sem, x, out):
    owner, partner, slot, places = send
    mine = source.at[owner, x]
    mine[...] = cast(token_sum(owner, places, source, first, recv, slots, sem, x))
    out.push(mine, slots.at[slot], sem.at[slot], {"context": partner})


def back_kernel(fs, ctx, ten, *refs):
    low_t, dy_t, hid, dpair, mid, cot, scale, slice_p, slice_o = refs[:9]
    dmid, dmid_all, datt, terms, out_p, out_d = refs[9:15]
    dws, nears, fars = refs[15:17], refs[17:19], refs[19:21]
    source, first, line, held, held_o, sums = refs[21:27]
    load, local, send, recv_c, recv_y, recv_z, recv_tx, recv_t, recv_x = refs[27:]
    f, y, core, twin, across = fsdp_place(fs)
    z, x = lax.axis_index("context"), lax.axis_index("tensor")
    chips = fs // 2
    around = [lax.rem(z + d, ctx) for d in range(ctx)]
    beside = [lax.rem(x + d, ten) for d in range(1, ten)]
    rows_of = [lax.rem(y + d, chips) for d in range(chips)]
    chip_order = rows_of[1:] + rows_of[:1]
    order = around[1:] + around[:1]
    greet([{"context": k} for k in around[1:]] + across + [twin] + [{"tensor": k} for k in beside])
    out = Sends(send)
    outs = (out_d, out_p)
    keeps = []

    def products(w):
        left, right = (dy_t, low_t)[w], (hid, dpair)[w]
        for row in chip_order:
            fill_product(dws[w], left, right, row * 2 + 1 - core, ctx)
            out.push(dws[w].at[row * 2 + 1 - core], nears[w].at[row], recv_c.at[w, row], twin)
        for row in chip_order:
            fill_product(dws[w], left, right, row * 2 + core, ctx)

    def over_chips(w):
        for k, row in enumerate(rows_of[1:]):
            arrived(nears[w].at[row], recv_c.at[w, row], twin)
            for d, owner in enumerate(order):
                mine = dws[w].at[row * 2 + core, owner]
                mine[...] = cast(mine[...].astype(single) + nears[w][row, owner].astype(single))
                out.push(mine, fars[w].at[k, d], recv_y.at[w, k, d], across[k])

    def over_context(w, d):
        if d == 0:
            arrived(nears[w].at[y], recv_c.at[w, y], twin)
        owner = order[d]
        mine = dws[w].at[f, owner]
        total = mine[...].astype(single) + nears[w][y, owner].astype(single)
        for k in range(chips - 1):
            arrived(fars[w].at[k, d], recv_y.at[w, k, d], twin)
            total = total + fars[w][k, d].astype(single)
        mine[...] = cast(total)
        if d < ctx - 1:
            out.push(mine, outs[w].at[z], recv_z.at[w, z], {"context": owner})
        else:
            keep = pltpu.make_async_copy(mine, outs[w].at[z], local.at[w])
            keep.start()
            keeps.append(keep)

    sends, own_slots = halving(z, ctx)
    owners = [send[0] for send in sends] + [z]
    products(0)
    over_chips(0)
    token_products(source, dpair, slice_p, held, load)
    token_start(source, first, recv_tx, out, beside, owners)
    over_context(0, 0)
    products(1)
    over_chips(1)
    for d, send_z in enumerate(sends):
        token_send(send_z, source, first, recv_tx, line, recv_t, x, out)
        over_context(0, d + 1)
    dnorm = token_sum(z, own_slots, source, first, recv_tx, line, recv_t, x)
    values = mid[...]
    inverse = lax.rsqrt(jnp.mean(values * values, axis=-1, keepdims=True) + norm_eps)
    normed = values * inverse
    dnormed = dnorm * (1.0 + scale[...])
    terms[...] = jnp.sum(dnorm * normed, axis=0, keepdims=True)
    total = cot[...] + inverse * (
        dnormed - normed * jnp.mean(dnormed * normed, axis=-1, keepdims=True)
    )
    dmid[...] = total
    dmid_all[x] = cast(total)
    for other in beside:
        out.push(dmid_all.at[x], dmid_all.at[x], recv_x.at[x], {"tensor": other})
    for d in range(ctx):
        over_context(1, d)
    for other in beside:
        arrived(dmid_all.at[other], recv_x.at[other], twin)
    count, width = dmid_all.shape[0] * dmid_all.shape[1], dmid_all.shape[2]
    deep = width // chips

    def use(k, tile):
        lanes = pl.ds(pl.multiple_of(k * deep, deep), deep)
        add = jnp.dot(
            dmid_all[:, :, lanes].reshape(count, deep), tile, preferred_element_type=single
        )

        @pl.when(k == 0)
        def _():
            sums[...] = add

        @pl.when(k > 0)
        def _():
            sums[...] += add

    chip_tiles(slice_o, held_o, load, use)
    datt[...] = cast(sums[...])
    for w in range(2):
        for k in around[1:]:
            arrived(outs[w].at[k], recv_z.at[w, k], twin)
    for keep in keeps:
        keep.wait()
    out.drain()


def mlp_back(low_t, dy_t, hid, dpair, mid, cot, scale, slice_p, slice_o, fs, ctx, ten, ident):
    rows, columns = low_t.shape[2], hid.shape[1]
    t_rows, width = mid.shape
    chips = fs // 2
    blocks = [(rows, columns), (rows, 2 * columns)]
    sends = ctx * (ten - 1) + 2 * ctx + 2 * (chips + (chips - 1) * ctx + ctx - 1) + ten - 1
    dma = pltpu.SemaphoreType.DMA
    shape = jax.ShapeDtypeStruct
    return pl.pallas_call(
        functools.partial(back_kernel, fs, ctx, ten),
        out_shape=[
            shape((t_rows, width), single),
            shape((ten, t_rows, width), half_type),
            shape((ten * t_rows, slice_o.shape[3]), half_type),
            shape((1, width), single),
            shape((ctx, rows, 2 * columns), half_type),
            shape((ctx, rows, columns), half_type),
        ],
        in_specs=[VMEM] * 7 + [ANY] * 2,
        out_specs=[VMEM] * 4 + [ANY] * 2,
        scratch_shapes=[pltpu.VMEM((fs, ctx, *b), half_type) for b in blocks]
        + [pltpu.VMEM((chips, ctx, *b), half_type) for b in blocks]
        + [pltpu.VMEM((chips - 1, ctx, *b), half_type) for b in blocks]
        + [
            pltpu.VMEM((ctx, ten, t_rows, width), half_type),
            pltpu.VMEM((ten - 1, ctx, t_rows, width), half_type),
            pltpu.VMEM((ctx, t_rows, width), half_type),
            pltpu.VMEM((2, 2, ctx, rows, 2 * columns), half_type),
            pltpu.VMEM((2, 2, ctx, *slice_o.shape[2:]), half_type),
            pltpu.VMEM((ten * t_rows, slice_o.shape[3]), single),
            dma((2,)),
            dma((2,)),
            dma((sends,)),
            dma((2, chips)),
            dma((2, chips - 1, ctx)),
            dma((2, ctx)),
            dma((ten - 1, ctx)),
            dma((ctx + 1,)),
            dma((ten,)),
        ],
        compiler_params=pltpu.CompilerParams(
            collective_id=ident, has_side_effects=True, vmem_limit_bytes=VMEM_ALL
        ),
        name=f"mlp_back_{ident}",
    )(low_t, dy_t, hid, dpair, mid, cot, scale, slice_p, slice_o)


def update_kernel(parts, *refs):
    count = len(refs) // 7
    for w in range(count):
        weight, first, second = refs[3 * w : 3 * w + 3]
        outs = refs[3 * count + 4 * w : 3 * count + 4 * w + 4]
        columns = weight.shape[1] // parts.shape[0]
        for k in range(parts.shape[0]):
            grad = parts[k, :, w * columns : (w + 1) * columns].astype(single)
            here = (slice(None), slice(k * columns, (k + 1) * columns))
            values = (grad, *adamw(weight[here], grad, first[here], second[here]))
            for out, value in zip(outs, values):
                out[here] = value


def update(parts, weights, ident):
    ctx, rows, columns = parts.shape
    step = 80 if rows % 80 == 0 else 8
    wide = weights[0][0].shape[1]
    spec = pl.BlockSpec((step, wide), lambda i: (i, 0))
    part = pl.BlockSpec((ctx, step, columns), lambda i: (0, i, 0))
    count = len(weights)
    outs = pl.pallas_call(
        update_kernel,
        grid=(rows // step,),
        out_shape=[jax.ShapeDtypeStruct((rows, wide), single)] * (4 * count),
        in_specs=[part] + [spec] * (3 * count),
        out_specs=[spec] * (4 * count),
        compiler_params=pltpu.CompilerParams(vmem_limit_bytes=VMEM_ALL),
        name=f"update_{ident}",
    )(parts, *(v for group in weights for v in group))
    return [outs[4 * w : 4 * w + 4] for w in range(count)]


def attn_kernel(fs, ctx, ten, *refs):
    low_t, dmid_t, d_query, att, own, cosine, sine, hidden, mid, dmid, scale, terms = refs[:12]
    hid, slice_d, slice_q = refs[12:15]
    out_q, out_o, out_s, out_kv, tokens = refs[15:20]
    dws, nears, fars, lines = refs[20:25], refs[25:30], refs[30:35], refs[35:40]
    source, first, line, first_k, line_k, d_qkv, dnorm, take = refs[40:48]
    held_d, held_q, tail, pool, own_sums = refs[48:53]
    load, send, recv_c, recv_y, recv_z, recv_tx, recv_t, recv_kx, recv_k, recv_n, recv_x = refs[53:]
    f, y, core, twin, across = fsdp_place(fs)
    z, x = lax.axis_index("context"), lax.axis_index("tensor")
    chips = fs // 2
    rows = low_t.shape[2]
    beside = [lax.rem(x + d, ten) for d in range(1, ten)]
    rows_of = [lax.rem(y + d, chips) for d in range(chips)]
    chip_order = rows_of[1:] + rows_of[:1]
    partners = [{"context": partner} for partner, _, _ in doubling(z, ctx)]
    greet(partners + across + [twin] + [{"tensor": k} for k in beside])
    out = Sends(send)
    sends, own_slots = halving(z, ctx)
    order = [send_z[0] for send_z in sends] + [z]
    kinds = (cast, cast, cast, cast, lambda v: v)
    heads = d_query.shape[1]
    widths = [dw.shape[-1] for dw in dws[:4]]
    rights = (
        d_qkv.at[:, : widths[0]],
        d_qkv.at[:, widths[0] :],
        att.at[:, : widths[2]],
        att.at[:, widths[2] :],
    )
    lefts = (low_t, low_t, dmid_t, dmid_t)

    def start(w):
        for row in chip_order:
            owner = row * 2 + 1 - core
            if w < 4:
                fill_product(dws[w], lefts[w], rights[w], owner, ctx)
            out.push(dws[w].at[owner], nears[w].at[row], recv_c.at[w, row], twin)
        if w < 4:
            for row in chip_order:
                fill_product(dws[w], lefts[w], rights[w], row * 2 + core, ctx)

    def over_chips(w):
        for k, row in enumerate(rows_of[1:]):
            arrived(nears[w].at[row], recv_c.at[w, row], twin)
            for owner in order:
                mine = dws[w].at[row * 2 + core, owner]
                mine[...] = kinds[w](mine[...].astype(single) + nears[w][row, owner].astype(single))
                out.push(mine, fars[w].at[k, owner], recv_y.at[w, k, owner], across[k])

    def summed_block(w, owner, places):
        total = dws[w][f, owner].astype(single) + nears[w][y, owner].astype(single)
        for k in range(chips - 1):
            arrived(fars[w].at[k, owner], recv_y.at[w, k, owner], twin)
            total = total + fars[w][k, owner].astype(single)
        return collect(total, lines[w], recv_z.at[w], places, twin)

    def over_context(w, d):
        if d == 0:
            arrived(nears[w].at[y], recv_c.at[w, y], twin)
        owner, partner, slot, places = sends[d]
        mine = dws[w].at[f, owner]
        mine[...] = kinds[w](summed_block(w, owner, places))
        out.push(mine, lines[w].at[slot], recv_z.at[w, slot], {"context": partner})

    def finish(w):
        return summed_block(w, z, own_slots)

    own_sums[...] = own[...]
    token_start(own_sums, first_k, recv_kx, out, beside, order)
    start(2)
    over_chips(2)
    token_products(source, hid, slice_d, held_d, load)
    token_start(source, first, recv_tx, out, beside, order)
    start(3)
    over_chips(3)
    early, late = range(ctx // 2), range(ctx // 2, ctx - 1)
    for d in early:
        token_send(sends[d], own_sums, first_k, recv_kx, line_k, recv_k, x, out)
    for d in early:
        over_context(2, d)
    for d in late:
        token_send(sends[d], own_sums, first_k, recv_kx, line_k, recv_k, x, out)
    summed = token_sum(z, own_slots, own_sums, first_k, recv_kx, line_k, recv_k, x)
    half = summed.shape[1] // 2
    a, b = summed[:, :half], summed[:, half:]
    c, s = cosine[...], sine[...]
    is_key = x == 0
    d_qkv[:, :heads] = d_query[...]
    d_qkv[:, heads : heads + half] = cast(jnp.where(is_key, a * c + b * s, a))
    d_qkv[:, heads + half :] = cast(jnp.where(is_key, b * c - a * s, b))
    start(0)
    over_chips(0)
    for d in late:
        over_context(2, d)
    token_products(dnorm, d_qkv, slice_q, held_q, load)
    for other in beside:
        out.push(dnorm.at[0, other], take.at[x], recv_n.at[x], {"tensor": other})
    for d in early:
        token_send(sends[d], source, first, recv_tx, line, recv_t, x, out)
    for d in early:
        over_context(3, d)
    start(1)
    for d in late:
        token_send(sends[d], source, first, recv_tx, line, recv_t, x, out)
    for d in late:
        over_context(3, d)
    dnorm_one = dnorm[0, x].astype(single)
    for other in beside:
        arrived(take.at[other], recv_n.at[other], twin)
        dnorm_one = dnorm_one + take[other].astype(single)
    values = hidden[...]
    inverse = lax.rsqrt(jnp.mean(values * values, axis=-1, keepdims=True) + norm_eps)
    normed = values * inverse
    dnormed = dnorm_one * (1.0 + scale[...])
    tokens[x, 1] = cast(
        dmid[...]
        + inverse * (dnormed - normed * jnp.mean(dnormed * normed, axis=-1, keepdims=True))
    )
    sums = jnp.sum(dnorm_one * normed, axis=0, keepdims=True)
    dws[4][...] = jnp.zeros_like(dws[4])
    for j in range(fs * ctx):
        at = slice(j * rows, (j + 1) * rows)
        dws[4][j // ctx, j % ctx, 0:1, :rows] = sums[:, at]
        dws[4][j // ctx, j % ctx, 1:2, :rows] = terms[:, at]
    start(4)
    over_chips(4)
    over_chips(1)

    def hand_over(t):
        for other in beside:
            out.push(tokens.at[x, t], tokens.at[x, t], recv_x.at[2 + t, x], {"tensor": other})

    hand_over(1)
    for d in early:
        over_context(0, d)
    tokens[x, 0] = cast(
        mid[...] + token_sum(z, own_slots, source, first, recv_tx, line, recv_t, x)
    )
    hand_over(0)
    for d in early:
        over_context(4, d)
    for d in late:
        over_context(0, d)
    for d in early:
        over_context(1, d)
    for w in (4, 1):
        for d in late:
            over_context(w, d)
    pool[x] = finish(4)
    for other in beside:
        out.push(pool.at[x], pool.at[x], recv_x.at[0, x], {"tensor": other})
    out_o[:, : widths[2]] = finish(2)
    out_o[:, widths[2] :] = finish(3)
    out_q[:, : widths[0]] = finish(0)
    grad = finish(1)
    out_q[:, widths[0] :] = grad[:, : heads - widths[0]]
    tail[x] = cast(grad[:, heads - widths[0] :])
    for other in beside:
        out.push(tail.at[x], tail.at[x], recv_x.at[1, x], {"tensor": other})
    for other in beside:
        arrived(pool.at[other], recv_x.at[0, other], twin)
        arrived(tail.at[other], recv_x.at[1, other], twin)
        for t in range(2):
            arrived(tokens.at[other, t], recv_x.at[2 + t, other], twin)
    total = pool[0]
    for k in range(1, ten):
        total = total + pool[k]
    out_s[...] = total
    columns = tail.shape[-1]
    for k in range(ten):
        out_kv[:, k * columns : (k + 1) * columns] = tail[k].astype(single)
    out.drain()


def attn_back(
    low_t, dmid_t, d_query, att, own, cosine, sine, hidden, mid, dmid, scale, terms, hid, slice_d, slice_q,
    fs, ctx, ten, ident,
):
    rows = low_t.shape[2]
    t_rows, width = mid.shape
    chips = fs // 2
    heads = d_query.shape[1]
    count, tail = own.shape[2:]
    lanes = -(-rows // 128) * 128
    cuts = [-(-total // 256) * 128 for total in (heads + tail, att.shape[1])]
    both = [
        ((rows, cuts[0]), half_type),
        ((rows, heads + tail - cuts[0]), half_type),
        ((rows, cuts[1]), half_type),
        ((rows, att.shape[1] - cuts[1]), half_type),
        ((8, lanes), single),
    ]
    sends = (
        2 * (ctx * (ten - 1) + 2 * ctx)
        + 5 * (ten - 1)
        + 5 * (chips + (chips - 1) * ctx + 2 * ctx)
    )
    dma = pltpu.SemaphoreType.DMA
    shape = jax.ShapeDtypeStruct
    return pl.pallas_call(
        functools.partial(attn_kernel, fs, ctx, ten),
        out_shape=[
            shape((rows, heads), single),
            shape((rows, att.shape[1]), single),
            shape((8, lanes), single),
            shape((rows, ten * tail), single),
            shape((ten, 2, t_rows, width), half_type),
        ],
        in_specs=[VMEM] * 13 + [ANY] * 2,
        out_specs=[VMEM] * 5,
        scratch_shapes=[pltpu.VMEM((fs, ctx, *b), t) for b, t in both]
        + [pltpu.VMEM((chips, ctx, *b), t) for b, t in both]
        + [pltpu.VMEM((chips - 1, ctx, *b), t) for b, t in both]
        + [pltpu.VMEM((ctx + 1, *b), t) for b, t in both]
        + [
            pltpu.VMEM((ctx, ten, t_rows, width), half_type),
            pltpu.VMEM((ten - 1, ctx, t_rows, width), half_type),
            pltpu.VMEM((ctx + 1, t_rows, width), half_type),
            pltpu.VMEM((ten - 1, ctx, count, tail), half_type),
            pltpu.VMEM((ctx + 1, count, tail), half_type),
            pltpu.VMEM((count, heads + tail), half_type),
            pltpu.VMEM((1, ten, t_rows, width), half_type),
            pltpu.VMEM((ten, t_rows, width), half_type),
            pltpu.VMEM((2, 2, ctx, *slice_d.shape[2:]), half_type),
            pltpu.VMEM((2, 2, ctx, *slice_q.shape[2:]), half_type),
            pltpu.VMEM((ten, rows, tail), half_type),
            pltpu.VMEM((ten, 8, lanes), single),
            pltpu.VMEM(own.shape, half_type),
            dma((2,)),
            dma((sends,)),
            dma((5, chips)),
            dma((5, chips - 1, ctx)),
            dma((5, ctx + 1)),
            dma((ten - 1, ctx)),
            dma((ctx + 1,)),
            dma((ten - 1, ctx)),
            dma((ctx + 1,)),
            dma((ten,)),
            dma((4, ten)),
        ],
        compiler_params=pltpu.CompilerParams(
            collective_id=ident, has_side_effects=True, vmem_limit_bytes=VMEM_ALL
        ),
        name=f"attn_back_{ident}",
    )(low_t, dmid_t, d_query, att, own, cosine, sine, hidden, mid, dmid, scale, terms, hid, slice_d, slice_q)


def on_device(hidden_in, cotangent, segment_ids, positions, *params):
    masters, firsts, seconds = params[:8], params[8:16], params[16:]
    (
        attn_scale,
        query_weight,
        keyval_weight,
        output_weight,
        mlp_scale,
        gate_weight,
        up_weight,
        down_weight,
    ) = masters
    fs, ctx, ten = (lax.axis_size(name) for name in ("fsdp", "context", "tensor"))
    x = lax.axis_index("tensor")
    context_index = lax.axis_index("context")
    block, width = hidden_in.shape[1:]
    rows = query_weight.shape[0]
    half_rows = block // ten
    heads_width = query_weight.shape[1]
    heads_here = heads_width // HD
    hidden = hidden_in[0]
    cot = cotangent[0]
    hidden_half = lax.dynamic_slice_in_dim(hidden, x * half_rows, half_rows, 0)
    cot_half = lax.dynamic_slice_in_dim(cot, x * half_rows, half_rows, 0)
    is_key = x == 0

    qkv_block = jnp.concatenate(
        [
            cast(query_weight),
            cast(lax.dynamic_slice_in_dim(keyval_weight, x * HD, HD, 1)),
        ],
        axis=1,
    )
    lanes = -(-max(rows, block) // 128) * 128
    wide = [
        jnp.pad(v, (0, lanes - v.shape[0]))
        for v in (attn_scale, mlp_scale, segment_ids[0].astype(single))
    ]
    small = jnp.stack(wide + [jnp.zeros((lanes,), single)] * 5)
    small_all, qkv_all, out_all, dy_all, part_p, part_d = spread(
        [small, qkv_block, cast(output_weight.T)],
        cast(cot_half),
        [gate_weight, up_weight, down_weight.T],
        fs,
        ctx,
        ten,
        1,
    )
    scale_one = cast(small_all[:, :, 0, :rows].reshape(-1)).astype(single)
    scale_two = cast(small_all[:, :, 1, :rows].reshape(-1)).astype(single)
    f = lax.axis_index("fsdp")
    seg_all = lax.dynamic_index_in_dim(small_all[:, :, 2, :block], f, 0, False).reshape(-1)
    qkv_full = qkv_all.reshape(width, -1)

    _, _, low_one = rms_forward(hidden, scale_one)
    qkv = dot(low_one, qkv_full, ((1,), (0,)))
    query = qkv[:, :heads_width].reshape(block, heads_here, HD)
    own = qkv[:, heads_width:]
    cosine, sine = rope_tables(positions[0])
    query_low = cast(rotate(query, cosine[:, None, :], sine[:, None, :]) * HD ** (-0.5))
    own_low = cast(jnp.where(is_key, rotate(own, cosine, sine), own))
    keyval_all = tokens_to_all(own_low, ctx, ten, 2).reshape(ctx, ten, block, HD)
    keys_all = keyval_all[:, 0].reshape(-1, HD)
    values_all = keyval_all[:, 1].reshape(-1, HD)
    rows_index = context_index * block + jnp.arange(block, dtype=jnp.int32)
    cols_index = jnp.arange(keys_all.shape[0], dtype=jnp.int32)
    allowed = (rows_index[:, None] >= cols_index[None, :]) & (
        segment_ids[0].astype(single)[:, None] == seg_all[None, :]
    )
    scores = jnp.einsum("bhd,jd->hbj", query_low, keys_all, preferred_element_type=single)
    masked = jnp.where(allowed, scores, masked_value)
    top = jnp.max(masked, axis=-1, keepdims=True)
    total = jnp.sum(jnp.where(allowed, jnp.exp(masked - top), 0.0), axis=-1, keepdims=True)
    lse = top + jnp.log(total)
    prob = jnp.where(allowed, jnp.exp(masked - lse), 0.0)
    prob_low = cast(prob)
    att_low = cast(
        jnp.einsum("hbj,jd->bhd", prob_low, values_all, preferred_element_type=single)
    )
    att_flat = att_low.reshape(block, heads_width)
    slice_p, slice_d, hid, dpair, low_t, dy_t, mid_half = mlp_forward(
        att_flat,
        hidden_half,
        scale_two[None],
        dy_all,
        part_p,
        part_d,
        out_all,
        fs,
        ctx,
        ten,
        4,
    )
    dmid_half, dmid_low, datt, terms_two, part_p, part_d = mlp_back(
        low_t, dy_t, hid, dpair, mid_half, cot_half, scale_two[None], slice_p, out_all, fs, ctx, ten, 5
    )

    dmid_low = dmid_low.reshape(block, width)
    datt_low = datt.reshape(block, heads_here, HD)
    delta = jnp.einsum("bhd,bhd->hb", datt_low, att_low, preferred_element_type=single)
    dprob = jnp.einsum("bhd,jd->hbj", datt_low, values_all, preferred_element_type=single)
    dscore_low = cast(prob * (dprob - delta[..., None]))
    dquery = jnp.einsum("hbj,jd->bhd", dscore_low, keys_all, preferred_element_type=single)
    dkey_part = jnp.einsum("hbj,bhd->jd", dscore_low, query_low, preferred_element_type=single)
    dvalue_part = jnp.einsum("hbj,bhd->jd", prob_low, datt_low, preferred_element_type=single)
    own_part = jnp.stack(
        [cast(part).reshape(ctx, block, HD) for part in (dkey_part, dvalue_part)], axis=1
    )
    dquery_low = cast(
        unrotate(dquery, cosine[:, None, :], sine[:, None, :]) * HD ** (-0.5)
    ).reshape(block, heads_width)
    row_blocks = (fs, ctx, rows, -1)
    grad_wq, grad_wo, grad_s, grad_wkv, outs = attn_back(
        low_one.T.reshape(row_blocks),
        dmid_low.T.reshape(row_blocks),
        dquery_low,
        att_flat,
        own_part,
        cosine,
        sine,
        hidden_half,
        mid_half,
        dmid_half,
        scale_one[None],
        terms_two,
        hid,
        slice_d,
        qkv_all,
        fs,
        ctx,
        ten,
        9,
    )
    outs = outs.transpose(1, 0, 2, 3).reshape(2, 1, block, width).astype(single)

    grads = (grad_s[0, :rows], grad_wq, grad_wkv, grad_wo.T, grad_s[1, :rows])
    results = [
        (grad, *adamw(weight, grad, first, second))
        for weight, grad, first, second in zip(masters, grads, firsts, seconds)
    ]
    groups = list(zip(masters, firsts, seconds))
    results += update(part_p, groups[5:7], 5)
    results += [[v.T for v in update(part_d, [[v.T for v in groups[7]]], 7)[0]]]
    return (
        outs[0],
        outs[1],
        *(entry[0] for entry in results),
        *(entry[1] for entry in results),
        *(entry[2] for entry in results),
        *(entry[3] for entry in results),
    )


def solution(mesh):
    both = ("fsdp", "context")
    tokens = P("fsdp", "context", None)
    weights = (
        P(both),
        P(both, "tensor"),
        P(both, None),
        P("tensor", both),
        P(both),
        P(both, "tensor"),
        P(both, "tensor"),
        P("tensor", both),
    )
    return jax.shard_map(
        on_device,
        mesh=mesh,
        in_specs=(tokens, tokens, P("fsdp", "context"), P("fsdp", "context"), *(weights * 3)),
        out_specs=(tokens, tokens, *(weights * 4)),
        check_vma=False,
    )
```
